128 devices in a mesh: dp: 4 (over x_hi, core), fsdp: 8 (over z, x_lo), tensor: 4 (over y).
Axes of the slice: x: 4 (x_hi: 2, x_lo: 2; x = x_hi * 2 + x_lo), y: 4, z: 4, core: 2. Of those that a mesh axis runs over, the one named last changes fastest.
Arguments:
- tokens: bfloat16 [32, 768, 8192], P(('dp', 'fsdp'), 'tensor'), may hold values from -6 to 6
- norm_gain: float32 [8192], replicated, may hold values from 0.85 to 4
- w_qkv: bfloat16 [8192, 5120], P(('dp', 'fsdp'), 'tensor'), may hold values from -0.3 to 0.3
- a_query: bfloat16 [8192, 16], replicated, may hold values from -0.0625 to 0.0625
- query_up_adapter: bfloat16 [16, 4096], P(None, 'tensor'), may hold values from -1.5 to 1.5
- a_value: bfloat16 [8192, 16], replicated, may hold values from -0.0625 to 0.0625
- value_up_adapter: bfloat16 [16, 512], P(None, 'tensor'), may hold values from -1.5 to 1.5
- out_grad: bfloat16 [32, 768, 4096], P(('dp', 'fsdp'), 'tensor'), may hold values from -6 to 6
Outputs:
- attn_out: bfloat16 [32, 768, 4096], P(('dp', 'fsdp'), 'tensor')
- grad_a_query: float32 [8192, 16], replicated
- grad_b_query: float32 [16, 4096], P(None, 'tensor')
- grad_a_value: float32 [8192, 16], replicated
- grad_b_value: float32 [16, 512], P(None, 'tensor')
The draws below stay inside these ranges and needn't reach their ends.
All inputs are finite; a program needn't handle non-finite values.
Results may differ from the reference program's by a relative error of at most 0.015.
The reference program's roundings to bfloat16 on the way count: a program that leaves them out, or rounds other values in their place, can miss the bound.
Values may be sent and summed in bfloat16 or wider, within the bound.
A program may use at most 256 MiB of HBM per device.

```python
import math
import jax
import jax.numpy as jnp
from jax import lax

D = 8192
KV = 4
HD = 128
RANK = 16
QUERY_PER_KV = 8
SEQ = 768
BATCH = 32
QCOLS = 4096
QKV = 5120


WEIGHT_EDGE = 0.296875


def draw_norm_gain(key, part):
    return 1.0 + 0.15 * jax.random.uniform(key, (D,), jnp.float32, -1.0, 1.0)


def draw_tokens(key, part):
    base = jax.random.normal(jax.random.fold_in(key, 11), (BATCH, SEQ, D), jnp.float32)
    return jnp.clip(base, -6.0, 6.0).astype(jnp.bfloat16)


def draw_w_qkv(key, part):
    base = jax.random.normal(jax.random.fold_in(key, 21), (D, QKV), jnp.float32) * (1.0 / math.sqrt(D))
    return jnp.clip(base, -WEIGHT_EDGE, WEIGHT_EDGE).astype(jnp.bfloat16)


def steps_of(stream_key, shape, pieces, least, largest):
    gain = 1.0
    for position, parts in pieces:
        heights = jax.random.uniform(jax.random.fold_in(jax.random.fold_in(stream_key, 6), position), (parts,), jnp.float32, least / len(pieces), largest / len(pieces))
        gain = gain * jnp.repeat(jnp.exp(heights), shape[position] // parts).reshape((-1,) + (1,) * (len(shape) - 1 - position))
    return gain


def normal_values(stream_key, extent, width, bound, shards=(), kind=jnp.bfloat16):
    loudness = steps_of(stream_key, extent, shards, -0.22, 0.18) if shards else 1.0
    drawn = jax.random.normal(stream_key, extent, jnp.float32) * width * loudness
    return jnp.minimum(jnp.maximum(drawn, -bound), bound).astype(kind)


def setup_inputs(seed: int = 0) -> dict:
    keys = jax.random.split(jax.random.key(seed), 9)
    tokens = draw_tokens(jax.random.fold_in(keys[8], 71), 0)
    norm_gain = draw_norm_gain(jax.random.fold_in(keys[8], 71), 0)
    w_qkv = draw_w_qkv(jax.random.fold_in(keys[8], 71), 0)
    a_query = normal_values(keys[3], (D, RANK), D ** -0.5, 0.0625)
    query_up_adapter = normal_values(keys[4], (RANK, QCOLS), RANK ** -0.5, 1.5, ((1, 4),))
    a_value = normal_values(keys[5], (D, RANK), D ** -0.5, 0.0625)
    value_up_adapter = normal_values(keys[6], (RANK, KV * HD), RANK ** -0.5, 1.5, ((1, 4),))
    out_grad = normal_values(keys[7], (BATCH, SEQ, QCOLS), 1.0, 6.0, ((0, 32), (1, 4)))
    return {"tokens": tokens, "norm_gain": norm_gain, "w_qkv": w_qkv, "a_query": a_query, "query_up_adapter": query_up_adapter, "a_value": a_value, "value_up_adapter": value_up_adapter, "out_grad": out_grad}


EPSILON = 1e-05
ADAPTER_SCALE = 2.0
ROPE_BASE = 500000.0

def normalize(own_rows, norm_gain):
    widened = own_rows.astype(jnp.float32)
    mean_square = lax.optimization_barrier(jnp.mean(widened * widened, axis=-1, keepdims=True))
    return (widened * lax.rsqrt(mean_square + EPSILON) * norm_gain).astype(jnp.bfloat16)

def rotary(heads_block):
    sequence_length = heads_block.shape[0]
    half_dim = heads_block.shape[-1] // 2
    positions = jnp.arange(sequence_length, dtype=jnp.float32)[:, None]
    inv_freq = ROPE_BASE ** (-jnp.arange(half_dim, dtype=jnp.float32) / half_dim)
    angles = positions * inv_freq
    cosine = jnp.cos(angles)[:, None, :]
    sine_table = jnp.sin(angles)[:, None, :]
    front_half = heads_block[..., :half_dim].astype(jnp.float32)
    back_half = heads_block[..., half_dim:].astype(jnp.float32)
    turned = jnp.concatenate([front_half * cosine - back_half * sine_table, back_half * cosine + front_half * sine_table], -1)
    return turned.astype(jnp.bfloat16)

def attend(query_rows, key_heads, value_rows):
    sequence_length = query_rows.shape[0]
    kv_heads = key_heads.shape[1] // HD
    rot_queries = rotary(query_rows.reshape(sequence_length, kv_heads * QUERY_PER_KV, HD))
    rot_keys = rotary(key_heads.reshape(sequence_length, kv_heads, HD))
    split_values = value_rows.reshape(sequence_length, kv_heads, HD)
    causal = jnp.arange(sequence_length)[:, None] >= jnp.arange(sequence_length)[None, :]

    def one_head(head_index):
        q_head = lax.dynamic_index_in_dim(rot_queries, head_index, 1, keepdims=False)
        k_head = lax.dynamic_index_in_dim(rot_keys, head_index // QUERY_PER_KV, 1, keepdims=False)
        v_head = lax.dynamic_index_in_dim(split_values, head_index // QUERY_PER_KV, 1, keepdims=False)
        scores = jnp.dot(q_head, k_head.T, preferred_element_type=jnp.float32) * (1.0 / math.sqrt(HD))
        scores = jnp.where(causal, scores, -1e+30)
        row_max = lax.optimization_barrier(jnp.max(scores, axis=-1, keepdims=True))
        weights = jnp.exp(scores - row_max)
        probabilities = (weights / lax.optimization_barrier(jnp.sum(weights, axis=-1, keepdims=True))).astype(jnp.bfloat16)
        return jnp.dot(probabilities, v_head, preferred_element_type=jnp.float32).astype(jnp.bfloat16)
    per_head = lax.map(one_head, jnp.arange(kv_heads * QUERY_PER_KV, dtype=jnp.int32))
    return jnp.transpose(per_head, (1, 0, 2)).reshape(sequence_length, kv_heads * QUERY_PER_KV * HD)

def reference(tokens, norm_gain, w_qkv, a_query, query_up_adapter, a_value, value_up_adapter, out_grad):
    adapters = jnp.concatenate([a_query, a_value], 1)
    narrow_rank_rows = a_query.shape[1]

    def one_sequence(pair):
        own_rows, grad_rows = pair
        normed_input = normalize(own_rows, norm_gain)
        sequence_length = normed_input.shape[0]
        projected = jnp.dot(normed_input, w_qkv, preferred_element_type=jnp.float32)
        down_projected = jnp.dot(normed_input, adapters, preferred_element_type=jnp.float32).astype(jnp.bfloat16)
        grouped_queries = projected.reshape(sequence_length, KV, QUERY_PER_KV + 2, HD)
        query_rows = (grouped_queries[:, :, :QUERY_PER_KV].reshape(sequence_length, -1) + ADAPTER_SCALE * jnp.dot(down_projected[:, :narrow_rank_rows], query_up_adapter, preferred_element_type=jnp.float32)).astype(jnp.bfloat16)
        key_heads = grouped_queries[:, :, QUERY_PER_KV].reshape(sequence_length, -1).astype(jnp.bfloat16)
        value_rows = (grouped_queries[:, :, QUERY_PER_KV + 1].reshape(sequence_length, -1) + ADAPTER_SCALE * jnp.dot(down_projected[:, narrow_rank_rows:], value_up_adapter, preferred_element_type=jnp.float32)).astype(jnp.bfloat16)
        attended, pullback = jax.vjp(attend, query_rows, key_heads, value_rows)
        query_gradient, grad_keys, value_gradient = pullback(grad_rows)
        query_up_gradient = ADAPTER_SCALE * jnp.einsum('fb,fd->bd', down_projected[:, :narrow_rank_rows], query_gradient, preferred_element_type=jnp.float32)
        value_up_gradient = ADAPTER_SCALE * jnp.einsum('fb,fd->bd', down_projected[:, narrow_rank_rows:], value_gradient, preferred_element_type=jnp.float32)
        middle_gradient = jnp.concatenate([jnp.dot(query_gradient, query_up_adapter.T, preferred_element_type=jnp.float32), jnp.dot(value_gradient, value_up_adapter.T, preferred_element_type=jnp.float32)], 1).astype(jnp.bfloat16)
        down_gradient = ADAPTER_SCALE * jnp.einsum('uh,ux->hx', normed_input, middle_gradient, preferred_element_type=jnp.float32)
        return (attended, down_gradient, query_up_gradient, value_up_gradient)
    attn_out, down_gradient, query_up_gradient, value_up_gradient = lax.map(one_sequence, (tokens, out_grad))
    down_gradient = lax.optimization_barrier(jnp.sum(down_gradient, axis=0))
    return (attn_out, down_gradient[:, :narrow_rank_rows], lax.optimization_barrier(jnp.sum(query_up_gradient, axis=0)), down_gradient[:, narrow_rank_rows:], lax.optimization_barrier(jnp.sum(value_up_gradient, axis=0)))
```

```python
import functools
import math

import jax
import jax.numpy as jnp
from jax import lax
from jax.experimental import pallas as pl
from jax.experimental.pallas import tpu as pltpu
from jax.sharding import PartitionSpec as P

HD = 128
QUERY_PER_KV = 8
RANK = 16
QB = 256

EPSILON = 1e-05
ADAPTER_SCALE = 2.0
ROPE_BASE = 500000.0
SCORE_SCALE = 1.0 / math.sqrt(HD)
LOG2E = 1.4426950408889634
ALL = ("dp", "fsdp", "tensor")


def from_everyone(array, axis):
    copies = jnp.broadcast_to(array, (lax.axis_size(axis), *array.shape))
    return lax.all_to_all(copies, axis, split_axis=0, concat_axis=0, tiled=True)


def normalize(own_rows, norm_gain):
    widened = own_rows.astype(jnp.float32)
    mean_square = jnp.mean(widened * widened, axis=-1, keepdims=True)
    return (widened * lax.rsqrt(mean_square + EPSILON) * norm_gain).astype(jnp.bfloat16)


def rotary_tables(sequence_length):
    half_dim = HD // 2
    positions = jnp.arange(sequence_length, dtype=jnp.float32)[:, None]
    inv_freq = ROPE_BASE ** (-jnp.arange(half_dim, dtype=jnp.float32) / half_dim)
    angles = positions * inv_freq
    cosine = jnp.cos(angles)
    sine = jnp.sin(angles)
    return jnp.concatenate([cosine, cosine], 1), jnp.concatenate([-sine, sine], 1)


def dot_nt(a, b):
    return lax.dot_general(a, b, (((1,), (1,)), ((), ())), preferred_element_type=jnp.float32)


def dot_nn(a, b):
    return jnp.dot(a, b, preferred_element_type=jnp.float32)


def rotate(x, cos, sin):
    return x * cos + pltpu.roll(x, HD // 2, 1) * sin


def attention_kernel(
    seq,
    proj_ref,
    key_ref,
    value_ref,
    down_ref,
    down_t_ref,
    qup_ref,
    vup_ref,
    cos_ref,
    sin_ref,
    grad_ref,
    out_ref,
    gbq_ref,
    gbv_ref,
    mid_t_ref,
    k_scr,
    v_scr,
    dv_scr,
    q_scr,
    dq_scr,
    mid_scr,
):
    head = pl.program_id(0)
    blocks = seq // QB

    @pl.when(head == 0)
    def _():
        k_scr[...] = rotate(
            key_ref[...].astype(jnp.bfloat16).astype(jnp.float32), cos_ref[...], sin_ref[...]
        ).astype(jnp.bfloat16)
        v_scr[...] = (
            value_ref[...] + ADAPTER_SCALE * dot_nn(down_ref[:, RANK:], vup_ref[...])
        ).astype(jnp.bfloat16)
        dv_scr[...] = jnp.zeros_like(dv_scr)
        mid_scr[...] = jnp.zeros_like(mid_scr)

    queries = (proj_ref[...] + ADAPTER_SCALE * dot_nn(down_ref[:, :RANK], qup_ref[...])).astype(
        jnp.bfloat16
    )
    q_scr[...] = rotate(queries.astype(jnp.float32), cos_ref[...], sin_ref[...]).astype(
        jnp.bfloat16
    )
    row = lax.broadcasted_iota(jnp.int32, (QB, QB), 0)
    col = lax.broadcasted_iota(jnp.int32, (QB, QB), 1)
    causal = row >= col
    factor = SCORE_SCALE * LOG2E
    for i in range(blocks):
        rows = slice(i * QB, (i + 1) * QB)
        q = q_scr[rows, :]
        grad = grad_ref[rows, :]
        grad_t = grad.T
        scores = []
        for j in range(i + 1):
            s = dot_nt(q, k_scr[j * QB : (j + 1) * QB, :])
            if j == i:
                s = jnp.where(causal, s, -1e30)
            scores.append(s)
        top = functools.reduce(jnp.maximum, scores)
        top = jnp.max(top, axis=-1, keepdims=True) * factor
        weights = [jnp.exp2(s * factor - top) for s in scores]
        total = jnp.sum(functools.reduce(jnp.add, weights), axis=-1, keepdims=True)
        inverse = 1.0 / total
        probs = [w * inverse for w in weights]
        rounded = [p.astype(jnp.bfloat16) for p in probs]
        attended = functools.reduce(
            jnp.add, [dot_nn(rounded[j], v_scr[j * QB : (j + 1) * QB, :]) for j in range(i + 1)]
        )
        out_ref[rows, :] = attended.astype(jnp.bfloat16)
        prods = []
        for j in range(i + 1):
            keys = slice(j * QB, (j + 1) * QB)
            dp = dot_nt(grad, v_scr[keys, :])
            prods.append(probs[j] * dp)
            dv_scr[:, keys] += dot_nn(grad_t, rounded[j])
        inner = jnp.sum(functools.reduce(jnp.add, prods), axis=-1, keepdims=True)
        ds = [(prods[j] - probs[j] * inner).astype(jnp.bfloat16) for j in range(i + 1)]
        dq = functools.reduce(
            jnp.add, [dot_nn(ds[j], k_scr[j * QB : (j + 1) * QB, :]) for j in range(i + 1)]
        )
        dq = (dq * SCORE_SCALE).astype(jnp.bfloat16).astype(jnp.float32)
        dq_scr[rows, :] = rotate(dq, cos_ref[rows, :], -sin_ref[rows, :]).astype(jnp.bfloat16)
    dq = dq_scr[...]
    gbq_ref[...] = ADAPTER_SCALE * dot_nn(down_t_ref[:RANK, :], dq)
    mid_scr[...] += dot_nt(qup_ref[...], dq)

    @pl.when(head == QUERY_PER_KV - 1)
    def _():
        dv = dv_scr[...].T.astype(jnp.bfloat16)
        gbv_ref[...] = ADAPTER_SCALE * dot_nn(down_t_ref[RANK:, :], dv)
        mid_t_ref[:RANK, :] = mid_scr[...]
        mid_t_ref[RANK:, :] = dot_nt(vup_ref[...], dv)


def attention(projected, down, down_t, qup, vup, cos, sin, grad_rows):
    seq = projected.shape[0]
    heads = QUERY_PER_KV

    def whole(shape):
        return pl.BlockSpec(shape, lambda h: (0, 0))

    column = lambda h: (0, h)
    return pl.pallas_call(
        functools.partial(attention_kernel, seq),
        grid=(heads,),
        in_specs=[
            pl.BlockSpec((seq, HD), column),
            pl.BlockSpec((seq, HD), lambda h: (0, heads)),
            pl.BlockSpec((seq, HD), lambda h: (0, heads + 1)),
            whole((seq, 2 * RANK)),
            whole((2 * RANK, seq)),
            pl.BlockSpec((RANK, HD), column),
            whole((RANK, HD)),
            whole((seq, HD)),
            whole((seq, HD)),
            pl.BlockSpec((seq, HD), column),
        ],
        out_specs=[
            pl.BlockSpec((seq, HD), column),
            pl.BlockSpec((RANK, HD), column),
            whole((RANK, HD)),
            whole((2 * RANK, seq)),
        ],
        out_shape=[
            jax.ShapeDtypeStruct((seq, heads * HD), jnp.bfloat16),
            jax.ShapeDtypeStruct((RANK, heads * HD), jnp.float32),
            jax.ShapeDtypeStruct((RANK, HD), jnp.float32),
            jax.ShapeDtypeStruct((2 * RANK, seq), jnp.float32),
        ],
        scratch_shapes=[
            pltpu.VMEM((seq, HD), jnp.bfloat16),
            pltpu.VMEM((seq, HD), jnp.bfloat16),
            pltpu.VMEM((HD, seq), jnp.float32),
            pltpu.VMEM((seq, HD), jnp.bfloat16),
            pltpu.VMEM((seq, HD), jnp.bfloat16),
            pltpu.VMEM((RANK, seq), jnp.float32),
        ],
        compiler_params=pltpu.CompilerParams(dimension_semantics=("arbitrary",)),
        cost_estimate=pl.CostEstimate(
            flops=10 * heads * seq * seq * HD,
            bytes_accessed=16 * seq * heads * HD,
            transcendentals=heads * seq * seq,
        ),
        name="attention_step",
    )(projected, projected, projected, down, down_t, qup, vup, cos, sin, grad_rows)


def local(tokens, norm_gain, w_qkv, a_query, query_up_adapter, a_value, value_up_adapter, out_grad):
    normed = normalize(tokens[0], norm_gain)
    tiles = from_everyone(normed, "tensor")
    gathered = tiles.reshape(-1, normed.shape[1])
    seq = gathered.shape[0]
    weights = lax.all_gather(w_qkv, ("dp", "fsdp"), axis=0, tiled=True)
    projected = jnp.dot(gathered, weights, preferred_element_type=jnp.float32)
    down = jnp.dot(
        gathered, jnp.concatenate([a_query, a_value], 1), preferred_element_type=jnp.float32
    ).astype(jnp.bfloat16)
    grad_rows = lax.all_to_all(out_grad[0], "tensor", split_axis=1, concat_axis=0, tiled=True)
    cos, sin = rotary_tables(seq)
    attended, gbq, gbv, mid_t = attention(
        projected, down, down.T, query_up_adapter, value_up_adapter, cos, sin, grad_rows
    )
    out_rows = lax.all_to_all(attended, "tensor", split_axis=0, concat_axis=1, tiled=True)
    groups = lax.axis_size("tensor")
    own = seq // groups
    mid_split = mid_t.reshape(2 * RANK, groups, own).transpose(1, 0, 2)
    mid = (
        lax.all_to_all(mid_split, "tensor", split_axis=0, concat_axis=0, tiled=True)
        .sum(axis=0)
        .astype(jnp.bfloat16)
    )
    grad_a = ADAPTER_SCALE * dot_nn(mid, normed)
    up = jnp.concatenate([gbq, gbv], 1)
    slots = jnp.zeros((groups, *up.shape), jnp.float32)
    slots = lax.dynamic_update_index_in_dim(slots, up, lax.axis_index("tensor"), 0)
    grad_a, slots = lax.psum((grad_a, slots), ALL)
    up = lax.dynamic_index_in_dim(slots, lax.axis_index("tensor"), 0, keepdims=False)
    return (
        out_rows[None],
        grad_a[:RANK].T,
        up[:, : gbq.shape[1]],
        grad_a[RANK:].T,
        up[:, gbq.shape[1] :],
    )


def solution(mesh):
    return jax.shard_map(
        local,
        mesh=mesh,
        in_specs=(
            P(("dp", "fsdp"), "tensor", None),
            P(),
            P(("dp", "fsdp"), "tensor"),
            P(),
            P(None, "tensor"),
            P(),
            P(None, "tensor"),
            P(("dp", "fsdp"), "tensor", None),
        ),
        out_specs=(
            P(("dp", "fsdp"), "tensor", None),
            P(),
            P(None, "tensor"),
            P(),
            P(None, "tensor"),
        ),
        check_vma=False,
    )
```

```python
import functools
import math

import jax
import jax.numpy as jnp
from jax import lax
from jax.experimental import pallas as pl
from jax.experimental.pallas import tpu as pltpu
from jax.sharding import PartitionSpec as P

HD = 128
QUERY_PER_KV = 8
RANK = 16
QB = 256

EPSILON = 1e-05
ADAPTER_SCALE = 2.0
ROPE_BASE = 500000.0
SCORE_SCALE = 1.0 / math.sqrt(HD)
LOG2E = 1.4426950408889634
ALL = ("dp", "fsdp", "tensor")


def rotary_tables(sequence_length):
    half_dim = HD // 2
    positions = jnp.arange(sequence_length, dtype=jnp.float32)[:, None]
    inv_freq = ROPE_BASE ** (-jnp.arange(half_dim, dtype=jnp.float32) / half_dim)
    angles = positions * inv_freq
    cosine = jnp.cos(angles)
    sine = jnp.sin(angles)
    return jnp.concatenate([cosine, cosine], 1), jnp.concatenate([-sine, sine], 1)


def dot_nt(a, b):
    return lax.dot_general(a, b, (((1,), (1,)), ((), ())), preferred_element_type=jnp.float32)


def dot_nn(a, b):
    return jnp.dot(a, b, preferred_element_type=jnp.float32)


def rotate(x, cos, sin):
    return x * cos + pltpu.roll(x, HD // 2, 1) * sin


def attention_kernel(
    seq,
    proj_ref,
    key_ref,
    value_ref,
    down_ref,
    down_t_ref,
    qup_ref,
    vup_ref,
    cos_ref,
    sin_ref,
    grad_ref,
    out_ref,
    gbq_ref,
    gbv_ref,
    mid_t_ref,
    k_scr,
    v_scr,
    dv_scr,
    q_scr,
    dq_scr,
    mid_scr,
):
    head = pl.program_id(0)
    blocks = seq // QB

    @pl.when(head == 0)
    def _():
        k_scr[...] = rotate(
            key_ref[...].astype(jnp.bfloat16).astype(jnp.float32), cos_ref[...], sin_ref[...]
        ).astype(jnp.bfloat16)
        v_scr[...] = (
            value_ref[...] + ADAPTER_SCALE * dot_nn(down_ref[:, RANK:], vup_ref[...])
        ).astype(jnp.bfloat16)
        dv_scr[...] = jnp.zeros_like(dv_scr)
        mid_scr[...] = jnp.zeros_like(mid_scr)

    queries = (proj_ref[...] + ADAPTER_SCALE * dot_nn(down_ref[:, :RANK], qup_ref[...])).astype(
        jnp.bfloat16
    )
    q_scr[...] = rotate(queries.astype(jnp.float32), cos_ref[...], sin_ref[...]).astype(
        jnp.bfloat16
    )
    row = lax.broadcasted_iota(jnp.int32, (QB, QB), 0)
    col = lax.broadcasted_iota(jnp.int32, (QB, QB), 1)
    causal = row >= col
    factor = SCORE_SCALE * LOG2E
    for i in range(blocks):
        rows = slice(i * QB, (i + 1) * QB)
        q = q_scr[rows, :]
        grad = grad_ref[rows, :]
        grad_t = grad.T
        scores = []
        for j in range(i + 1):
            s = dot_nt(q, k_scr[j * QB : (j + 1) * QB, :])
            if j == i:
                s = jnp.where(causal, s, -1e30)
            scores.append(s)
        top = functools.reduce(jnp.maximum, scores)
        top = jnp.max(top, axis=-1, keepdims=True) * factor
        weights = [jnp.exp2(s * factor - top) for s in scores]
        total = jnp.sum(functools.reduce(jnp.add, weights), axis=-1, keepdims=True)
        inverse = 1.0 / total
        probs = [w * inverse for w in weights]
        rounded = [p.astype(jnp.bfloat16) for p in probs]
        attended = functools.reduce(
            jnp.add, [dot_nn(rounded[j], v_scr[j * QB : (j + 1) * QB, :]) for j in range(i + 1)]
        )
        out_ref[rows, :] = attended.astype(jnp.bfloat16)
        prods = []
        for j in range(i + 1):
            keys = slice(j * QB, (j + 1) * QB)
            dp = dot_nt(grad, v_scr[keys, :])
            prods.append(probs[j] * dp)
            dv_scr[:, keys] += dot_nn(grad_t, rounded[j])
        inner = jnp.sum(functools.reduce(jnp.add, prods), axis=-1, keepdims=True)
        ds = [(prods[j] - probs[j] * inner).astype(jnp.bfloat16) for j in range(i + 1)]
        dq = functools.reduce(
            jnp.add, [dot_nn(ds[j], k_scr[j * QB : (j + 1) * QB, :]) for j in range(i + 1)]
        )
        dq = (dq * SCORE_SCALE).astype(jnp.bfloat16).astype(jnp.float32)
        dq_scr[rows, :] = rotate(dq, cos_ref[rows, :], -sin_ref[rows, :]).astype(jnp.bfloat16)
    dq = dq_scr[...]
    gbq_ref[...] = ADAPTER_SCALE * dot_nn(down_t_ref[:RANK, :], dq)
    mid_scr[...] += dot_nt(qup_ref[...], dq)

    @pl.when(head == QUERY_PER_KV - 1)
    def _():
        dv = dv_scr[...].T.astype(jnp.bfloat16)
        gbv_ref[...] = ADAPTER_SCALE * dot_nn(down_t_ref[RANK:, :], dv)
        mid_t_ref[:RANK, :] = mid_scr[...]
        mid_t_ref[RANK:, :] = dot_nt(vup_ref[...], dv)


def attention(projected, down, down_t, qup, vup, cos, sin, grad_rows):
    seq = projected.shape[0]
    heads = QUERY_PER_KV

    def whole(shape):
        return pl.BlockSpec(shape, lambda h: (0, 0))

    column = lambda h: (0, h)
    return pl.pallas_call(
        functools.partial(attention_kernel, seq),
        grid=(heads,),
        in_specs=[
            pl.BlockSpec((seq, HD), column),
            pl.BlockSpec((seq, HD), lambda h: (0, heads)),
            pl.BlockSpec((seq, HD), lambda h: (0, heads + 1)),
            whole((seq, 2 * RANK)),
            whole((2 * RANK, seq)),
            pl.BlockSpec((RANK, HD), column),
            whole((RANK, HD)),
            whole((seq, HD)),
            whole((seq, HD)),
            pl.BlockSpec((seq, HD), column),
        ],
        out_specs=[
            pl.BlockSpec((seq, HD), column),
            pl.BlockSpec((RANK, HD), column),
            whole((RANK, HD)),
            whole((2 * RANK, seq)),
        ],
        out_shape=[
            jax.ShapeDtypeStruct((seq, heads * HD), jnp.bfloat16),
            jax.ShapeDtypeStruct((RANK, heads * HD), jnp.float32),
            jax.ShapeDtypeStruct((RANK, HD), jnp.float32),
            jax.ShapeDtypeStruct((2 * RANK, seq), jnp.float32),
        ],
        scratch_shapes=[
            pltpu.VMEM((seq, HD), jnp.bfloat16),
            pltpu.VMEM((seq, HD), jnp.bfloat16),
            pltpu.VMEM((HD, seq), jnp.float32),
            pltpu.VMEM((seq, HD), jnp.bfloat16),
            pltpu.VMEM((seq, HD), jnp.bfloat16),
            pltpu.VMEM((RANK, seq), jnp.float32),
        ],
        compiler_params=pltpu.CompilerParams(dimension_semantics=("arbitrary",)),
        cost_estimate=pl.CostEstimate(
            flops=10 * heads * seq * seq * HD,
            bytes_accessed=16 * seq * heads * HD,
            transcendentals=heads * seq * seq,
        ),
        name="attention_step",
    )(projected, projected, projected, down, down_t, qup, vup, cos, sin, grad_rows)


MESH = pl.DeviceIdType.MESH
CHUNKS = 8
OFFSETS = (0, 3, 1, 2)


class Place:
    def __init__(self):
        self.dp = lax.axis_index("dp")
        self.fs = lax.axis_index("fsdp")
        self.y = lax.axis_index("tensor")
        self.core = lax.rem(self.dp, 2)
        self.x = lax.div(self.dp, 2) * 2 + lax.rem(self.fs, 2)
        self.z = lax.div(self.fs, 2)

    def ring(self, core):
        first = self.x * (1 - core) + self.z * core
        second = self.z * (1 - core) + self.x * core
        return first, second

    def plane(self, core, a, b):
        first, second = self.ring(core)
        first = lax.rem(first + a, 4)
        second = lax.rem(second + b, 4)
        x = first * (1 - core) + second * core
        z = second * (1 - core) + first * core
        return lax.div(x, 2) * 2 + core, z * 2 + lax.rem(x, 2)

    def near(self, a, b):
        return (*self.plane(self.core, a, b), self.y)

    def along(self, c):
        return (self.dp, self.fs, lax.rem(self.y + c, 4))

    def partner(self):
        return (self.dp + 1 - 2 * self.core, self.fs, self.y)


def project_kernel(
    rows,
    tok_hbm,
    gain_ref,
    w_hbm,
    adapt_ref,
    proj_hbm,
    normed_hbm,
    down_ref,
    raw,
    scale_scr,
    x_buf,
    w_buf,
    acc,
    down_scr,
    tok_sem,
    own_sem,
    out_sem,
    w_send,
    w_recv,
    d_send,
    d_recv,
    x_send,
    x_recv,
):
    me = Place()
    shard = w_hbm.shape[0]
    half = shard // 2
    width = tok_hbm.shape[1]
    wide = width // CHUNKS
    cols = w_hbm.shape[1]
    parts = tok_sem.shape[0]
    part = rows // parts

    def tok_copy(i):
        piece = pl.ds(i * part, part)
        return pltpu.make_async_copy(tok_hbm.at[piece], raw.at[piece], tok_sem.at[i])

    for i in range(parts):
        tok_copy(i).start()

    def block(core, a, b):
        dp, fs = me.plane(core, a, b)
        return pl.multiple_of((dp * 8 + fs) * shard, shard)

    own = block(me.core, 0, 0)
    own_copy = pltpu.make_async_copy(w_hbm, w_buf.at[pl.ds(own, shard)], own_sem)
    own_copy.start()

    barrier = pltpu.get_barrier_semaphore()
    neighbours = (
        me.near(1, 0),
        me.near(3, 0),
        me.near(0, 1),
        me.near(0, 3),
        me.along(1),
        me.along(3),
        me.partner(),
    )
    for device in neighbours:
        pl.semaphore_signal(barrier, inc=1, device_id=device, device_id_type=MESH)
    pl.semaphore_wait(barrier, len(neighbours))

    sends = []

    def w_copy(a, b, device, kind, way, piece=None, source=None):
        start = block(me.core, a, b)
        size = shard
        if piece is not None:
            start, size = pl.multiple_of(start + piece * half, half), half
        dst = w_buf.at[pl.ds(start, size)]
        return pltpu.make_async_remote_copy(
            src_ref=dst if source is None else source,
            dst_ref=dst,
            send_sem=w_send.at[kind, way],
            recv_sem=w_recv.at[kind, way],
            device_id=device,
            device_id_type=MESH,
        )

    def w_start(*args, **kwargs):
        copy = w_copy(*args, **kwargs)
        copy.start()
        sends.append(copy)

    def d_copy(core, event, a, b, source=None):
        dst = w_buf.at[pl.ds(block(core, a, b), shard)]
        return pltpu.make_async_remote_copy(
            src_ref=dst if source is None else source,
            dst_ref=dst,
            send_sem=d_send.at[event],
            recv_sem=d_recv.at[event],
            device_id=me.partner(),
            device_id_type=MESH,
        )

    order = []

    def share(a, b, source=None):
        copy = d_copy(me.core, len(order), a, b, source)
        copy.start()
        sends.append(copy)
        order.append((a, b))

    w_start(0, 0, me.near(1, 0), 4, 0, source=w_hbm)
    w_start(0, 0, me.near(3, 0), 4, 1, source=w_hbm)
    w_start(0, 0, me.near(0, 1), 0, 0, source=w_hbm)
    w_start(0, 0, me.near(0, 3), 0, 1, source=w_hbm)
    share(0, 0, source=w_hbm)

    for i in range(parts):
        tok_copy(i).wait()

        @pl.loop(0, part // 16)
        def _(r):
            piece = pl.ds(pl.multiple_of(i * part + r * 16, 16), 16)
            squares = jnp.zeros((16, wide), jnp.float32)
            for c in range(CHUNKS):
                value = raw[piece, c * wide : (c + 1) * wide].astype(jnp.float32)
                squares = squares + value * value
            mean = jnp.sum(squares, axis=-1, keepdims=True) * (1.0 / width)
            scale_scr[piece, :] = jnp.broadcast_to(lax.rsqrt(mean + EPSILON), (16, 128))

    def x_copy(row_block, chunk, device, way):
        ref = x_buf.at[row_block, chunk]
        return pltpu.make_async_remote_copy(
            src_ref=ref,
            dst_ref=ref,
            send_sem=x_send.at[way, chunk],
            recv_sem=x_recv.at[way // 2 * 2 if way > 1 else way, chunk],
            device_id=device,
            device_id_type=MESH,
        )

    def normalize_chunk(c):
        lanes = slice(c * wide, (c + 1) * wide)

        @pl.loop(0, rows // 16)
        def _(r):
            piece = pl.ds(pl.multiple_of(r * 16, 16), 16)
            scale = scale_scr[piece, 0:1]
            value = raw[piece, lanes].astype(jnp.float32)
            x_buf[me.y, c, piece, :] = (value * scale * gain_ref[:, lanes]).astype(jnp.bfloat16)

    def x_start(row_block, chunk, device, way):
        copy = x_copy(row_block, chunk, device, way)
        copy.start()
        sends.append(copy)

    middle = CHUNKS // 2
    for c in range(middle):
        normalize_chunk(c)
        normalize_chunk(c + middle)
        x_start(me.y, c, me.along(1), 0)
        x_start(me.y, c + middle, me.along(3), 1)
    for c in range(middle):
        x_start(me.y, c + middle, me.along(1), 0)
        x_start(me.y, c, me.along(3), 1)

    acc[...] = jnp.zeros_like(acc)
    down_scr[...] = jnp.zeros_like(down_scr)

    def normed_copy(c):
        return pltpu.make_async_copy(x_buf.at[me.y, c], normed_hbm.at[c], out_sem.at[4 + c])

    for c in range(CHUNKS):
        normed_copy(c).start()

    def arrived(a, b, kind, way, piece=None):
        w_copy(a, b, me.near(0, 1), kind, way, piece).wait_recv()

    def spread(a, kind):
        w_start(a, 0, me.near(0, 1), kind, 0)
        w_start(a, 0, me.near(0, 3), kind, 1)

    own_copy.wait()
    arrived(3, 0, 4, 0)
    w_start(3, 0, me.near(1, 0), 4, 2, piece=0)
    spread(3, 1)
    share(3, 0)
    arrived(1, 0, 4, 1)
    w_start(1, 0, me.near(3, 0), 4, 3, piece=1)
    spread(1, 2)
    share(1, 0)
    for kind, a in enumerate(OFFSETS):
        if kind == 3:
            arrived(2, 0, 4, 2, piece=0)
            arrived(2, 0, 4, 3, piece=1)
            spread(2, 3)
            share(2, 0)
        arrived(a, 3, kind, 0)
        w_start(a, 3, me.near(0, 1), kind, 2, piece=0)
        share(a, 3)
        arrived(a, 1, kind, 1)
        w_start(a, 1, me.near(0, 3), kind, 3, piece=1)
        share(a, 1)
        if kind > 0:
            before = OFFSETS[kind - 1]
            arrived(before, 2, kind - 1, 2, piece=0)
            arrived(before, 2, kind - 1, 3, piece=1)
            share(before, 2)
    arrived(OFFSETS[3], 2, 3, 2, piece=0)
    arrived(OFFSETS[3], 2, 3, 3, piece=1)
    share(OFFSETS[3], 2)

    minus = lax.rem(me.y + 3, 4)
    plus = lax.rem(me.y + 1, 4)
    far = lax.rem(me.y + 2, 4)
    for c in range(middle):
        x_copy(minus, c, me.along(1), 0).wait_recv()
        x_start(minus, c, me.along(1), 2)
        x_copy(plus, c + middle, me.along(1), 1).wait_recv()
        x_start(plus, c + middle, me.along(3), 2)

    for event, (a, b) in enumerate(order):
        d_copy(1 - me.core, event, a, b).wait_recv()

    def multiply(row_block, chunk):
        value = x_buf[row_block, chunk]
        lines = pl.ds(pl.multiple_of(row_block * rows, rows), rows)
        depth = pl.ds(pl.multiple_of(chunk * wide, wide), wide)
        for n in range(cols // 256):
            lanes = slice(n * 256, (n + 1) * 256)
            acc[lines, lanes] += dot_nn(value, w_buf[depth, lanes])
        down_scr[lines, :] += dot_nt(value, adapt_ref[:, depth])

    def result_copy(i, row_block):
        lines = pl.ds(pl.multiple_of(row_block * rows, rows), rows)
        return pltpu.make_async_copy(acc.at[lines], proj_hbm.at[lines], out_sem.at[i])

    @pl.loop(0, CHUNKS)
    def _(c):
        multiply(me.y, c)

    result_copy(0, me.y).start()

    @pl.loop(0, CHUNKS)
    def _(c):
        @pl.when(c >= middle)
        def _():
            x_copy(minus, c, me.along(1), 0).wait_recv()

        multiply(minus, c)

    result_copy(1, minus).start()

    @pl.loop(0, CHUNKS)
    def _(c):
        @pl.when(c < middle)
        def _():
            x_copy(plus, c, me.along(1), 1).wait_recv()

        multiply(plus, c)

    result_copy(2, plus).start()

    @pl.loop(0, middle)
    def _(c):
        x_copy(far, c, me.along(1), 2).wait_recv()
        multiply(far, c)
        x_copy(far, c + middle, me.along(1), 2).wait_recv()
        multiply(far, c + middle)

    result_copy(3, far).start()
    down_ref[...] = down_scr[...].astype(jnp.bfloat16)
    for copy in sends:
        copy.wait_send()
    for c in range(CHUNKS):
        normed_copy(c).wait()
    for i, row_block in enumerate((me.y, minus, plus, far)):
        result_copy(i, row_block).wait()


def gather_project(tokens, gain, w_qkv, adapters_t):
    rows, width = tokens.shape
    shard, cols = w_qkv.shape
    seq = 4 * rows
    wide = width // CHUNKS
    anywhere = pl.BlockSpec(memory_space=pl.ANY)
    inside = pl.BlockSpec(memory_space=pltpu.VMEM)
    dma = pltpu.SemaphoreType.DMA
    return pl.pallas_call(
        functools.partial(project_kernel, rows),
        in_specs=[anywhere, inside, anywhere, inside],
        out_specs=[anywhere, anywhere, inside],
        out_shape=[
            jax.ShapeDtypeStruct((seq, cols), jnp.float32),
            jax.ShapeDtypeStruct((CHUNKS, rows, wide), jnp.bfloat16),
            jax.ShapeDtypeStruct((seq, 2 * RANK), jnp.bfloat16),
        ],
        scratch_shapes=[
            pltpu.VMEM((rows, width), jnp.bfloat16),
            pltpu.VMEM((rows, 128), jnp.float32),
            pltpu.VMEM((4, CHUNKS, rows, wide), jnp.bfloat16),
            pltpu.VMEM((width, cols), jnp.bfloat16),
            pltpu.VMEM((seq, cols), jnp.float32),
            pltpu.VMEM((seq, 2 * RANK), jnp.float32),
            dma((4,)),
            dma(()),
            dma((4 + CHUNKS,)),
            dma((5, 4)),
            dma((5, 4)),
            dma((16,)),
            dma((16,)),
            dma((3, CHUNKS)),
            dma((3, CHUNKS)),
        ],
        compiler_params=pltpu.CompilerParams(
            collective_id=1, has_side_effects=True, vmem_limit_bytes=56 << 20
        ),
        cost_estimate=pl.CostEstimate(
            flops=2 * seq * width * cols, bytes_accessed=20 * 1000 * 1000, transcendentals=0
        ),
        name="gather_project",
    )(tokens, gain.reshape(1, width), w_qkv, adapters_t)


def local(tokens, norm_gain, w_qkv, a_query, query_up_adapter, a_value, value_up_adapter, out_grad):
    projected, normed, down = gather_project(
        tokens[0], norm_gain, w_qkv, jnp.concatenate([a_query.T, a_value.T], 0)
    )
    seq = projected.shape[0]
    grad_rows = lax.all_to_all(out_grad[0], "tensor", split_axis=1, concat_axis=0, tiled=True)
    cos, sin = rotary_tables(seq)
    attended, gbq, gbv, mid_t = attention(
        projected, down, down.T, query_up_adapter, value_up_adapter, cos, sin, grad_rows
    )
    out_rows = lax.all_to_all(attended, "tensor", split_axis=0, concat_axis=1, tiled=True)
    groups = lax.axis_size("tensor")
    own = seq // groups
    mid_split = mid_t.reshape(2 * RANK, groups, own).transpose(1, 0, 2)
    mid = (
        lax.all_to_all(mid_split, "tensor", split_axis=0, concat_axis=0, tiled=True)
        .sum(axis=0)
        .astype(jnp.bfloat16)
    )
    grad_a = ADAPTER_SCALE * jnp.einsum("rp,cpw->rcw", mid, normed, preferred_element_type=jnp.float32)
    grad_a = grad_a.reshape(2 * RANK, -1)
    up = jnp.concatenate([gbq, gbv], 1)
    slots = jnp.zeros((groups, *up.shape), jnp.float32)
    slots = lax.dynamic_update_index_in_dim(slots, up, lax.axis_index("tensor"), 0)
    grad_a, slots = lax.psum((grad_a, slots), ALL)
    up = lax.dynamic_index_in_dim(slots, lax.axis_index("tensor"), 0, keepdims=False)
    return (
        out_rows[None],
        grad_a[:RANK].T,
        up[:, : gbq.shape[1]],
        grad_a[RANK:].T,
        up[:, gbq.shape[1] :],
    )


def solution(mesh):
    return jax.shard_map(
        local,
        mesh=mesh,
        in_specs=(
            P(("dp", "fsdp"), "tensor", None),
            P(),
            P(("dp", "fsdp"), "tensor"),
            P(),
            P(None, "tensor"),
            P(),
            P(None, "tensor"),
            P(("dp", "fsdp"), "tensor", None),
        ),
        out_specs=(
            P(("dp", "fsdp"), "tensor", None),
            P(),
            P(None, "tensor"),
            P(),
            P(None, "tensor"),
        ),
        check_vma=False,
    )
```

```python
import functools
import math

import jax
import jax.numpy as jnp
import numpy as np
from jax import lax
from jax.experimental import pallas as pl
from jax.experimental.pallas import tpu as pltpu
from jax.sharding import PartitionSpec as P

HD = 128
QUERY_PER_KV = 8
RANK = 16
QB = 256

EPSILON = 1e-05
ADAPTER_SCALE = 2.0
ROPE_BASE = 500000.0
SCORE_SCALE = 1.0 / math.sqrt(HD)
LOG2E = 1.4426950408889634


def rotary_tables(sequence_length):
    half_dim = HD // 2
    inv_freq = ROPE_BASE ** (-np.arange(half_dim) / half_dim)
    angles = np.arange(sequence_length)[:, None] * inv_freq
    cosine, sine = np.cos(angles), np.sin(angles)
    return (
        np.concatenate([cosine, cosine], 1).astype(np.float32),
        np.concatenate([-sine, sine], 1).astype(np.float32),
    )


def dot_nt(a, b):
    return lax.dot_general(a, b, (((1,), (1,)), ((), ())), preferred_element_type=jnp.float32)


def dot_nn(a, b):
    return jnp.dot(a, b, preferred_element_type=jnp.float32)


def rotate(x, cos, sin):
    return x * cos + pltpu.roll(x, HD // 2, 1) * sin


MESH = pl.DeviceIdType.MESH
CHUNKS = 8
OFFSETS = (0, 3, 1, 2)


class Place:
    def __init__(self):
        self.dp = lax.axis_index("dp")
        self.fs = lax.axis_index("fsdp")
        self.y = lax.axis_index("tensor")
        self.core = lax.rem(self.dp, 2)
        self.x = lax.div(self.dp, 2) * 2 + lax.rem(self.fs, 2)
        self.z = lax.div(self.fs, 2)

    def ring(self, core):
        first = self.x * (1 - core) + self.z * core
        second = self.z * (1 - core) + self.x * core
        return first, second

    def plane(self, core, a, b):
        first, second = self.ring(core)
        first = lax.rem(first + a, 4)
        second = lax.rem(second + b, 4)
        x = first * (1 - core) + second * core
        z = second * (1 - core) + first * core
        return lax.div(x, 2) * 2 + core, z * 2 + lax.rem(x, 2)

    def near(self, a, b):
        return (*self.plane(self.core, a, b), self.y)

    def along(self, c):
        return (self.dp, self.fs, lax.rem(self.y + c, 4))

    def partner(self):
        return (self.dp + 1 - 2 * self.core, self.fs, self.y)


def project_kernel(
    rows,
    tok_hbm,
    gain_ref,
    w_hbm,
    adapt_ref,
    proj_hbm,
    normed_hbm,
    down_ref,
    raw,
    scale_scr,
    x_buf,
    w_buf,
    acc,
    down_scr,
    tok_sem,
    own_sem,
    out_sem,
    w_send,
    w_recv,
    d_send,
    d_recv,
    x_send,
    x_recv,
):
    me = Place()
    shard = w_hbm.shape[0]
    half = shard // 2
    width = tok_hbm.shape[1]
    wide = width // CHUNKS
    cols = w_hbm.shape[1]
    parts = tok_sem.shape[0]
    part = rows // parts

    def tok_copy(i):
        piece = pl.ds(i * part, part)
        return pltpu.make_async_copy(tok_hbm.at[piece], raw.at[piece], tok_sem.at[i])

    for i in range(parts):
        tok_copy(i).start()

    def block(core, a, b):
        dp, fs = me.plane(core, a, b)
        return pl.multiple_of((dp * 8 + fs) * shard, shard)

    own = block(me.core, 0, 0)
    own_copy = pltpu.make_async_copy(w_hbm, w_buf.at[pl.ds(own, shard)], own_sem)
    own_copy.start()

    barrier = pltpu.get_barrier_semaphore()
    neighbours = (
        me.near(1, 0),
        me.near(3, 0),
        me.near(0, 1),
        me.near(0, 3),
        me.along(1),
        me.along(3),
        me.partner(),
    )
    for device in neighbours:
        pl.semaphore_signal(barrier, inc=1, device_id=device, device_id_type=MESH)
    pl.semaphore_wait(barrier, len(neighbours))

    sends = []

    def w_copy(a, b, device, kind, way, piece=None, source=None):
        start = block(me.core, a, b)
        size = shard
        if piece is not None:
            start, size = pl.multiple_of(start + piece * half, half), half
        dst = w_buf.at[pl.ds(start, size)]
        return pltpu.make_async_remote_copy(
            src_ref=dst if source is None else source,
            dst_ref=dst,
            send_sem=w_send.at[kind, way],
            recv_sem=w_recv.at[kind, way],
            device_id=device,
            device_id_type=MESH,
        )

    def w_start(*args, **kwargs):
        copy = w_copy(*args, **kwargs)
        copy.start()
        sends.append(copy)

    def d_copy(core, event, a, b, source=None):
        dst = w_buf.at[pl.ds(block(core, a, b), shard)]
        return pltpu.make_async_remote_copy(
            src_ref=dst if source is None else source,
            dst_ref=dst,
            send_sem=d_send.at[event],
            recv_sem=d_recv.at[event],
            device_id=me.partner(),
            device_id_type=MESH,
        )

    order = []

    def share(a, b, source=None):
        copy = d_copy(me.core, len(order), a, b, source)
        copy.start()
        sends.append(copy)
        order.append((a, b))

    w_start(0, 0, me.near(1, 0), 4, 0, source=w_hbm)
    w_start(0, 0, me.near(3, 0), 4, 1, source=w_hbm)
    w_start(0, 0, me.near(0, 1), 0, 0, source=w_hbm)
    w_start(0, 0, me.near(0, 3), 0, 1, source=w_hbm)
    share(0, 0, source=w_hbm)

    for i in range(parts):
        tok_copy(i).wait()

        @pl.loop(0, part // 16)
        def _(r):
            piece = pl.ds(pl.multiple_of(i * part + r * 16, 16), 16)
            squares = jnp.zeros((16, wide), jnp.float32)
            for c in range(CHUNKS):
                value = raw[piece, c * wide : (c + 1) * wide].astype(jnp.float32)
                squares = squares + value * value
            mean = jnp.sum(squares, axis=-1, keepdims=True) * (1.0 / width)
            scale_scr[piece, :] = jnp.broadcast_to(lax.rsqrt(mean + EPSILON), (16, 128))

    def x_copy(row_block, chunk, device, way):
        ref = x_buf.at[row_block, chunk]
        return pltpu.make_async_remote_copy(
            src_ref=ref,
            dst_ref=ref,
            send_sem=x_send.at[way, chunk],
            recv_sem=x_recv.at[way // 2 * 2 if way > 1 else way, chunk],
            device_id=device,
            device_id_type=MESH,
        )

    def normalize_chunk(c):
        lanes = slice(c * wide, (c + 1) * wide)

        @pl.loop(0, rows // 16)
        def _(r):
            piece = pl.ds(pl.multiple_of(r * 16, 16), 16)
            scale = scale_scr[piece, 0:1]
            value = raw[piece, lanes].astype(jnp.float32)
            x_buf[me.y, c, piece, :] = (value * scale * gain_ref[:, lanes]).astype(jnp.bfloat16)

    def x_start(row_block, chunk, device, way):
        copy = x_copy(row_block, chunk, device, way)
        copy.start()
        sends.append(copy)

    middle = CHUNKS // 2
    for c in range(middle):
        normalize_chunk(c)
        normalize_chunk(c + middle)
        x_start(me.y, c, me.along(1), 0)
        x_start(me.y, c + middle, me.along(3), 1)
    for c in range(middle):
        x_start(me.y, c + middle, me.along(1), 0)
        x_start(me.y, c, me.along(3), 1)

    acc[...] = jnp.zeros_like(acc)
    down_scr[...] = jnp.zeros_like(down_scr)

    def normed_copy(c):
        return pltpu.make_async_copy(x_buf.at[me.y, c], normed_hbm.at[c], out_sem.at[4 + c])

    for c in range(CHUNKS):
        normed_copy(c).start()

    def arrived(a, b, kind, way, piece=None):
        w_copy(a, b, me.near(0, 1), kind, way, piece).wait_recv()

    def spread(a, kind):
        w_start(a, 0, me.near(0, 1), kind, 0)
        w_start(a, 0, me.near(0, 3), kind, 1)

    own_copy.wait()
    arrived(3, 0, 4, 0)
    w_start(3, 0, me.near(1, 0), 4, 2, piece=0)
    spread(3, 1)
    share(3, 0)
    arrived(1, 0, 4, 1)
    w_start(1, 0, me.near(3, 0), 4, 3, piece=1)
    spread(1, 2)
    share(1, 0)
    for kind, a in enumerate(OFFSETS):
        if kind == 3:
            arrived(2, 0, 4, 2, piece=0)
            arrived(2, 0, 4, 3, piece=1)
            spread(2, 3)
            share(2, 0)
        arrived(a, 3, kind, 0)
        w_start(a, 3, me.near(0, 1), kind, 2, piece=0)
        share(a, 3)
        arrived(a, 1, kind, 1)
        w_start(a, 1, me.near(0, 3), kind, 3, piece=1)
        share(a, 1)
        if kind > 0:
            before = OFFSETS[kind - 1]
            arrived(before, 2, kind - 1, 2, piece=0)
            arrived(before, 2, kind - 1, 3, piece=1)
            share(before, 2)
    arrived(OFFSETS[3], 2, 3, 2, piece=0)
    arrived(OFFSETS[3], 2, 3, 3, piece=1)
    share(OFFSETS[3], 2)

    minus = lax.rem(me.y + 3, 4)
    plus = lax.rem(me.y + 1, 4)
    far = lax.rem(me.y + 2, 4)
    for c in range(middle):
        x_copy(minus, c, me.along(1), 0).wait_recv()
        x_start(minus, c, me.along(1), 2)
        x_copy(plus, c + middle, me.along(1), 1).wait_recv()
        x_start(plus, c + middle, me.along(3), 2)

    for event, (a, b) in enumerate(order):
        d_copy(1 - me.core, event, a, b).wait_recv()

    def multiply(row_block, chunk):
        value = x_buf[row_block, chunk]
        lines = pl.ds(pl.multiple_of(row_block * rows, rows), rows)
        depth = pl.ds(pl.multiple_of(chunk * wide, wide), wide)
        for n in range(cols // 256):
            lanes = slice(n * 256, (n + 1) * 256)
            acc[lines, lanes] += dot_nn(value, w_buf[depth, lanes])
        down_scr[lines, :] += dot_nt(value, adapt_ref[:, depth])

    def result_copy(i, row_block):
        lines = pl.ds(pl.multiple_of(row_block * rows, rows), rows)
        return pltpu.make_async_copy(acc.at[lines], proj_hbm.at[lines], out_sem.at[i])

    @pl.loop(0, CHUNKS)
    def _(c):
        multiply(me.y, c)

    result_copy(0, me.y).start()

    @pl.loop(0, CHUNKS)
    def _(c):
        @pl.when(c >= middle)
        def _():
            x_copy(minus, c, me.along(1), 0).wait_recv()

        multiply(minus, c)

    result_copy(1, minus).start()

    @pl.loop(0, CHUNKS)
    def _(c):
        @pl.when(c < middle)
        def _():
            x_copy(plus, c, me.along(1), 1).wait_recv()

        multiply(plus, c)

    result_copy(2, plus).start()

    @pl.loop(0, middle)
    def _(c):
        x_copy(far, c, me.along(1), 2).wait_recv()
        multiply(far, c)
        x_copy(far, c + middle, me.along(1), 2).wait_recv()
        multiply(far, c + middle)

    result_copy(3, far).start()
    down_ref[...] = down_scr[...].astype(jnp.bfloat16)
    for copy in sends:
        copy.wait_send()
    for c in range(CHUNKS):
        normed_copy(c).wait()
    for i, row_block in enumerate((me.y, minus, plus, far)):
        result_copy(i, row_block).wait()


def gather_project(tokens, gain, w_qkv, adapters_t):
    rows, width = tokens.shape
    shard, cols = w_qkv.shape
    seq = 4 * rows
    wide = width // CHUNKS
    anywhere = pl.BlockSpec(memory_space=pl.ANY)
    inside = pl.BlockSpec(memory_space=pltpu.VMEM)
    dma = pltpu.SemaphoreType.DMA
    return pl.pallas_call(
        functools.partial(project_kernel, rows),
        in_specs=[anywhere, inside, anywhere, inside],
        out_specs=[anywhere, anywhere, inside],
        out_shape=[
            jax.ShapeDtypeStruct((seq, cols), jnp.float32),
            jax.ShapeDtypeStruct((CHUNKS, rows, wide), jnp.bfloat16),
            jax.ShapeDtypeStruct((seq, 2 * RANK), jnp.bfloat16),
        ],
        scratch_shapes=[
            pltpu.VMEM((rows, width), jnp.bfloat16),
            pltpu.VMEM((rows, 128), jnp.float32),
            pltpu.VMEM((4, CHUNKS, rows, wide), jnp.bfloat16),
            pltpu.VMEM((width, cols), jnp.bfloat16),
            pltpu.VMEM((seq, cols), jnp.float32),
            pltpu.VMEM((seq, 2 * RANK), jnp.float32),
            dma((4,)),
            dma(()),
            dma((4 + CHUNKS,)),
            dma((5, 4)),
            dma((5, 4)),
            dma((16,)),
            dma((16,)),
            dma((3, CHUNKS)),
            dma((3, CHUNKS)),
        ],
        compiler_params=pltpu.CompilerParams(
            collective_id=1, has_side_effects=True, vmem_limit_bytes=56 << 20
        ),
        cost_estimate=pl.CostEstimate(
            flops=2 * seq * width * cols, bytes_accessed=20 * 1000 * 1000, transcendentals=0
        ),
        name="gather_project",
    )(tokens, gain.reshape(1, width), w_qkv, adapters_t)


CHIPS = 64
PLANE = 16


def attention_kernel(
    seq,
    proj_ref,
    key_ref,
    value_ref,
    down_ref,
    qup_ref,
    vup_ref,
    cos_ref,
    sin_ref,
    grad_hbm,
    normed_hbm,
    out_hbm,
    ga_q_hbm,
    ga_v_hbm,
    gb_q_hbm,
    gb_v_hbm,
    k_scr,
    v_scr,
    dv_scr,
    q_scr,
    dq_scr,
    down_t,
    mid_scr,
    mid_recv,
    stage,
    g_buf,
    o_buf,
    n_buf,
    part,
    part_recv,
    total,
    rs_recv,
    final,
    res,
    up_part,
    up_recv,
    up_total,
    up_rs,
    up_final,
    up_res,
    local_sem,
    own_sem,
    o_own_sem,
    g_send,
    g_recv,
    o_send,
    o_recv,
    m_send,
    m_recv,
    c_send,
    c_recv,
    r_send,
    r_recv,
):
    me = Place()
    head = pl.program_id(0)
    heads = QUERY_PER_KV
    rows = seq // 4
    group = heads * HD
    blocks = seq // QB
    plane = lax.div(me.dp, 2) * 8 + me.fs
    chip = plane * 4 + me.y

    def lines(block):
        return pl.ds(pl.multiple_of(block * rows, rows), rows)

    def columns(block, h):
        return pl.ds(pl.multiple_of(block * group + h * HD, HD), HD)

    def remote(src, dst, send, recv, device):
        return pltpu.make_async_remote_copy(
            src_ref=src,
            dst_ref=dst,
            send_sem=send,
            recv_sem=recv,
            device_id=device,
            device_id_type=MESH,
        )

    def of_chip(index):
        at = lax.div(index, 4)
        return (lax.div(at, 8) * 2 + me.core, lax.rem(at, 8), lax.rem(index, 4))

    stage_copy = pltpu.make_async_copy(grad_hbm, stage, local_sem.at[0])
    normed_copy = pltpu.make_async_copy(normed_hbm, n_buf, local_sem.at[1])

    def own_grad(h):
        return pltpu.make_async_copy(
            grad_hbm.at[:, columns(me.y, h)], g_buf.at[h, lines(me.y)], own_sem.at[h]
        )

    def grad_copy(h, c):
        to = lax.rem(me.y + c, 4)
        return remote(
            stage.at[:, columns(to, h)],
            g_buf.at[h, lines(me.y)],
            g_send.at[h, c - 1],
            g_recv.at[h, c - 1],
            me.along(c),
        )

    def grad_arrival(h, c):
        ref = g_buf.at[h, lines(lax.rem(me.y + 4 - c, 4))]
        return remote(ref, ref, g_send.at[h, c - 1], g_recv.at[h, c - 1], me.along(c))

    def own_out(h):
        return pltpu.make_async_copy(
            o_buf.at[h, lines(me.y)], out_hbm.at[:, columns(me.y, h)], o_own_sem.at[h]
        )

    def out_copy(h, c):
        to = lax.rem(me.y + c, 4)
        return remote(
            o_buf.at[h, lines(to)],
            out_hbm.at[:, columns(me.y, h)],
            o_send.at[h, c - 1],
            o_recv.at[h, c - 1],
            me.along(c),
        )

    def out_arrival(h, c):
        ref = out_hbm.at[:, columns(lax.rem(me.y + 4 - c, 4), h)]
        return remote(ref, ref, o_send.at[h, c - 1], o_recv.at[h, c - 1], me.along(c))

    @pl.when(head == 0)
    def _():
        stage_copy.start()
        barrier = pltpu.get_barrier_semaphore()

        @pl.loop(1, CHIPS)
        def _(o):
            pl.semaphore_signal(
                barrier, inc=1, device_id=of_chip(lax.rem(chip + o, CHIPS)), device_id_type=MESH
            )

        pl.semaphore_signal(barrier, inc=1, device_id=me.partner(), device_id_type=MESH)

        @pl.loop(0, heads)
        def _(h):
            own_grad(h).start()

        normed_copy.start()
        stage_copy.wait()
        pl.semaphore_wait(barrier, CHIPS)

        @pl.loop(0, heads)
        def _(h):
            for c in (1, 3, 2):
                grad_copy(h, c).start()

        k_scr[...] = rotate(
            key_ref[...].astype(jnp.bfloat16).astype(jnp.float32), cos_ref[...], sin_ref[...]
        ).astype(jnp.bfloat16)
        v_scr[...] = (
            value_ref[...] + ADAPTER_SCALE * dot_nn(down_ref[:, RANK:], vup_ref[...])
        ).astype(jnp.bfloat16)
        down_t[...] = down_ref[...].astype(jnp.float32).T.astype(jnp.bfloat16)
        dv_scr[...] = jnp.zeros_like(dv_scr)
        mid_scr[...] = jnp.zeros_like(mid_scr)
        up_part[...] = jnp.zeros_like(up_part)

    queries = (proj_ref[...] + ADAPTER_SCALE * dot_nn(down_ref[:, :RANK], qup_ref[...])).astype(
        jnp.bfloat16
    )
    q_scr[...] = rotate(queries.astype(jnp.float32), cos_ref[...], sin_ref[...]).astype(
        jnp.bfloat16
    )
    own_grad(head).wait()
    for c in (1, 3, 2):
        grad_arrival(head, c).wait_recv()

    row = lax.broadcasted_iota(jnp.int32, (QB, QB), 0)
    col = lax.broadcasted_iota(jnp.int32, (QB, QB), 1)
    causal = row >= col
    factor = SCORE_SCALE * LOG2E
    for i in range(blocks):
        own_rows = slice(i * QB, (i + 1) * QB)
        q = q_scr[own_rows, :]
        grad = g_buf[head, own_rows, :]
        grad_t = grad.T
        scores = []
        for j in range(i + 1):
            s = dot_nt(q, k_scr[j * QB : (j + 1) * QB, :])
            if j == i:
                s = jnp.where(causal, s, -1e30)
            scores.append(s)
        top = functools.reduce(jnp.maximum, scores)
        top = jnp.max(top, axis=-1, keepdims=True) * factor
        weights = [jnp.exp2(s * factor - top) for s in scores]
        whole = jnp.sum(functools.reduce(jnp.add, weights), axis=-1, keepdims=True)
        inverse = 1.0 / whole
        probs = [w * inverse for w in weights]
        rounded = [p.astype(jnp.bfloat16) for p in probs]
        attended = functools.reduce(
            jnp.add, [dot_nn(rounded[j], v_scr[j * QB : (j + 1) * QB, :]) for j in range(i + 1)]
        )
        o_buf[head, own_rows, :] = attended.astype(jnp.bfloat16)
        prods = []
        for j in range(i + 1):
            keys = slice(j * QB, (j + 1) * QB)
            dp = dot_nt(grad, v_scr[keys, :])
            prods.append(probs[j] * dp)
            dv_scr[:, keys] += dot_nn(grad_t, rounded[j])
        inner = jnp.sum(functools.reduce(jnp.add, prods), axis=-1, keepdims=True)
        ds = [(prods[j] - probs[j] * inner).astype(jnp.bfloat16) for j in range(i + 1)]
        dq = functools.reduce(
            jnp.add, [dot_nn(ds[j], k_scr[j * QB : (j + 1) * QB, :]) for j in range(i + 1)]
        )
        dq = (dq * SCORE_SCALE).astype(jnp.bfloat16).astype(jnp.float32)
        dq_scr[own_rows, :] = rotate(dq, cos_ref[own_rows, :], -sin_ref[own_rows, :]).astype(
            jnp.bfloat16
        )

    own_out(head).start()
    for c in (1, 3, 2):
        out_copy(head, c).start()
    up = dot_nn(down_t[:RANK, :], dq_scr[...])
    up_part[0, head] = up[:8]
    up_part[1, head] = up[8:]
    for b in range(4):
        mid_scr[b, :RANK, :] += dot_nt(qup_ref[...], dq_scr[b * rows : (b + 1) * rows, :])

    @pl.when(head == heads - 1)
    def _():
        dv = dv_scr[...].T.astype(jnp.bfloat16)
        for b in range(4):
            mid_scr[b, RANK:, :] = dot_nt(vup_ref[...], dv[b * rows : (b + 1) * rows])
        up = dot_nn(down_t[RANK:, :], dv)
        up_part[0, heads] = up[:8]
        up_part[1, heads] = up[8:]

        def mid_copy(c):
            return remote(
                mid_scr.at[lax.rem(me.y + c, 4)],
                mid_recv.at[c - 1],
                m_send.at[c - 1],
                m_recv.at[c - 1],
                me.along(c),
            )

        for c in (1, 3, 2):
            mid_copy(c).start()
        up_swap = remote(
            up_part.at[1 - me.core], up_recv, c_send.at[0], c_recv.at[0], me.partner()
        )
        up_swap.start()
        normed_copy.wait()
        for c in (1, 3, 2):
            mid_copy(c).wait_recv()
        mid = (mid_scr[me.y] + mid_recv[0] + mid_recv[1] + mid_recv[2]).astype(jnp.bfloat16)

        def partial(half):
            @pl.loop(0, 4)
            def _(n):
                made = dot_nn(mid, n_buf[half * 4 + n])
                for r in range(4):
                    for k in range(4):
                        part[half * CHIPS + r * 16 + n * 4 + k] = made[
                            r * 8 : (r + 1) * 8, k * 256 : (k + 1) * 256
                        ]

        def of_half(half):
            return pl.ds(pl.multiple_of(half * CHIPS, CHIPS), CHIPS)

        partial(1 - me.core)
        swap = remote(
            part.at[of_half(1 - me.core)], part_recv, c_send.at[1], c_recv.at[1], me.partner()
        )
        swap.start()
        partial(me.core)
        up_swap.wait_recv()
        up_total[...] = up_part[me.core] + up_recv[...]
        swap.wait_recv()

        @pl.loop(0, CHIPS // 8)
        def _(n):
            piece = pl.ds(pl.multiple_of(n * 8, 8), 8)
            mine = pl.ds(pl.multiple_of(me.core * CHIPS + n * 8, 8), 8)
            total[piece] = part[mine] + part_recv[piece]

        @pl.loop(1, PLANE)
        def _(o):
            to = lax.rem(plane + o, PLANE)
            remote(
                up_total.at[to], up_rs.at[o - 1], r_send.at[1], r_recv.at[1], of_chip(to * 4 + me.y)
            ).start()

        @pl.loop(1, CHIPS)
        def _(o):
            to = lax.rem(chip + o, CHIPS)
            remote(
                total.at[to], rs_recv.at[o - 1], r_send.at[0], r_recv.at[0], of_chip(to)
            ).start()

        up_many = remote(up_rs, up_rs, r_send.at[1], r_recv.at[1], me.partner())
        many = remote(rs_recv, rs_recv, r_send.at[0], r_recv.at[0], me.partner())
        up_many.wait_recv()
        up_sum = lax.fori_loop(
            0, PLANE - 1, lambda o, value: value + up_rs[o], up_total[plane], unroll=True
        )
        up_final[...] = ADAPTER_SCALE * up_sum
        many.wait_recv()
        summed = lax.fori_loop(0, CHIPS - 1, lambda o, value: value + rs_recv[o], total[chip])
        final[...] = ADAPTER_SCALE * summed

        def place(at):
            r = pl.multiple_of(lax.div(at, 16) * 8, 8)
            k = pl.multiple_of(me.core * 4096 + lax.rem(at, 16) * 256, 256)
            return res.at[pl.ds(r, 8), pl.ds(k, 256)]

        def up_place(at):
            return up_res.at[me.core, :, pl.ds(pl.multiple_of(at * HD, HD), HD)]

        @pl.loop(1, PLANE)
        def _(o):
            to = lax.rem(plane + o, PLANE)
            remote(
                up_final, up_place(plane), r_send.at[3], r_recv.at[3], of_chip(to * 4 + me.y)
            ).start()

        @pl.loop(1, CHIPS)
        def _(o):
            to = lax.rem(chip + o, CHIPS)
            remote(final, place(chip), r_send.at[2], r_recv.at[2], of_chip(to)).start()

        r = pl.multiple_of(lax.div(chip, 16) * 8, 8)
        k = pl.multiple_of(me.core * 4096 + lax.rem(chip, 16) * 256, 256)
        res[pl.ds(r, 8), pl.ds(k, 256)] = final[...]
        up_res[me.core, :, pl.ds(pl.multiple_of(plane * HD, HD), HD)] = up_final[...]
        up_all = remote(up_rs, up_rs, r_send.at[3], r_recv.at[3], me.partner())
        all_of = remote(rs_recv, rs_recv, r_send.at[2], r_recv.at[2], me.partner())
        up_all.wait_recv()
        up_half = remote(
            up_res.at[me.core], up_res.at[me.core], c_send.at[2], c_recv.at[2], me.partner()
        )
        up_half.start()
        all_of.wait_recv()
        kept = res.at[:, pl.ds(pl.multiple_of(me.core * 4096, 4096), 4096)]
        other = res.at[:, pl.ds(pl.multiple_of((1 - me.core) * 4096, 4096), 4096)]
        half = remote(kept, kept, c_send.at[3], c_recv.at[3], me.partner())
        half.start()
        up_other = up_res.at[1 - me.core]
        remote(up_other, up_other, c_send.at[2], c_recv.at[2], me.partner()).wait_recv()
        remote(other, other, c_send.at[3], c_recv.at[3], me.partner()).wait_recv()
        writes = [
            pltpu.make_async_copy(res.at[pl.ds(0, RANK)], ga_q_hbm, local_sem.at[2]),
            pltpu.make_async_copy(res.at[pl.ds(RANK, RANK)], ga_v_hbm, local_sem.at[3]),
        ]
        for b in range(2):
            writes.append(
                pltpu.make_async_copy(
                    up_res.at[b, :, pl.ds(0, group)],
                    gb_q_hbm.at[pl.ds(8 * b, 8)],
                    local_sem.at[4 + b],
                )
            )
            writes.append(
                pltpu.make_async_copy(
                    up_res.at[b, :, pl.ds(group, HD)],
                    gb_v_hbm.at[pl.ds(8 * b, 8)],
                    local_sem.at[6 + b],
                )
            )
        for copy in writes:
            copy.start()

        @pl.loop(0, heads)
        def _(h):
            own_out(h).wait()
            for c in (1, 3, 2):
                grad_copy(h, c).wait_send()
                out_copy(h, c).wait_send()
                out_arrival(h, c).wait_recv()

        for c in (1, 3, 2):
            mid_copy(c).wait_send()
        for copy in (up_swap, swap, many, up_many, all_of, up_all, up_half, half):
            copy.wait_send()
        for copy in writes:
            copy.wait()


def attention(projected, down, qup, vup, cos, sin, out_grad, normed):
    seq = projected.shape[0]
    heads = QUERY_PER_KV
    rows = seq // 4
    width = normed.shape[0] * normed.shape[2]

    def whole(shape):
        return pl.BlockSpec(shape, lambda h: (0, 0))

    anywhere = pl.BlockSpec(memory_space=pl.ANY)
    column = lambda h: (0, h)
    dma = pltpu.SemaphoreType.DMA
    f32, bf16 = jnp.float32, jnp.bfloat16
    return pl.pallas_call(
        functools.partial(attention_kernel, seq),
        grid=(heads,),
        in_specs=[
            pl.BlockSpec((seq, HD), column),
            pl.BlockSpec((seq, HD), lambda h: (0, heads)),
            pl.BlockSpec((seq, HD), lambda h: (0, heads + 1)),
            whole((seq, 2 * RANK)),
            pl.BlockSpec((RANK, HD), column),
            whole((RANK, HD)),
            whole((seq, HD)),
            whole((seq, HD)),
            anywhere,
            anywhere,
        ],
        out_specs=[anywhere] * 5,
        out_shape=[
            jax.ShapeDtypeStruct((rows, 4 * heads * HD), bf16),
            jax.ShapeDtypeStruct((RANK, width), f32),
            jax.ShapeDtypeStruct((RANK, width), f32),
            jax.ShapeDtypeStruct((RANK, heads * HD), f32),
            jax.ShapeDtypeStruct((RANK, HD), f32),
        ],
        scratch_shapes=[
            pltpu.VMEM((seq, HD), bf16),
            pltpu.VMEM((seq, HD), bf16),
            pltpu.VMEM((HD, seq), f32),
            pltpu.VMEM((seq, HD), bf16),
            pltpu.VMEM((seq, HD), bf16),
            pltpu.VMEM((2 * RANK, seq), bf16),
            pltpu.VMEM((4, 2 * RANK, rows), f32),
            pltpu.VMEM((3, 2 * RANK, rows), f32),
            pltpu.VMEM((rows, 4 * heads * HD), bf16),
            pltpu.VMEM((heads, seq, HD), bf16),
            pltpu.VMEM((heads, seq, HD), bf16),
            pltpu.VMEM(normed.shape, bf16),
            pltpu.VMEM((2 * CHIPS, 8, 256), f32),
            pltpu.VMEM((CHIPS, 8, 256), f32),
            pltpu.VMEM((CHIPS, 8, 256), f32),
            pltpu.VMEM((CHIPS - 1, 8, 256), f32),
            pltpu.VMEM((8, 256), f32),
            pltpu.VMEM((2 * RANK, width), f32),
            pltpu.VMEM((2, PLANE, 8, HD), f32),
            pltpu.VMEM((PLANE, 8, HD), f32),
            pltpu.VMEM((PLANE, 8, HD), f32),
            pltpu.VMEM((PLANE - 1, 8, HD), f32),
            pltpu.VMEM((8, HD), f32),
            pltpu.VMEM((2, 8, PLANE * HD), f32),
            dma((8,)),
            dma((heads,)),
            dma((heads,)),
            dma((heads, 3)),
            dma((heads, 3)),
            dma((heads, 3)),
            dma((heads, 3)),
            dma((3,)),
            dma((3,)),
            dma((4,)),
            dma((4,)),
            dma((4,)),
            dma((4,)),
        ],
        compiler_params=pltpu.CompilerParams(
            dimension_semantics=("arbitrary",),
            collective_id=2,
            has_side_effects=True,
            vmem_limit_bytes=48 << 20,
        ),
        cost_estimate=pl.CostEstimate(
            flops=10 * heads * seq * seq * HD,
            bytes_accessed=16 * seq * heads * HD,
            transcendentals=heads * seq * seq,
        ),
        name="attention_step",
    )(projected, projected, projected, down, qup, vup, cos, sin, out_grad, normed)


def local(tokens, norm_gain, w_qkv, a_query, query_up_adapter, a_value, value_up_adapter, out_grad):
    projected, normed, down = gather_project(
        tokens[0], norm_gain, w_qkv, jnp.concatenate([a_query.T, a_value.T], 0)
    )
    cos, sin = rotary_tables(projected.shape[0])
    out_rows, ga_query, ga_value, gb_query, gb_value = attention(
        projected, down, query_up_adapter, value_up_adapter, cos, sin, out_grad[0], normed
    )
    return out_rows[None], ga_query.T, gb_query, ga_value.T, gb_value


def solution(mesh):
    return jax.shard_map(
        local,
        mesh=mesh,
        in_specs=(
            P(("dp", "fsdp"), "tensor", None),
            P(),
            P(("dp", "fsdp"), "tensor"),
            P(),
            P(None, "tensor"),
            P(),
            P(None, "tensor"),
            P(("dp", "fsdp"), "tensor", None),
        ),
        out_specs=(
            P(("dp", "fsdp"), "tensor", None),
            P(),
            P(None, "tensor"),
            P(),
            P(None, "tensor"),
        ),
        check_vma=False,
    )
```

```python
import functools
import math

import jax
import jax.numpy as jnp
import numpy as np
from jax import lax
from jax.experimental import pallas as pl
from jax.experimental.pallas import tpu as pltpu
from jax.sharding import PartitionSpec as P

HD = 128
QUERY_PER_KV = 8
RANK = 16
QB = 256

EPSILON = 1e-05
ADAPTER_SCALE = 2.0
ROPE_BASE = 500000.0
SCORE_SCALE = 1.0 / math.sqrt(HD)
LOG2E = 1.4426950408889634


def rotary_tables(sequence_length):
    half_dim = HD // 2
    inv_freq = ROPE_BASE ** (-np.arange(half_dim) / half_dim)
    angles = np.arange(sequence_length)[:, None] * inv_freq
    cosine, sine = np.cos(angles), np.sin(angles)
    return (
        np.concatenate([cosine, cosine], 1).astype(np.float32),
        np.concatenate([-sine, sine], 1).astype(np.float32),
    )


def dot_nt(a, b):
    return lax.dot_general(a, b, (((1,), (1,)), ((), ())), preferred_element_type=jnp.float32)


def dot_nn(a, b):
    return jnp.dot(a, b, preferred_element_type=jnp.float32)


def rotate(x, cos, sin):
    return x * cos + pltpu.roll(x, HD // 2, 1) * sin


MESH = pl.DeviceIdType.MESH
CHUNKS = 8
OFFSETS = (0, 3, 1, 2)


class Place:
    def __init__(self):
        self.dp = lax.axis_index("dp")
        self.fs = lax.axis_index("fsdp")
        self.y = lax.axis_index("tensor")
        self.core = lax.rem(self.dp, 2)
        self.x = lax.div(self.dp, 2) * 2 + lax.rem(self.fs, 2)
        self.z = lax.div(self.fs, 2)

    def ring(self, core):
        first = self.x * (1 - core) + self.z * core
        second = self.z * (1 - core) + self.x * core
        return first, second

    def plane(self, core, a, b):
        first, second = self.ring(core)
        first = lax.rem(first + a, 4)
        second = lax.rem(second + b, 4)
        x = first * (1 - core) + second * core
        z = second * (1 - core) + first * core
        return lax.div(x, 2) * 2 + core, z * 2 + lax.rem(x, 2)

    def near(self, a, b):
        return (*self.plane(self.core, a, b), self.y)

    def along(self, c):
        return (self.dp, self.fs, lax.rem(self.y + c, 4))

    def partner(self):
        return (self.dp + 1 - 2 * self.core, self.fs, self.y)


CHIPS = 64
PLANE = 16
LAG = 2


def step_kernel(
    rows,
    tok_hbm,
    gain_hbm,
    w_hbm,
    aq_hbm,
    av_hbm,
    qup_hbm,
    vup_hbm,
    cos_hbm,
    sin_hbm,
    grad_hbm,
    out_hbm,
    ga_q_hbm,
    ga_v_hbm,
    gb_q_hbm,
    gb_v_hbm,
    raw,
    scale_scr,
    x_buf,
    w_buf,
    acc,
    down_scr,
    gain_ref,
    adapt_ref,
    qup_ref,
    vup_ref,
    cos_ref,
    sin_ref,
    stage,
    q_buf,
    k_scr,
    v_scr,
    down_b,
    down_t,
    dv_scr,
    dq_scr,
    mid_scr,
    mid_recv,
    mid_all,
    g_buf,
    o_buf,
    part,
    part_recv,
    up_part,
    up_recv,
    total,
    rs_recv,
    final,
    up_final,
    res,
    up_res,
    ag_size,
    tok_sem,
    load_sem,
    own_sem,
    w_send,
    w_recv,
    d_send,
    d_recv,
    x_send,
    x_recv,
    own_g_sem,
    o_own_sem,
    g_send,
    g_recv,
    o_send,
    o_recv,
    m_send,
    m_recv,
    c_send,
    c_recv,
    r_send,
    r_recv,
    write_sem,
):
    heads = QUERY_PER_KV
    group = heads * HD
    seq = 4 * rows
    blocks = seq // QB

    me = Place()
    shard = w_hbm.shape[0]
    half_shard = shard // 2
    width = tok_hbm.shape[1]
    wide = width // CHUNKS
    cols = w_hbm.shape[1]
    parts = tok_sem.shape[0]
    span = rows // parts

    def tok_copy(i):
        piece = pl.ds(i * span, span)
        return pltpu.make_async_copy(tok_hbm.at[piece], raw.at[piece], tok_sem.at[i])

    for i in range(parts):
        tok_copy(i).start()

    loads = [
        pltpu.make_async_copy(src, dst, load_sem.at[i])
        for i, (src, dst) in enumerate(
            (
                (gain_hbm, gain_ref),
                (aq_hbm, adapt_ref.at[pl.ds(0, RANK)]),
                (av_hbm, adapt_ref.at[pl.ds(RANK, RANK)]),
                (qup_hbm, qup_ref),
                (vup_hbm, vup_ref),
                (cos_hbm, cos_ref),
                (sin_hbm, sin_ref),
                (grad_hbm, stage),
            )
        )
    ]

    def block(core, a, b):
        dp, fs = me.plane(core, a, b)
        return pl.multiple_of((dp * 8 + fs) * shard, shard)

    own = block(me.core, 0, 0)
    own_copy = pltpu.make_async_copy(w_hbm, w_buf.at[pl.ds(own, shard)], own_sem)
    own_copy.start()

    plane = lax.div(me.dp, 2) * 8 + me.fs
    chip = plane * 4 + me.y

    def of_chip(index):
        at = lax.div(index, 4)
        return (lax.div(at, 8) * 2 + me.core, lax.rem(at, 8), lax.rem(index, 4))

    barrier = pltpu.get_barrier_semaphore()

    @pl.loop(1, CHIPS)
    def _(o):
        pl.semaphore_signal(
            barrier, inc=1, device_id=of_chip(lax.rem(chip + o, CHIPS)), device_id_type=MESH
        )

    pl.semaphore_signal(barrier, inc=1, device_id=me.partner(), device_id_type=MESH)
    for load in loads:
        load.start()

    def lines_of(block):
        return pl.ds(pl.multiple_of(block * rows, rows), rows)

    def columns(block, h):
        return pl.ds(pl.multiple_of(block * group + h * HD, HD), HD)

    def remote(src, dst, send, recv, device):
        return pltpu.make_async_remote_copy(
            src_ref=src,
            dst_ref=dst,
            send_sem=send,
            recv_sem=recv,
            device_id=device,
            device_id_type=MESH,
        )

    def own_grad(h):
        return pltpu.make_async_copy(
            grad_hbm.at[:, columns(me.y, h)], g_buf.at[h, lines_of(me.y)], own_g_sem.at[h]
        )

    def grad_copy(h, c):
        to = lax.rem(me.y + c, 4)
        return remote(
            stage.at[:, columns(to, h)],
            g_buf.at[h, lines_of(me.y)],
            g_send.at[h, c - 1],
            g_recv.at[h, c - 1],
            me.along(c),
        )

    def grad_arrival(h, c):
        ref = g_buf.at[h, lines_of(lax.rem(me.y + 4 - c, 4))]
        return remote(ref, ref, g_send.at[h, c - 1], g_recv.at[h, c - 1], me.along(c))

    def own_out(h):
        return pltpu.make_async_copy(
            o_buf.at[h, lines_of(me.y)], out_hbm.at[:, columns(me.y, h)], o_own_sem.at[h]
        )

    def out_copy(h, c):
        to = lax.rem(me.y + c, 4)
        return remote(
            o_buf.at[h, lines_of(to)],
            out_hbm.at[:, columns(me.y, h)],
            o_send.at[h, c - 1],
            o_recv.at[h, c - 1],
            me.along(c),
        )

    def out_arrival(h, c):
        ref = out_hbm.at[:, columns(lax.rem(me.y + 4 - c, 4), h)]
        return remote(ref, ref, o_send.at[h, c - 1], o_recv.at[h, c - 1], me.along(c))

    sends = []

    def w_copy(a, b, device, kind, way, piece=None, source=None):
        start = block(me.core, a, b)
        size = shard
        if piece is not None:
            start, size = pl.multiple_of(start + piece * half_shard, half_shard), half_shard
        dst = w_buf.at[pl.ds(start, size)]
        return pltpu.make_async_remote_copy(
            src_ref=dst if source is None else source,
            dst_ref=dst,
            send_sem=w_send.at[kind, way],
            recv_sem=w_recv.at[kind, way],
            device_id=device,
            device_id_type=MESH,
        )

    def w_start(*args, **kwargs):
        copy = w_copy(*args, **kwargs)
        copy.start()
        sends.append(copy)

    def d_copy(core, event, a, b, source=None):
        dst = w_buf.at[pl.ds(block(core, a, b), shard)]
        return pltpu.make_async_remote_copy(
            src_ref=dst if source is None else source,
            dst_ref=dst,
            send_sem=d_send.at[event],
            recv_sem=d_recv.at[event],
            device_id=me.partner(),
            device_id_type=MESH,
        )

    order = []

    def share(a, b, source=None):
        copy = d_copy(me.core, len(order), a, b, source)
        copy.start()
        sends.append(copy)
        order.append((a, b))

    for i in range(parts):
        tok_copy(i).wait()

        @pl.loop(0, span // 16)
        def _(r):
            piece = pl.ds(pl.multiple_of(i * span + r * 16, 16), 16)
            squares = jnp.zeros((16, wide), jnp.float32)
            for c in range(CHUNKS):
                value = raw[piece, c * wide : (c + 1) * wide].astype(jnp.float32)
                squares = squares + value * value
            mean = jnp.sum(squares, axis=-1, keepdims=True) * (1.0 / width)
            scale_scr[piece, :] = jnp.broadcast_to(lax.rsqrt(mean + EPSILON), (16, 128))

    def x_copy(row_block, chunk, device, way):
        ref = x_buf.at[row_block, chunk]
        return pltpu.make_async_remote_copy(
            src_ref=ref,
            dst_ref=ref,
            send_sem=x_send.at[way, chunk],
            recv_sem=x_recv.at[way // 2 * 2 if way > 1 else way, chunk],
            device_id=device,
            device_id_type=MESH,
        )

    def normalize_chunk(c):
        @pl.loop(0, rows // 16)
        def _(r):
            piece = pl.ds(pl.multiple_of(r * 16, 16), 16)
            scale = scale_scr[piece, :]
            for k in range(wide // 128):
                lanes = slice(c * wide + k * 128, c * wide + (k + 1) * 128)
                value = raw[piece, lanes].astype(jnp.float32)
                x_buf[me.y, c, piece, k * 128 : (k + 1) * 128] = (
                    value * scale * gain_ref[:, lanes]
                ).astype(jnp.bfloat16)

    def x_start(row_block, chunk, device, way):
        copy = x_copy(row_block, chunk, device, way)
        copy.start()
        sends.append(copy)

    middle = CHUNKS // 2
    loads[0].wait()
    normalize_chunk(0)
    normalize_chunk(middle)
    pl.semaphore_wait(barrier, CHIPS)

    w_start(0, 0, me.near(1, 0), 4, 0, source=w_hbm)
    w_start(0, 0, me.near(3, 0), 4, 1, source=w_hbm)
    w_start(0, 0, me.near(0, 1), 0, 0, source=w_hbm)
    w_start(0, 0, me.near(0, 3), 0, 1, source=w_hbm)
    share(0, 0, source=w_hbm)

    for c in range(middle):
        x_start(me.y, c, me.along(1), 0)
        x_start(me.y, c + middle, me.along(3), 1)
        if c + 1 < middle:
            normalize_chunk(c + 1)
            normalize_chunk(c + 1 + middle)
    for c in range(middle):
        x_start(me.y, c + middle, me.along(1), 0)
        x_start(me.y, c, me.along(3), 1)

    acc[...] = jnp.zeros_like(acc)
    down_scr[...] = jnp.zeros_like(down_scr)

    dv_scr[...] = jnp.zeros_like(dv_scr)
    mid_scr[...] = jnp.zeros_like(mid_scr)
    up_part[...] = jnp.zeros_like(up_part)
    for load in loads[1:]:
        load.wait()

    def arrived(a, b, kind, way, piece=None):
        w_copy(a, b, me.near(0, 1), kind, way, piece).wait_recv()

    def spread(a, kind):
        w_start(a, 0, me.near(0, 1), kind, 0)
        w_start(a, 0, me.near(0, 3), kind, 1)

    own_copy.wait()
    arrived(3, 0, 4, 0)
    w_start(3, 0, me.near(1, 0), 4, 2, piece=0)
    spread(3, 1)
    share(3, 0)
    arrived(1, 0, 4, 1)
    w_start(1, 0, me.near(3, 0), 4, 3, piece=1)
    spread(1, 2)
    share(1, 0)
    for kind, a in enumerate(OFFSETS):
        if kind == 3:
            arrived(2, 0, 4, 2, piece=0)
            arrived(2, 0, 4, 3, piece=1)
            spread(2, 3)
            share(2, 0)
        arrived(a, 3, kind, 0)
        w_start(a, 3, me.near(0, 1), kind, 2, piece=0)
        share(a, 3)
        arrived(a, 1, kind, 1)
        w_start(a, 1, me.near(0, 3), kind, 3, piece=1)
        share(a, 1)
        if kind > 0:
            before = OFFSETS[kind - 1]
            arrived(before, 2, kind - 1, 2, piece=0)
            arrived(before, 2, kind - 1, 3, piece=1)
            share(before, 2)
    arrived(OFFSETS[3], 2, 3, 2, piece=0)
    arrived(OFFSETS[3], 2, 3, 3, piece=1)
    share(OFFSETS[3], 2)

    minus = lax.rem(me.y + 3, 4)
    plus = lax.rem(me.y + 1, 4)
    far = lax.rem(me.y + 2, 4)
    for c in range(middle):
        x_copy(minus, c, me.along(1), 0).wait_recv()
        x_start(minus, c, me.along(1), 2)
        x_copy(plus, c + middle, me.along(1), 1).wait_recv()
        x_start(plus, c + middle, me.along(3), 2)

    @pl.loop(0, heads)
    def _(h):
        own_grad(h).start()
        for c in (1, 3, 2):
            grad_copy(h, c).start()

    for event, (a, b) in enumerate(order):
        d_copy(1 - me.core, event, a, b).wait_recv()

    def multiply(row_block, chunk):
        value = x_buf[row_block, chunk]
        lines = pl.ds(pl.multiple_of(row_block * rows, rows), rows)
        depth = pl.ds(pl.multiple_of(chunk * wide, wide), wide)
        for n in range(cols // 256):
            lanes = slice(n * 256, (n + 1) * 256)
            acc[lines, lanes] += dot_nn(value, w_buf[depth, lanes])
        down_scr[lines, :] += dot_nt(value, adapt_ref[:, depth])

    def prepare(row_block):
        lines = pl.ds(pl.multiple_of(row_block * rows, rows), rows)
        down = down_scr[lines, :].astype(jnp.bfloat16)
        down_b[lines, :] = down
        cos, sin = cos_ref[lines, :], sin_ref[lines, :]
        for h in range(heads):
            lanes = slice(h * HD, (h + 1) * HD)
            value = acc[lines, lanes] + ADAPTER_SCALE * dot_nn(down[:, :RANK], qup_ref[:, lanes])
            value = value.astype(jnp.bfloat16).astype(jnp.float32)
            q_buf[h, lines, :] = rotate(value, cos, sin).astype(jnp.bfloat16)
        value = acc[lines, group : group + HD].astype(jnp.bfloat16).astype(jnp.float32)
        k_scr[lines, :] = rotate(value, cos, sin).astype(jnp.bfloat16)
        v_scr[lines, :] = (
            acc[lines, group + HD :] + ADAPTER_SCALE * dot_nn(down[:, RANK:], vup_ref[...])
        ).astype(jnp.bfloat16)

    @pl.loop(0, CHUNKS)
    def _(c):
        multiply(me.y, c)

    @pl.loop(0, CHUNKS)
    def _(c):
        @pl.when(c >= middle)
        def _():
            x_copy(minus, c, me.along(1), 0).wait_recv()

        multiply(minus, c)

    @pl.loop(0, CHUNKS)
    def _(c):
        @pl.when(c < middle)
        def _():
            x_copy(plus, c, me.along(1), 1).wait_recv()

        multiply(plus, c)

    @pl.loop(0, 3)
    def _(c):
        prepare(lax.rem(me.y + 3 + c, 4))

    @pl.loop(0, middle)
    def _(c):
        x_copy(far, c, me.along(1), 2).wait_recv()
        multiply(far, c)
        x_copy(far, c + middle, me.along(1), 2).wait_recv()
        multiply(far, c + middle)

    prepare(far)
    down_t[...] = down_b[...].astype(jnp.float32).T.astype(jnp.bfloat16)

    row = lax.broadcasted_iota(jnp.int32, (QB, QB), 0)
    col = lax.broadcasted_iota(jnp.int32, (QB, QB), 1)
    causal = row >= col
    factor = SCORE_SCALE * LOG2E

    def send_out(h):
        own_out(h).start()
        for c in (1, 3, 2):
            out_copy(h, c).start()

    @pl.loop(0, heads)
    def _(head):
        own_grad(head).wait()
        for c in (1, 3, 2):
            grad_arrival(head, c).wait_recv()

        for i in range(blocks):
            own_rows = slice(i * QB, (i + 1) * QB)
            q = q_buf[head, own_rows, :]
            grad = g_buf[head, own_rows, :]
            grad_t = grad.T
            scores = []
            for j in range(i + 1):
                s = dot_nt(q, k_scr[j * QB : (j + 1) * QB, :])
                if j == i:
                    s = jnp.where(causal, s, -1e30)
                scores.append(s)
            top = functools.reduce(jnp.maximum, scores)
            top = jnp.max(top, axis=-1, keepdims=True) * factor
            weights = [jnp.exp2(s * factor - top) for s in scores]
            whole = jnp.sum(functools.reduce(jnp.add, weights), axis=-1, keepdims=True)
            inverse = 1.0 / whole
            probs = [w * inverse for w in weights]
            rounded = [p.astype(jnp.bfloat16) for p in probs]
            attended = functools.reduce(
                jnp.add, [dot_nn(rounded[j], v_scr[j * QB : (j + 1) * QB, :]) for j in range(i + 1)]
            )
            o_buf[head, own_rows, :] = attended.astype(jnp.bfloat16)
            prods = []
            for j in range(i + 1):
                keys = slice(j * QB, (j + 1) * QB)
                dp = dot_nt(grad, v_scr[keys, :])
                prods.append(probs[j] * dp)
                dv_scr[:, keys] += dot_nn(grad_t, rounded[j])
            inner = jnp.sum(functools.reduce(jnp.add, prods), axis=-1, keepdims=True)
            ds = [(prods[j] - probs[j] * inner).astype(jnp.bfloat16) for j in range(i + 1)]
            dq = functools.reduce(
                jnp.add, [dot_nn(ds[j], k_scr[j * QB : (j + 1) * QB, :]) for j in range(i + 1)]
            )
            dq = (dq * SCORE_SCALE).astype(jnp.bfloat16).astype(jnp.float32)
            dq_scr[own_rows, :] = rotate(dq, cos_ref[own_rows, :], -sin_ref[own_rows, :]).astype(
                jnp.bfloat16
            )


        @pl.when(head >= LAG)
        def _():
            send_out(head - LAG)

        up = dot_nn(down_t[:RANK, :], dq_scr[...])
        up_part[0, head, :, :HD] = up[:8]
        up_part[1, head, :, :HD] = up[8:]
        lanes = pl.ds(pl.multiple_of(head * HD, HD), HD)
        for b in range(4):
            mid_scr[b, :RANK, :] += dot_nt(qup_ref[:, lanes], dq_scr[b * rows : (b + 1) * rows, :])

    dv = dv_scr[...].T.astype(jnp.bfloat16)
    for b in range(4):
        mid_scr[b, RANK:, :] = dot_nt(vup_ref[...], dv[b * rows : (b + 1) * rows])
    up = dot_nn(down_t[RANK:, :], dv)
    up_part[0, heads, :, :HD] = up[:8]
    up_part[1, heads, :, :HD] = up[8:]

    def mid_copy(c):
        return remote(
            mid_scr.at[lax.rem(me.y + c, 4)],
            mid_recv.at[c - 1],
            m_send.at[c - 1],
            m_recv.at[c - 1],
            me.along(c),
        )

    def mid_share(c):
        return remote(
            mid_all.at[me.y], mid_all.at[me.y], m_send.at[2 + c], m_recv.at[2 + c], me.along(c)
        )

    def mid_other(c):
        ref = mid_all.at[lax.rem(me.y + 4 - c, 4)]
        return remote(ref, ref, m_send.at[2 + c], m_recv.at[2 + c], me.along(c))

    for c in (1, 3, 2):
        mid_copy(c).start()
    for c in (1, 3, 2):
        mid_copy(c).wait_recv()
    mid_all[me.y] = (mid_scr[me.y] + mid_recv[0] + mid_recv[1] + mid_recv[2]).astype(jnp.bfloat16)
    for c in (1, 3, 2):
        mid_share(c).start()

    @pl.loop(heads - LAG, heads)
    def _(h):
        send_out(h)

    for c in (1, 3, 2):
        mid_other(c).wait_recv()

    def partial(half):
        made = dot_nn(mid_all[0], x_buf[0, 2 * me.y + half])
        for b in range(1, 4):
            made += dot_nn(mid_all[b], x_buf[b, 2 * me.y + half])
        for r in range(4):
            for k in range(4):
                part[half, r * 4 + k] = made[r * 8 : (r + 1) * 8, k * 256 : (k + 1) * 256]

    partial(1 - me.core)
    swap = remote(part.at[1 - me.core], part_recv, c_send.at[0], c_recv.at[0], me.partner())
    up_swap = remote(up_part.at[1 - me.core], up_recv, c_send.at[1], c_recv.at[1], me.partner())
    swap.start()
    up_swap.start()
    partial(me.core)
    up_swap.wait_recv()
    swap.wait_recv()
    total[:, :, :256] = part[me.core] + part_recv[...]
    total[:, :, 256:] = up_part[me.core] + up_recv[...]

    @pl.loop(1, PLANE)
    def _(o):
        to = lax.rem(plane + o, PLANE)
        remote(
            total.at[to], rs_recv.at[o - 1], r_send.at[0], r_recv.at[0], of_chip(to * 4 + me.y)
        ).start()

    many = remote(rs_recv, rs_recv, r_send.at[0], r_recv.at[0], me.partner())
    many.wait_recv()
    summed = total[plane]
    for o in range(PLANE - 1):
        summed += rs_recv[o]
    summed = ADAPTER_SCALE * summed
    final[...] = summed[:, :256]
    up_final[...] = summed[:, 256:]

    at_rows = pl.ds(pl.multiple_of(lax.div(plane, 4) * 8, 8), 8)
    at_cols = pl.ds(pl.multiple_of(lax.rem(plane, 4) * 256, 256), 256)
    up_cols = pl.ds(pl.multiple_of(plane * HD, HD), HD)

    @pl.loop(1, CHIPS)
    def _(o):
        to = lax.rem(chip + o, CHIPS)
        remote(
            final,
            res.at[me.core, me.y, at_rows, at_cols],
            r_send.at[1],
            r_recv.at[1],
            of_chip(to),
        ).start()

    @pl.loop(1, PLANE)
    def _(o):
        to = lax.rem(plane + o, PLANE)
        remote(
            up_final,
            up_res.at[me.core, :, up_cols],
            r_send.at[2],
            r_recv.at[2],
            of_chip(to * 4 + me.y),
        ).start()

    res[me.core, me.y, at_rows, at_cols] = final[...]
    up_res[me.core, :, up_cols] = up_final[...]
    all_of = remote(ag_size, ag_size, r_send.at[1], r_recv.at[1], me.partner())
    up_size = part_recv.at[pl.ds(0, PLANE - 1), :, pl.ds(0, HD)]
    up_all = remote(up_size, up_size, r_send.at[2], r_recv.at[2], me.partner())
    up_all.wait_recv()
    up_half = remote(
        up_res.at[me.core], up_res.at[me.core], c_send.at[2], c_recv.at[2], me.partner()
    )
    up_half.start()
    all_of.wait_recv()
    half = remote(res.at[me.core], res.at[me.core], c_send.at[3], c_recv.at[3], me.partner())
    half.start()

    def grad_a_writes(b, first):
        copies = []
        for yy in range(4):
            cols_out = pl.ds(pl.multiple_of(yy * 2048 + b * 1024, 1024), 1024)
            for i, dst in enumerate((ga_q_hbm, ga_v_hbm)):
                copies.append(
                    pltpu.make_async_copy(
                        res.at[b, yy, pl.ds(i * RANK, RANK)],
                        dst.at[:, cols_out],
                        write_sem.at[first + yy * 2 + i],
                    )
                )
        return copies

    def grad_b_writes(b, first):
        eight = pl.ds(pl.multiple_of(b * 8, 8), 8)
        return [
            pltpu.make_async_copy(
                up_res.at[b, :, pl.ds(0, group)], gb_q_hbm.at[eight], write_sem.at[first]
            ),
            pltpu.make_async_copy(
                up_res.at[b, :, pl.ds(group, HD)], gb_v_hbm.at[eight], write_sem.at[first + 1]
            ),
        ]

    writes = grad_a_writes(me.core, 0) + grad_b_writes(me.core, 8)
    for copy in writes:
        copy.start()
    @pl.loop(0, heads)
    def _(h):
        own_out(h).wait()
        for c in (1, 3, 2):
            grad_copy(h, c).wait_send()
            out_copy(h, c).wait_send()
            out_arrival(h, c).wait_recv()

    for copy in sends:
        copy.wait_send()
    up_other = up_res.at[1 - me.core]
    remote(up_other, up_other, c_send.at[2], c_recv.at[2], me.partner()).wait_recv()
    other = res.at[1 - me.core]
    remote(other, other, c_send.at[3], c_recv.at[3], me.partner()).wait_recv()
    late = grad_a_writes(1 - me.core, 10) + grad_b_writes(1 - me.core, 18)
    for copy in late:
        copy.start()
    for c in (1, 3, 2):
        mid_copy(c).wait_send()
        mid_share(c).wait_send()
    for copy in (up_swap, swap, many, all_of, up_all, up_half, half):
        copy.wait_send()
    for copy in writes + late:
        copy.wait()


def fused_step(tokens, gain, w_qkv, aq_t, av_t, qup, vup, cos, sin, out_grad):
    rows, width = tokens.shape
    shard, cols = w_qkv.shape
    heads = QUERY_PER_KV
    seq = 4 * rows
    wide = width // CHUNKS
    anywhere = pl.BlockSpec(memory_space=pl.ANY)
    dma = pltpu.SemaphoreType.DMA
    f32, bf16 = jnp.float32, jnp.bfloat16
    return pl.pallas_call(
        functools.partial(step_kernel, rows),
        in_specs=[anywhere] * 10,
        out_specs=[anywhere] * 5,
        out_shape=[
            jax.ShapeDtypeStruct((rows, 4 * heads * HD), bf16),
            jax.ShapeDtypeStruct((RANK, width), f32),
            jax.ShapeDtypeStruct((RANK, width), f32),
            jax.ShapeDtypeStruct((RANK, heads * HD), f32),
            jax.ShapeDtypeStruct((RANK, HD), f32),
        ],
        scratch_shapes=[
            pltpu.VMEM((rows, width), bf16),
            pltpu.VMEM((rows, 128), f32),
            pltpu.VMEM((4, CHUNKS, rows, wide), bf16),
            pltpu.VMEM((width, cols), bf16),
            pltpu.VMEM((seq, cols), f32),
            pltpu.VMEM((seq, 2 * RANK), f32),
            pltpu.VMEM((1, width), f32),
            pltpu.VMEM((2 * RANK, width), bf16),
            pltpu.VMEM((RANK, heads * HD), bf16),
            pltpu.VMEM((RANK, HD), bf16),
            pltpu.VMEM((seq, HD), f32),
            pltpu.VMEM((seq, HD), f32),
            pltpu.VMEM((rows, 4 * heads * HD), bf16),
            pltpu.VMEM((heads, seq, HD), bf16),
            pltpu.VMEM((seq, HD), bf16),
            pltpu.VMEM((seq, HD), bf16),
            pltpu.VMEM((seq, 2 * RANK), bf16),
            pltpu.VMEM((2 * RANK, seq), bf16),
            pltpu.VMEM((HD, seq), f32),
            pltpu.VMEM((seq, HD), bf16),
            pltpu.VMEM((4, 2 * RANK, rows), f32),
            pltpu.VMEM((3, 2 * RANK, rows), f32),
            pltpu.VMEM((4, 2 * RANK, rows), bf16),
            pltpu.VMEM((heads, seq, HD), bf16),
            pltpu.VMEM((heads, seq, HD), bf16),
            pltpu.VMEM((2, PLANE, 8, 256), f32),
            pltpu.VMEM((PLANE, 8, 256), f32),
            pltpu.VMEM((2, PLANE, 8, HD), f32),
            pltpu.VMEM((PLANE, 8, HD), f32),
            pltpu.VMEM((PLANE, 8, 256 + HD), f32),
            pltpu.VMEM((PLANE - 1, 8, 256 + HD), f32),
            pltpu.VMEM((8, 256), f32),
            pltpu.VMEM((8, HD), f32),
            pltpu.VMEM((2, 4, 2 * RANK, 1024), f32),
            pltpu.VMEM((2, 8, PLANE * HD), f32),
            pltpu.VMEM((CHIPS - 1, 8, 256), f32),
            dma((4,)),
            dma((8,)),
            dma(()),
            dma((5, 4)),
            dma((5, 4)),
            dma((16,)),
            dma((16,)),
            dma((3, CHUNKS)),
            dma((3, CHUNKS)),
            dma((heads,)),
            dma((heads,)),
            dma((heads, 3)),
            dma((heads, 3)),
            dma((heads, 3)),
            dma((heads, 3)),
            dma((6,)),
            dma((6,)),
            dma((4,)),
            dma((4,)),
            dma((3,)),
            dma((3,)),
            dma((20,)),
        ],
        compiler_params=pltpu.CompilerParams(
            collective_id=1, has_side_effects=True, vmem_limit_bytes=63 << 20
        ),
        cost_estimate=pl.CostEstimate(
            flops=2 * seq * width * cols,
            bytes_accessed=10 * 1000 * 1000,
            transcendentals=heads * seq * seq,
        ),
        name="fused_step",
    )(tokens, gain.reshape(1, width), w_qkv, aq_t, av_t, qup, vup, cos, sin, out_grad)


def local(tokens, norm_gain, w_qkv, a_query, query_up_adapter, a_value, value_up_adapter, out_grad):
    cos, sin = rotary_tables(4 * tokens.shape[1])
    out_rows, ga_query, ga_value, gb_query, gb_value = fused_step(
        tokens[0],
        norm_gain,
        w_qkv,
        a_query.T,
        a_value.T,
        query_up_adapter,
        value_up_adapter,
        cos,
        sin,
        out_grad[0],
    )
    return out_rows[None], ga_query.T, gb_query, ga_value.T, gb_value


def solution(mesh):
    return jax.shard_map(
        local,
        mesh=mesh,
        in_specs=(
            P(("dp", "fsdp"), "tensor", None),
            P(),
            P(("dp", "fsdp"), "tensor"),
            P(),
            P(None, "tensor"),
            P(),
            P(None, "tensor"),
            P(("dp", "fsdp"), "tensor", None),
        ),
        out_specs=(
            P(("dp", "fsdp"), "tensor", None),
            P(),
            P(None, "tensor"),
            P(),
            P(None, "tensor"),
        ),
        check_vma=False,
    )
```

```python
import functools
import math

import jax
import jax.numpy as jnp
import numpy as np
from jax import lax
from jax.experimental import pallas as pl
from jax.experimental.pallas import tpu as pltpu
from jax.sharding import PartitionSpec as P

HD = 128
QUERY_PER_KV = 8
RANK = 16
QB = 384

EPSILON = 1e-05
ADAPTER_SCALE = 2.0
ROPE_BASE = 500000.0
SCORE_SCALE = 1.0 / math.sqrt(HD)
LOG2E = 1.4426950408889634


def rotary_tables(sequence_length):
    half_dim = HD // 2
    inv_freq = ROPE_BASE ** (-np.arange(half_dim) / half_dim)
    angles = np.arange(sequence_length)[:, None] * inv_freq
    cosine, sine = np.cos(angles), np.sin(angles)
    return (
        np.concatenate([cosine, cosine], 1).astype(np.float32),
        np.concatenate([-sine, sine], 1).astype(np.float32),
    )


def dot_nt(a, b):
    return lax.dot_general(a, b, (((1,), (1,)), ((), ())), preferred_element_type=jnp.float32)


def dot_nn(a, b):
    return jnp.dot(a, b, preferred_element_type=jnp.float32)


def rotate(x, cos, sin):
    return x * cos + pltpu.roll(x, HD // 2, 1) * sin


MESH = pl.DeviceIdType.MESH
CHUNKS = 8
OFFSETS = (0, 3, 1, 2)


class Place:
    def __init__(self):
        self.dp = lax.axis_index("dp")
        self.fs = lax.axis_index("fsdp")
        self.y = lax.axis_index("tensor")
        self.core = lax.rem(self.dp, 2)
        self.x = lax.div(self.dp, 2) * 2 + lax.rem(self.fs, 2)
        self.z = lax.div(self.fs, 2)

    def ring(self, core):
        first = self.x * (1 - core) + self.z * core
        second = self.z * (1 - core) + self.x * core
        return first, second

    def plane(self, core, a, b):
        first, second = self.ring(core)
        first = lax.rem(first + a, 4)
        second = lax.rem(second + b, 4)
        x = first * (1 - core) + second * core
        z = second * (1 - core) + first * core
        return lax.div(x, 2) * 2 + core, z * 2 + lax.rem(x, 2)

    def near(self, a, b):
        return (*self.plane(self.core, a, b), self.y)

    def along(self, c):
        return (self.dp, self.fs, lax.rem(self.y + c, 4))

    def partner(self):
        return (self.dp + 1 - 2 * self.core, self.fs, self.y)


CHIPS = 64
PLANE = 16
LAG = 4
AROUND = sorted(
    ((a, b) for a in range(4) for b in range(4)),
    key=lambda step: -sum(min(n, 4 - n) for n in step),
)


def step_kernel(
    rows,
    tok_hbm,
    gain_hbm,
    w_hbm,
    aq_hbm,
    av_hbm,
    qup_hbm,
    vup_hbm,
    cos_hbm,
    sin_hbm,
    grad_hbm,
    out_hbm,
    ga_q_hbm,
    ga_v_hbm,
    gb_hbm,
    raw,
    scale_scr,
    x_buf,
    w_buf,
    acc,
    down_scr,
    gain_ref,
    adapt_ref,
    qup_ref,
    vup_ref,
    cos_ref,
    sin_ref,
    stage,
    q_buf,
    k_scr,
    v_scr,
    down_b,
    down_t,
    dv_scr,
    dq_all,
    mid_scr,
    mid_recv,
    mid_all,
    g_buf,
    o_buf,
    part,
    part_recv,
    up_part,
    up_recv,
    total,
    rs_recv,
    final,
    up_final,
    res,
    up_res,
    ag_size,
    tok_sem,
    load_sem,
    own_sem,
    w_send,
    w_recv,
    d_send,
    d_recv,
    x_send,
    x_recv,
    own_g_sem,
    o_own_sem,
    g_send,
    g_recv,
    o_send,
    o_recv,
    m_send,
    m_recv,
    c_send,
    c_recv,
    r_send,
    r_recv,
    write_sem,
):
    heads = QUERY_PER_KV
    group = heads * HD
    seq = 4 * rows
    blocks = seq // QB

    me = Place()
    shard = w_hbm.shape[0]
    half_shard = shard // 2
    width = tok_hbm.shape[1]
    wide = width // CHUNKS
    cols = w_hbm.shape[1]
    parts = tok_sem.shape[0]
    span = rows // parts

    def tok_copy(i):
        piece = pl.ds(i * span, span)
        return pltpu.make_async_copy(tok_hbm.at[piece], raw.at[piece], tok_sem.at[i])

    for i in range(parts):
        tok_copy(i).start()

    loads = [
        pltpu.make_async_copy(src, dst, load_sem.at[i])
        for i, (src, dst) in enumerate(
            (
                (gain_hbm, gain_ref),
                (aq_hbm, adapt_ref.at[pl.ds(0, RANK)]),
                (av_hbm, adapt_ref.at[pl.ds(RANK, RANK)]),
                (qup_hbm, qup_ref),
                (vup_hbm, vup_ref),
                (cos_hbm, cos_ref),
                (sin_hbm, sin_ref),
                (grad_hbm, stage),
            )
        )
    ]

    def block(core, a, b):
        dp, fs = me.plane(core, a, b)
        return pl.multiple_of((dp * 8 + fs) * shard, shard)

    own = block(me.core, 0, 0)
    own_copy = pltpu.make_async_copy(w_hbm, w_buf.at[pl.ds(own, shard)], own_sem)
    own_copy.start()

    plane = lax.div(me.dp, 2) * 8 + me.fs

    barrier = pltpu.get_barrier_semaphore()

    neighbours = (
        me.along(1),
        me.along(3),
        me.along(2),
        me.near(1, 0),
        me.near(3, 0),
        me.near(0, 1),
        me.near(0, 3),
        me.partner(),
    )
    for device in neighbours:
        pl.semaphore_signal(barrier, inc=1, device_id=device, device_id_type=MESH)
    for load in loads:
        load.start()

    def lines_of(block):
        return pl.ds(pl.multiple_of(block * rows, rows), rows)

    def columns(block, h):
        return pl.ds(pl.multiple_of(block * group + h * HD, HD), HD)

    def remote(src, dst, send, recv, device):
        return pltpu.make_async_remote_copy(
            src_ref=src,
            dst_ref=dst,
            send_sem=send,
            recv_sem=recv,
            device_id=device,
            device_id_type=MESH,
        )

    def own_grad(h):
        return pltpu.make_async_copy(
            grad_hbm.at[:, columns(me.y, h)], g_buf.at[h, lines_of(me.y)], own_g_sem.at[h]
        )

    def grad_copy(h, c):
        to = lax.rem(me.y + c, 4)
        return remote(
            stage.at[:, columns(to, h)],
            g_buf.at[h, lines_of(me.y)],
            g_send.at[h, c - 1],
            g_recv.at[h, c - 1],
            me.along(c),
        )

    def grad_arrival(h, c):
        ref = g_buf.at[h, lines_of(lax.rem(me.y + 4 - c, 4))]
        return remote(ref, ref, g_send.at[h, c - 1], g_recv.at[h, c - 1], me.along(c))

    def own_out(h):
        return pltpu.make_async_copy(
            o_buf.at[h, lines_of(me.y)], out_hbm.at[:, columns(me.y, h)], o_own_sem.at[h]
        )

    def out_copy(h, c):
        to = lax.rem(me.y + c, 4)
        return remote(
            o_buf.at[h, lines_of(to)],
            out_hbm.at[:, columns(me.y, h)],
            o_send.at[h, c - 1],
            o_recv.at[h, c - 1],
            me.along(c),
        )

    def out_arrival(h, c):
        ref = out_hbm.at[:, columns(lax.rem(me.y + 4 - c, 4), h)]
        return remote(ref, ref, o_send.at[h, c - 1], o_recv.at[h, c - 1], me.along(c))

    sends = []

    def w_copy(a, b, device, kind, way, piece=None, source=None):
        start = block(me.core, a, b)
        size = shard
        if piece is not None:
            start, size = pl.multiple_of(start + piece * half_shard, half_shard), half_shard
        dst = w_buf.at[pl.ds(start, size)]
        return pltpu.make_async_remote_copy(
            src_ref=dst if source is None else source,
            dst_ref=dst,
            send_sem=w_send.at[kind, way],
            recv_sem=w_recv.at[kind, way],
            device_id=device,
            device_id_type=MESH,
        )

    def w_start(*args, **kwargs):
        copy = w_copy(*args, **kwargs)
        copy.start()
        sends.append(copy)

    def d_copy(core, event, a, b, source=None):
        dst = w_buf.at[pl.ds(block(core, a, b), shard)]
        return pltpu.make_async_remote_copy(
            src_ref=dst if source is None else source,
            dst_ref=dst,
            send_sem=d_send.at[event],
            recv_sem=d_recv.at[event],
            device_id=me.partner(),
            device_id_type=MESH,
        )

    order = []

    def share(a, b, source=None):
        copy = d_copy(me.core, len(order), a, b, source)
        copy.start()
        sends.append(copy)
        order.append((a, b))

    for i in range(parts):
        tok_copy(i).wait()

        @pl.loop(0, span // 16)
        def _(r):
            piece = pl.ds(pl.multiple_of(i * span + r * 16, 16), 16)
            squares = jnp.zeros((16, wide), jnp.float32)
            for c in range(CHUNKS):
                value = raw[piece, c * wide : (c + 1) * wide].astype(jnp.float32)
                squares = squares + value * value
            mean = jnp.sum(squares, axis=-1, keepdims=True) * (1.0 / width)
            scale_scr[piece, :] = jnp.broadcast_to(lax.rsqrt(mean + EPSILON), (16, 128))

    def x_copy(row_block, chunk, device, way):
        ref = x_buf.at[row_block, chunk]
        return pltpu.make_async_remote_copy(
            src_ref=ref,
            dst_ref=ref,
            send_sem=x_send.at[way, chunk],
            recv_sem=x_recv.at[way // 2 * 2 if way > 1 else way, chunk],
            device_id=device,
            device_id_type=MESH,
        )

    def normalize_chunk(c):
        @pl.loop(0, rows // 16)
        def _(r):
            piece = pl.ds(pl.multiple_of(r * 16, 16), 16)
            scale = scale_scr[piece, :]
            for k in range(wide // 128):
                lanes = slice(c * wide + k * 128, c * wide + (k + 1) * 128)
                value = raw[piece, lanes].astype(jnp.float32)
                x_buf[me.y, c, piece, k * 128 : (k + 1) * 128] = (
                    value * scale * gain_ref[:, lanes]
                ).astype(jnp.bfloat16)

    def x_start(row_block, chunk, device, way):
        copy = x_copy(row_block, chunk, device, way)
        copy.start()
        sends.append(copy)

    middle = CHUNKS // 2
    loads[0].wait()
    normalize_chunk(0)
    normalize_chunk(middle)
    pl.semaphore_wait(barrier, len(neighbours))

    w_start(0, 0, me.near(1, 0), 4, 0, source=w_hbm)
    w_start(0, 0, me.near(3, 0), 4, 1, source=w_hbm)
    w_start(0, 0, me.near(0, 1), 0, 0, source=w_hbm)
    w_start(0, 0, me.near(0, 3), 0, 1, source=w_hbm)
    share(0, 0, source=w_hbm)

    for c in range(middle):
        x_start(me.y, c, me.along(1), 0)
        x_start(me.y, c + middle, me.along(3), 1)
        if c + 1 < middle:
            normalize_chunk(c + 1)
            normalize_chunk(c + 1 + middle)
    for c in range(middle):
        x_start(me.y, c + middle, me.along(1), 0)
        x_start(me.y, c, me.along(3), 1)

    acc[...] = jnp.zeros_like(acc)
    down_scr[...] = jnp.zeros_like(down_scr)

    dv_scr[...] = jnp.zeros_like(dv_scr)
    up_part[...] = jnp.zeros_like(up_part)
    for load in loads[1:]:
        load.wait()

    def arrived(a, b, kind, way, piece=None):
        w_copy(a, b, me.near(0, 1), kind, way, piece).wait_recv()

    def spread(a, kind):
        w_start(a, 0, me.near(0, 1), kind, 0)
        w_start(a, 0, me.near(0, 3), kind, 1)

    own_copy.wait()
    arrived(3, 0, 4, 0)
    w_start(3, 0, me.near(1, 0), 4, 2, piece=0)
    spread(3, 1)
    share(3, 0)
    arrived(1, 0, 4, 1)
    w_start(1, 0, me.near(3, 0), 4, 3, piece=1)
    spread(1, 2)
    share(1, 0)
    for kind, a in enumerate(OFFSETS):
        if kind == 3:
            arrived(2, 0, 4, 2, piece=0)
            arrived(2, 0, 4, 3, piece=1)
            spread(2, 3)
            share(2, 0)
        arrived(a, 3, kind, 0)
        w_start(a, 3, me.near(0, 1), kind, 2, piece=0)
        share(a, 3)
        arrived(a, 1, kind, 1)
        w_start(a, 1, me.near(0, 3), kind, 3, piece=1)
        share(a, 1)
        if kind > 0:
            before = OFFSETS[kind - 1]
            arrived(before, 2, kind - 1, 2, piece=0)
            arrived(before, 2, kind - 1, 3, piece=1)
            share(before, 2)
    arrived(OFFSETS[3], 2, 3, 2, piece=0)
    arrived(OFFSETS[3], 2, 3, 3, piece=1)
    share(OFFSETS[3], 2)

    minus = lax.rem(me.y + 3, 4)
    plus = lax.rem(me.y + 1, 4)
    far = lax.rem(me.y + 2, 4)
    for c in range(middle):
        x_copy(minus, c, me.along(1), 0).wait_recv()
        x_start(minus, c, me.along(1), 2)
        x_copy(plus, c + middle, me.along(1), 1).wait_recv()
        x_start(plus, c + middle, me.along(3), 2)

    @pl.loop(0, heads)
    def _(h):
        own_grad(h).start()
        for c in (1, 3, 2):
            grad_copy(h, c).start()

    for event, (a, b) in enumerate(order):
        d_copy(1 - me.core, event, a, b).wait_recv()

    def multiply(row_block, chunk):
        value = x_buf[row_block, chunk]
        lines = pl.ds(pl.multiple_of(row_block * rows, rows), rows)
        depth = pl.ds(pl.multiple_of(chunk * wide, wide), wide)
        for n in range(cols // 256):
            lanes = slice(n * 256, (n + 1) * 256)
            acc[lines, lanes] += dot_nn(value, w_buf[depth, lanes])
        down_scr[lines, :] += dot_nt(value, adapt_ref[:, depth])

    def prepare(row_block):
        lines = pl.ds(pl.multiple_of(row_block * rows, rows), rows)
        down = down_scr[lines, :].astype(jnp.bfloat16)
        down_b[lines, :] = down
        cos, sin = cos_ref[lines, :], sin_ref[lines, :]
        for h in range(heads):
            lanes = slice(h * HD, (h + 1) * HD)
            value = acc[lines, lanes] + ADAPTER_SCALE * dot_nn(down[:, :RANK], qup_ref[:, lanes])
            value = value.astype(jnp.bfloat16).astype(jnp.float32)
            q_buf[h, lines, :] = rotate(value, cos, sin).astype(jnp.bfloat16)
        value = acc[lines, group : group + HD].astype(jnp.bfloat16).astype(jnp.float32)
        k_scr[lines, :] = rotate(value, cos, sin).astype(jnp.bfloat16)
        v_scr[lines, :] = (
            acc[lines, group + HD :] + ADAPTER_SCALE * dot_nn(down[:, RANK:], vup_ref[...])
        ).astype(jnp.bfloat16)

    @pl.loop(0, CHUNKS)
    def _(c):
        multiply(me.y, c)

    @pl.loop(0, CHUNKS)
    def _(c):
        @pl.when(c >= middle)
        def _():
            x_copy(minus, c, me.along(1), 0).wait_recv()

        multiply(minus, c)

    @pl.loop(0, CHUNKS)
    def _(c):
        @pl.when(c < middle)
        def _():
            x_copy(plus, c, me.along(1), 1).wait_recv()

        multiply(plus, c)

    @pl.loop(0, 3)
    def _(c):
        prepare(lax.rem(me.y + 3 + c, 4))

    @pl.loop(0, middle)
    def _(c):
        x_copy(far, c, me.along(1), 2).wait_recv()
        multiply(far, c)
        x_copy(far, c + middle, me.along(1), 2).wait_recv()
        multiply(far, c + middle)

    prepare(far)
    down_t[...] = down_b[...].astype(jnp.float32).T.astype(jnp.bfloat16)

    row = lax.broadcasted_iota(jnp.int32, (QB, QB), 0)
    col = lax.broadcasted_iota(jnp.int32, (QB, QB), 1)
    causal = row >= col
    factor = SCORE_SCALE * LOG2E

    def send_out(h):
        own_out(h).start()
        for c in (1, 3, 2):
            out_copy(h, c).start()

    @pl.loop(0, heads)
    def _(head):
        own_grad(head).wait()
        for c in (1, 3, 2):
            grad_arrival(head, c).wait_recv()
        head_lanes = pl.ds(pl.multiple_of(head * HD, HD), HD)

        for i in range(blocks):
            own_rows = slice(i * QB, (i + 1) * QB)
            q = q_buf[head, own_rows, :]
            grad = g_buf[head, own_rows, :]
            grad_t = grad.T
            scores = []
            for j in range(i + 1):
                s = dot_nt(q, k_scr[j * QB : (j + 1) * QB, :])
                if j == i:
                    s = jnp.where(causal, s, -1e30)
                scores.append(s)
            top = functools.reduce(jnp.maximum, scores)
            top = jnp.max(top, axis=-1, keepdims=True) * factor
            weights = [jnp.exp2(s * factor - top) for s in scores]
            whole = jnp.sum(functools.reduce(jnp.add, weights), axis=-1, keepdims=True)
            inverse = 1.0 / whole
            probs = [w * inverse for w in weights]
            rounded = [p.astype(jnp.bfloat16) for p in probs]
            attended = functools.reduce(
                jnp.add, [dot_nn(rounded[j], v_scr[j * QB : (j + 1) * QB, :]) for j in range(i + 1)]
            )
            o_buf[head, own_rows, :] = attended.astype(jnp.bfloat16)
            prods = []
            for j in range(i + 1):
                keys = slice(j * QB, (j + 1) * QB)
                dp = dot_nt(grad, v_scr[keys, :])
                prods.append(probs[j] * dp)
                dv_scr[:, keys] += dot_nn(grad_t, rounded[j])
            inner = jnp.sum(functools.reduce(jnp.add, prods), axis=-1, keepdims=True)
            ds = [(prods[j] - probs[j] * inner).astype(jnp.bfloat16) for j in range(i + 1)]
            dq = functools.reduce(
                jnp.add, [dot_nn(ds[j], k_scr[j * QB : (j + 1) * QB, :]) for j in range(i + 1)]
            )
            dq = (dq * SCORE_SCALE).astype(jnp.bfloat16).astype(jnp.float32)
            dq_all[own_rows, head_lanes] = rotate(dq, cos_ref[own_rows, :], -sin_ref[own_rows, :]).astype(
                jnp.bfloat16
            )


        @pl.when(head >= LAG)
        def _():
            send_out(head - LAG)

    dv = dv_scr[...].T.astype(jnp.bfloat16)
    mid = jnp.concatenate([dot_nt(dq_all[...], qup_ref[...]), dot_nt(dv, vup_ref[...])], 1)
    mid_t = mid.T
    for b in range(4):
        mid_scr[b] = mid_t[:, b * rows : (b + 1) * rows]

    def mid_copy(c):
        return remote(
            mid_scr.at[lax.rem(me.y + c, 4)],
            mid_recv.at[c - 1],
            m_send.at[c - 1],
            m_recv.at[c - 1],
            me.along(c),
        )

    def mid_share(c):
        return remote(
            mid_all.at[me.y], mid_all.at[me.y], m_send.at[2 + c], m_recv.at[2 + c], me.along(c)
        )

    def mid_other(c):
        ref = mid_all.at[lax.rem(me.y + 4 - c, 4)]
        return remote(ref, ref, m_send.at[2 + c], m_recv.at[2 + c], me.along(c))

    for c in (1, 3, 2):
        mid_copy(c).start()
    for n in range(4):
        up = dot_nn(down_t[:RANK, :], dq_all[:, n * 256 : (n + 1) * 256])
        for h in range(2):
            up_part[0, 2 * n + h] = up[:8, h * HD : (h + 1) * HD]
            up_part[1, 2 * n + h] = up[8:, h * HD : (h + 1) * HD]
    up = dot_nn(down_t[RANK:, :], dv)
    up_part[0, heads] = up[:8]
    up_part[1, heads] = up[8:]
    for c in (1, 3, 2):
        mid_copy(c).wait_recv()
    mid_all[me.y] = (mid_scr[me.y] + mid_recv[0] + mid_recv[1] + mid_recv[2]).astype(jnp.bfloat16)
    for c in (1, 3, 2):
        mid_share(c).start()

    @pl.loop(heads - LAG, heads)
    def _(h):
        send_out(h)

    for c in (1, 3, 2):
        mid_other(c).wait_recv()

    def partial(half):
        made = dot_nn(mid_all[0], x_buf[0, 2 * me.y + half])
        for b in range(1, 4):
            made += dot_nn(mid_all[b], x_buf[b, 2 * me.y + half])
        for r in range(2):
            for k in range(8):
                part[half, r * 8 + k] = made[r * 16 : (r + 1) * 16, k * HD : (k + 1) * HD]

    partial(1 - me.core)
    swap = remote(part.at[1 - me.core], part_recv, c_send.at[0], c_recv.at[0], me.partner())
    up_swap = remote(up_part.at[1 - me.core], up_recv, c_send.at[1], c_recv.at[1], me.partner())
    swap.start()
    up_swap.start()
    partial(me.core)
    up_swap.wait_recv()
    swap.wait_recv()
    total[:, :16] = part[me.core] + part_recv[...]
    total[:, 16:] = up_part[me.core] + up_recv[...]

    for n, (a, b) in enumerate(AROUND[:-1]):
        dp, fs = me.plane(me.core, a, b)
        remote(
            total.at[lax.div(dp, 2) * 8 + fs],
            rs_recv.at[n],
            r_send.at[0],
            r_recv.at[0],
            (dp, fs, me.y),
        ).start()

    many = remote(rs_recv, rs_recv, r_send.at[0], r_recv.at[0], me.partner())
    many.wait_recv()
    summed = total[plane]
    for o in range(PLANE - 1):
        summed += rs_recv[o]
    final[...] = (ADAPTER_SCALE * summed[:16]).astype(jnp.bfloat16)
    up_final[...] = summed[16:]

    at_rows = pl.ds(pl.multiple_of(lax.div(plane, 8) * 16, 16), 16)
    at_cols = pl.ds(pl.multiple_of(lax.rem(plane, 8) * HD, HD), HD)
    up_cols = pl.ds(pl.multiple_of(plane * HD, HD), HD)

    for a, b in AROUND:
        near = me.plane(me.core, a, b)
        for c in (2, 1, 3, 0):
            if a or b or c:
                remote(
                    final,
                    res.at[me.core, me.y, at_rows, at_cols],
                    r_send.at[1],
                    r_recv.at[1],
                    (*near, lax.rem(me.y + c, 4)),
                ).start()
    for a, b in AROUND[:-1]:
        remote(
            up_final, up_res.at[me.core, :, up_cols], r_send.at[2], r_recv.at[2], me.near(a, b)
        ).start()

    res[me.core, me.y, at_rows, at_cols] = final[...]
    up_res[me.core, :, up_cols] = up_final[...]
    all_of = remote(ag_size, ag_size, r_send.at[1], r_recv.at[1], me.partner())
    up_size = rs_recv.at[:, pl.ds(0, 8)]
    up_all = remote(up_size, up_size, r_send.at[2], r_recv.at[2], me.partner())
    up_all.wait_recv()
    up_half = remote(
        up_res.at[me.core], up_res.at[me.core], c_send.at[2], c_recv.at[2], me.partner()
    )
    up_half.start()
    all_of.wait_recv()
    half = remote(res.at[me.core], res.at[me.core], c_send.at[3], c_recv.at[3], me.partner())
    half.start()

    def grad_a_writes(b, first):
        copies = []
        for yy in range(4):
            cols_out = pl.ds(pl.multiple_of(yy * 2048 + b * 1024, 1024), 1024)
            for i, dst in enumerate((ga_q_hbm, ga_v_hbm)):
                copies.append(
                    pltpu.make_async_copy(
                        res.at[b, yy, pl.ds(i * RANK, RANK)],
                        dst.at[:, cols_out],
                        write_sem.at[first + yy * 2 + i],
                    )
                )
        return copies

    def grad_b_writes(b, first):
        eight = pl.ds(pl.multiple_of(b * 8, 8), 8)
        return [
            pltpu.make_async_copy(
                up_res.at[b, :, pl.ds(0, group + HD)], gb_hbm.at[eight], write_sem.at[first]
            )
        ]

    writes = grad_a_writes(me.core, 0) + grad_b_writes(me.core, 8)
    for copy in writes:
        copy.start()
    @pl.loop(0, heads)
    def _(h):
        own_out(h).wait()
        for c in (1, 3, 2):
            grad_copy(h, c).wait_send()
            out_copy(h, c).wait_send()
            out_arrival(h, c).wait_recv()

    for copy in sends:
        copy.wait_send()
    up_other = up_res.at[1 - me.core]
    remote(up_other, up_other, c_send.at[2], c_recv.at[2], me.partner()).wait_recv()
    other = res.at[1 - me.core]
    remote(other, other, c_send.at[3], c_recv.at[3], me.partner()).wait_recv()
    late = grad_a_writes(1 - me.core, 10) + grad_b_writes(1 - me.core, 18)
    for copy in late:
        copy.start()
    for c in (1, 3, 2):
        mid_copy(c).wait_send()
        mid_share(c).wait_send()
    for copy in (up_swap, swap, many, all_of, up_all, up_half, half):
        copy.wait_send()
    for copy in writes + late:
        copy.wait()


def fused_step(tokens, gain, w_qkv, aq_t, av_t, qup, vup, cos, sin, out_grad):
    rows, width = tokens.shape
    shard, cols = w_qkv.shape
    heads = QUERY_PER_KV
    seq = 4 * rows
    wide = width // CHUNKS
    anywhere = pl.BlockSpec(memory_space=pl.ANY)
    dma = pltpu.SemaphoreType.DMA
    f32, bf16 = jnp.float32, jnp.bfloat16
    return pl.pallas_call(
        functools.partial(step_kernel, rows),
        in_specs=[anywhere] * 10,
        out_specs=[anywhere] * 4,
        out_shape=[
            jax.ShapeDtypeStruct((rows, 4 * heads * HD), bf16),
            jax.ShapeDtypeStruct((RANK, width), bf16),
            jax.ShapeDtypeStruct((RANK, width), bf16),
            jax.ShapeDtypeStruct((RANK, (heads + 1) * HD), f32),
        ],
        scratch_shapes=[
            pltpu.VMEM((rows, width), bf16),
            pltpu.VMEM((rows, 128), f32),
            pltpu.VMEM((4, CHUNKS, rows, wide), bf16),
            pltpu.VMEM((width, cols), bf16),
            pltpu.VMEM((seq, cols), f32),
            pltpu.VMEM((seq, 2 * RANK), f32),
            pltpu.VMEM((1, width), f32),
            pltpu.VMEM((2 * RANK, width), bf16),
            pltpu.VMEM((RANK, heads * HD), bf16),
            pltpu.VMEM((RANK, HD), bf16),
            pltpu.VMEM((seq, HD), f32),
            pltpu.VMEM((seq, HD), f32),
            pltpu.VMEM((rows, 4 * heads * HD), bf16),
            pltpu.VMEM((heads, seq, HD), bf16),
            pltpu.VMEM((seq, HD), bf16),
            pltpu.VMEM((seq, HD), bf16),
            pltpu.VMEM((seq, 2 * RANK), bf16),
            pltpu.VMEM((2 * RANK, seq), bf16),
            pltpu.VMEM((HD, seq), f32),
            pltpu.VMEM((seq, heads * HD), bf16),
            pltpu.VMEM((4, 2 * RANK, rows), f32),
            pltpu.VMEM((3, 2 * RANK, rows), f32),
            pltpu.VMEM((4, 2 * RANK, rows), bf16),
            pltpu.VMEM((heads, seq, HD), bf16),
            pltpu.VMEM((heads, seq, HD), bf16),
            pltpu.VMEM((2, PLANE, 16, HD), f32),
            pltpu.VMEM((PLANE, 16, HD), f32),
            pltpu.VMEM((2, PLANE, 8, HD), f32),
            pltpu.VMEM((PLANE, 8, HD), f32),
            pltpu.VMEM((PLANE, 24, HD), f32),
            pltpu.VMEM((PLANE - 1, 24, HD), f32),
            pltpu.VMEM((16, HD), bf16),
            pltpu.VMEM((8, HD), f32),
            pltpu.VMEM((2, 4, 2 * RANK, 1024), bf16),
            pltpu.VMEM((2, 8, PLANE * HD), f32),
            pltpu.VMEM((CHIPS - 1, 16, HD), bf16),
            dma((4,)),
            dma((8,)),
            dma(()),
            dma((5, 4)),
            dma((5, 4)),
            dma((16,)),
            dma((16,)),
            dma((3, CHUNKS)),
            dma((3, CHUNKS)),
            dma((heads,)),
            dma((heads,)),
            dma((heads, 3)),
            dma((heads, 3)),
            dma((heads, 3)),
            dma((heads, 3)),
            dma((6,)),
            dma((6,)),
            dma((4,)),
            dma((4,)),
            dma((3,)),
            dma((3,)),
            dma((20,)),
        ],
        compiler_params=pltpu.CompilerParams(
            collective_id=1, has_side_effects=True, vmem_limit_bytes=63 << 20
        ),
        cost_estimate=pl.CostEstimate(
            flops=2 * seq * width * cols,
            bytes_accessed=10 * 1000 * 1000,
            transcendentals=heads * seq * seq,
        ),
        name="fused_step",
    )(tokens, gain.reshape(1, width), w_qkv, aq_t, av_t, qup, vup, cos, sin, out_grad)


def local(tokens, norm_gain, w_qkv, a_query, query_up_adapter, a_value, value_up_adapter, out_grad):
    cos, sin = rotary_tables(4 * tokens.shape[1])
    out_rows, ga_query, ga_value, grad_b = fused_step(
        tokens[0],
        norm_gain,
        w_qkv,
        a_query.T,
        a_value.T,
        query_up_adapter,
        value_up_adapter,
        cos,
        sin,
        out_grad[0],
    )
    return (
        out_rows[None],
        ga_query.T.astype(jnp.float32),
        ADAPTER_SCALE * grad_b[:, : query_up_adapter.shape[1]],
        ga_value.T.astype(jnp.float32),
        ADAPTER_SCALE * grad_b[:, query_up_adapter.shape[1] :],
    )


def solution(mesh):
    return jax.shard_map(
        local,
        mesh=mesh,
        in_specs=(
            P(("dp", "fsdp"), "tensor", None),
            P(),
            P(("dp", "fsdp"), "tensor"),
            P(),
            P(None, "tensor"),
            P(),
            P(None, "tensor"),
            P(("dp", "fsdp"), "tensor", None),
        ),
        out_specs=(
            P(("dp", "fsdp"), "tensor", None),
            P(),
            P(None, "tensor"),
            P(),
            P(None, "tensor"),
        ),
        check_vma=False,
    )
```

```python
import functools
import math

import jax
import jax.numpy as jnp
import numpy as np
from jax import lax
from jax.experimental import pallas as pl
from jax.experimental.pallas import tpu as pltpu
from jax.sharding import PartitionSpec as P

HD = 128
QUERY_PER_KV = 8
RANK = 16
QB = 384

EPSILON = 1e-05
ADAPTER_SCALE = 2.0
ROPE_BASE = 500000.0
SCORE_SCALE = 1.0 / math.sqrt(HD)
LOG2E = 1.4426950408889634


def rotary_tables(sequence_length):
    half_dim = HD // 2
    inv_freq = ROPE_BASE ** (-np.arange(half_dim) / half_dim)
    angles = np.arange(sequence_length)[:, None] * inv_freq
    cosine, sine = np.cos(angles), np.sin(angles)
    return (
        np.concatenate([cosine, cosine], 1).astype(np.float32),
        np.concatenate([-sine, sine], 1).astype(np.float32),
    )


def dot_nt(a, b):
    return lax.dot_general(a, b, (((1,), (1,)), ((), ())), preferred_element_type=jnp.float32)


def dot_nn(a, b):
    return jnp.dot(a, b, preferred_element_type=jnp.float32)


def rotate(x, cos, sin):
    return x * cos + pltpu.roll(x, HD // 2, 1) * sin


MESH = pl.DeviceIdType.MESH
CHUNKS = 16
OFFSETS = (0, 3, 1, 2)


class Place:
    def __init__(self):
        self.dp = lax.axis_index("dp")
        self.fs = lax.axis_index("fsdp")
        self.y = lax.axis_index("tensor")
        self.core = lax.rem(self.dp, 2)
        self.x = lax.div(self.dp, 2) * 2 + lax.rem(self.fs, 2)
        self.z = lax.div(self.fs, 2)

    def ring(self, core):
        first = self.x * (1 - core) + self.z * core
        second = self.z * (1 - core) + self.x * core
        return first, second

    def plane(self, core, a, b):
        first, second = self.ring(core)
        first = lax.rem(first + a, 4)
        second = lax.rem(second + b, 4)
        x = first * (1 - core) + second * core
        z = second * (1 - core) + first * core
        return lax.div(x, 2) * 2 + core, z * 2 + lax.rem(x, 2)

    def near(self, a, b):
        return (*self.plane(self.core, a, b), self.y)

    def along(self, c):
        return (self.dp, self.fs, lax.rem(self.y + c, 4))

    def partner(self):
        return (self.dp + 1 - 2 * self.core, self.fs, self.y)


CHIPS = 64
PLANE = 16
LAG = 4
EARLY = 2
AROUND = sorted(
    ((a, b) for a in range(4) for b in range(4)),
    key=lambda step: -sum(min(n, 4 - n) for n in step),
)


def step_kernel(
    rows,
    tok_hbm,
    gain_hbm,
    w_hbm,
    aq_hbm,
    av_hbm,
    qup_hbm,
    vup_hbm,
    cos_hbm,
    sin_hbm,
    grad_hbm,
    out_hbm,
    ga_q_hbm,
    ga_v_hbm,
    gb_hbm,
    raw,
    scale_scr,
    x_buf,
    w_buf,
    acc,
    down_scr,
    gain_ref,
    adapt_ref,
    qup_ref,
    vup_ref,
    cos_ref,
    sin_ref,
    stage,
    q_buf,
    k_scr,
    v_scr,
    down_b,
    down_t,
    dv_scr,
    dq_all,
    mid_scr,
    mid_recv,
    mid_all,
    g_buf,
    o_buf,
    part,
    part_recv,
    up_part,
    up_recv,
    total,
    rs_recv,
    final,
    up_final,
    res,
    up_res,
    ag_size,
    tok_sem,
    load_sem,
    own_sem,
    w_send,
    w_recv,
    d_send,
    d_recv,
    x_send,
    x_recv,
    own_g_sem,
    o_own_sem,
    g_send,
    g_recv,
    o_send,
    o_recv,
    m_send,
    m_recv,
    c_send,
    c_recv,
    r_send,
    r_recv,
    write_sem,
):
    heads = QUERY_PER_KV
    group = heads * HD
    seq = 4 * rows
    blocks = seq // QB

    me = Place()
    shard = w_hbm.shape[0]
    half_shard = shard // 2
    width = tok_hbm.shape[1]
    wide = width // CHUNKS
    cols = w_hbm.shape[1]
    parts = tok_sem.shape[0]
    span = rows // parts

    def tok_copy(i):
        piece = pl.ds(i * span, span)
        return pltpu.make_async_copy(tok_hbm.at[piece], raw.at[piece], tok_sem.at[i])

    for i in range(parts):
        tok_copy(i).start()

    loads = [
        pltpu.make_async_copy(src, dst, load_sem.at[i])
        for i, (src, dst) in enumerate(
            (
                (gain_hbm, gain_ref),
                (aq_hbm, adapt_ref.at[pl.ds(0, RANK)]),
                (av_hbm, adapt_ref.at[pl.ds(RANK, RANK)]),
                (qup_hbm, qup_ref),
                (vup_hbm, vup_ref),
                (cos_hbm, cos_ref),
                (sin_hbm, sin_ref),
                (grad_hbm, stage),
            )
        )
    ]

    def block(core, a, b):
        dp, fs = me.plane(core, a, b)
        return pl.multiple_of((dp * 8 + fs) * shard, shard)

    own = block(me.core, 0, 0)
    own_copy = pltpu.make_async_copy(w_hbm, w_buf.at[pl.ds(own, shard)], own_sem)
    own_copy.start()

    plane = lax.div(me.dp, 2) * 8 + me.fs

    barrier = pltpu.get_barrier_semaphore()

    neighbours = (
        me.along(1),
        me.along(3),
        me.along(2),
        me.near(1, 0),
        me.near(3, 0),
        me.near(0, 1),
        me.near(0, 3),
        me.partner(),
    )
    for device in neighbours:
        pl.semaphore_signal(barrier, inc=1, device_id=device, device_id_type=MESH)
    for load in loads:
        load.start()

    def lines_of(block):
        return pl.ds(pl.multiple_of(block * rows, rows), rows)

    def columns(block, h):
        return pl.ds(pl.multiple_of(block * group + h * HD, HD), HD)

    def remote(src, dst, send, recv, device):
        return pltpu.make_async_remote_copy(
            src_ref=src,
            dst_ref=dst,
            send_sem=send,
            recv_sem=recv,
            device_id=device,
            device_id_type=MESH,
        )

    def own_grad(h):
        return pltpu.make_async_copy(
            grad_hbm.at[:, columns(me.y, h)], g_buf.at[h, lines_of(me.y)], own_g_sem.at[h]
        )

    def grad_copy(h, c):
        to = lax.rem(me.y + c, 4)
        return remote(
            stage.at[:, columns(to, h)],
            g_buf.at[h, lines_of(me.y)],
            g_send.at[h, c - 1],
            g_recv.at[h, c - 1],
            me.along(c),
        )

    def grad_arrival(h, c):
        ref = g_buf.at[h, lines_of(lax.rem(me.y + 4 - c, 4))]
        return remote(ref, ref, g_send.at[h, c - 1], g_recv.at[h, c - 1], me.along(c))

    def own_out(h):
        return pltpu.make_async_copy(
            o_buf.at[h, lines_of(me.y)], out_hbm.at[:, columns(me.y, h)], o_own_sem.at[h]
        )

    def out_copy(h, c):
        to = lax.rem(me.y + c, 4)
        return remote(
            o_buf.at[h, lines_of(to)],
            out_hbm.at[:, columns(me.y, h)],
            o_send.at[h, c - 1],
            o_recv.at[h, c - 1],
            me.along(c),
        )

    def out_arrival(h, c):
        ref = out_hbm.at[:, columns(lax.rem(me.y + 4 - c, 4), h)]
        return remote(ref, ref, o_send.at[h, c - 1], o_recv.at[h, c - 1], me.along(c))

    sends = []

    def w_copy(a, b, device, kind, way, piece=None, source=None):
        start = block(me.core, a, b)
        size = shard
        if piece is not None:
            start, size = pl.multiple_of(start + piece * half_shard, half_shard), half_shard
        dst = w_buf.at[pl.ds(start, size)]
        return pltpu.make_async_remote_copy(
            src_ref=dst if source is None else source,
            dst_ref=dst,
            send_sem=w_send.at[kind, way],
            recv_sem=w_recv.at[kind, way],
            device_id=device,
            device_id_type=MESH,
        )

    def w_start(*args, **kwargs):
        copy = w_copy(*args, **kwargs)
        copy.start()
        sends.append(copy)

    def d_copy(core, event, a, b, source=None):
        dst = w_buf.at[pl.ds(block(core, a, b), shard)]
        return pltpu.make_async_remote_copy(
            src_ref=dst if source is None else source,
            dst_ref=dst,
            send_sem=d_send.at[event],
            recv_sem=d_recv.at[event],
            device_id=me.partner(),
            device_id_type=MESH,
        )

    order = []

    def share(a, b, source=None):
        copy = d_copy(me.core, len(order), a, b, source)
        copy.start()
        sends.append(copy)
        order.append((a, b))

    for i in range(parts):
        tok_copy(i).wait()

        @pl.loop(0, span // 16)
        def _(r):
            piece = pl.ds(pl.multiple_of(i * span + r * 16, 16), 16)
            squares = jnp.zeros((16, wide), jnp.float32)
            for c in range(CHUNKS):
                value = raw[piece, c * wide : (c + 1) * wide].astype(jnp.float32)
                squares = squares + value * value
            mean = jnp.sum(squares, axis=-1, keepdims=True) * (1.0 / width)
            scale_scr[piece, :] = jnp.broadcast_to(lax.rsqrt(mean + EPSILON), (16, 128))

    def x_copy(row_block, chunk, device, way):
        ref = x_buf.at[row_block, chunk]
        return pltpu.make_async_remote_copy(
            src_ref=ref,
            dst_ref=ref,
            send_sem=x_send.at[way, chunk],
            recv_sem=x_recv.at[way // 2 * 2 if way > 1 else way, chunk],
            device_id=device,
            device_id_type=MESH,
        )

    def normalize_chunk(c):
        @pl.loop(0, rows // 16)
        def _(r):
            piece = pl.ds(pl.multiple_of(r * 16, 16), 16)
            scale = scale_scr[piece, :]
            for k in range(wide // 128):
                lanes = slice(c * wide + k * 128, c * wide + (k + 1) * 128)
                value = raw[piece, lanes].astype(jnp.float32)
                x_buf[me.y, c, piece, k * 128 : (k + 1) * 128] = (
                    value * scale * gain_ref[:, lanes]
                ).astype(jnp.bfloat16)

    def x_start(row_block, chunk, device, way):
        copy = x_copy(row_block, chunk, device, way)
        copy.start()
        sends.append(copy)

    middle = CHUNKS // 2
    loads[0].wait()
    normalize_chunk(0)
    normalize_chunk(middle)
    pl.semaphore_wait(barrier, len(neighbours))

    w_start(0, 0, me.near(1, 0), 4, 0, source=w_hbm)
    w_start(0, 0, me.near(3, 0), 4, 1, source=w_hbm)
    w_start(0, 0, me.near(0, 1), 0, 0, source=w_hbm)
    w_start(0, 0, me.near(0, 3), 0, 1, source=w_hbm)
    share(0, 0, source=w_hbm)

    for c in range(middle):
        x_start(me.y, c, me.along(1), 0)
        x_start(me.y, c + middle, me.along(3), 1)
        if c + 1 < middle:
            normalize_chunk(c + 1)
            normalize_chunk(c + 1 + middle)
    for c in range(middle):
        x_start(me.y, c + middle, me.along(1), 0)
        x_start(me.y, c, me.along(3), 1)

    acc[...] = jnp.zeros_like(acc)
    down_scr[...] = jnp.zeros_like(down_scr)

    dv_scr[...] = jnp.zeros_like(dv_scr)
    up_part[...] = jnp.zeros_like(up_part)
    for load in loads[1:]:
        load.wait()

    def arrived(a, b, kind, way, piece=None):
        w_copy(a, b, me.near(0, 1), kind, way, piece).wait_recv()

    def spread(a, kind):
        w_start(a, 0, me.near(0, 1), kind, 0)
        w_start(a, 0, me.near(0, 3), kind, 1)

    own_copy.wait()
    arrived(3, 0, 4, 0)
    w_start(3, 0, me.near(1, 0), 4, 2, piece=0)
    spread(3, 1)
    share(3, 0)
    arrived(1, 0, 4, 1)
    w_start(1, 0, me.near(3, 0), 4, 3, piece=1)
    spread(1, 2)
    share(1, 0)
    for kind, a in enumerate(OFFSETS):
        if kind == 3:
            arrived(2, 0, 4, 2, piece=0)
            arrived(2, 0, 4, 3, piece=1)
            spread(2, 3)
            share(2, 0)
        arrived(a, 3, kind, 0)
        w_start(a, 3, me.near(0, 1), kind, 2, piece=0)
        share(a, 3)
        arrived(a, 1, kind, 1)
        w_start(a, 1, me.near(0, 3), kind, 3, piece=1)
        share(a, 1)
        if kind > 0:
            before = OFFSETS[kind - 1]
            arrived(before, 2, kind - 1, 2, piece=0)
            arrived(before, 2, kind - 1, 3, piece=1)
            share(before, 2)
    arrived(OFFSETS[3], 2, 3, 2, piece=0)
    arrived(OFFSETS[3], 2, 3, 3, piece=1)
    share(OFFSETS[3], 2)

    minus = lax.rem(me.y + 3, 4)
    plus = lax.rem(me.y + 1, 4)
    far = lax.rem(me.y + 2, 4)
    for c in range(middle):
        x_copy(minus, c, me.along(1), 0).wait_recv()
        x_start(minus, c, me.along(1), 2)
        x_copy(plus, c + middle, me.along(1), 1).wait_recv()
        x_start(plus, c + middle, me.along(3), 2)

    def send_grads(first, last):
        @pl.loop(first, last)
        def _(h):
            for c in (1, 3, 2):
                grad_copy(h, c).start()

    @pl.loop(0, heads)
    def _(h):
        own_grad(h).start()

    send_grads(0, EARLY)

    for event, (a, b) in enumerate(order):
        d_copy(1 - me.core, event, a, b).wait_recv()

    def multiply(row_block, chunk):
        value = x_buf[row_block, chunk]
        lines = pl.ds(pl.multiple_of(row_block * rows, rows), rows)
        depth = pl.ds(pl.multiple_of(chunk * wide, wide), wide)
        for n in range(cols // 256):
            lanes = slice(n * 256, (n + 1) * 256)
            acc[lines, lanes] += dot_nn(value, w_buf[depth, lanes])
        down_scr[lines, :] += dot_nt(value, adapt_ref[:, depth])

    def prepare(row_block):
        lines = pl.ds(pl.multiple_of(row_block * rows, rows), rows)
        down = down_scr[lines, :].astype(jnp.bfloat16)
        down_b[lines, :] = down
        cos, sin = cos_ref[lines, :], sin_ref[lines, :]
        for h in range(heads):
            lanes = slice(h * HD, (h + 1) * HD)
            value = acc[lines, lanes] + ADAPTER_SCALE * dot_nn(down[:, :RANK], qup_ref[:, lanes])
            value = value.astype(jnp.bfloat16).astype(jnp.float32)
            q_buf[h, lines, :] = rotate(value, cos, sin).astype(jnp.bfloat16)
        value = acc[lines, group : group + HD].astype(jnp.bfloat16).astype(jnp.float32)
        k_scr[lines, :] = rotate(value, cos, sin).astype(jnp.bfloat16)
        v_scr[lines, :] = (
            acc[lines, group + HD :] + ADAPTER_SCALE * dot_nn(down[:, RANK:], vup_ref[...])
        ).astype(jnp.bfloat16)

    @pl.loop(0, CHUNKS)
    def _(c):
        multiply(me.y, c)

    @pl.loop(0, CHUNKS)
    def _(c):
        @pl.when(c >= middle)
        def _():
            x_copy(minus, c, me.along(1), 0).wait_recv()

        multiply(minus, c)

    @pl.loop(0, CHUNKS)
    def _(c):
        @pl.when(c < middle)
        def _():
            x_copy(plus, c, me.along(1), 1).wait_recv()

        multiply(plus, c)

    @pl.loop(0, 3)
    def _(c):
        prepare(lax.rem(me.y + 3 + c, 4))

    @pl.loop(0, middle)
    def _(c):
        x_copy(far, c, me.along(1), 2).wait_recv()
        multiply(far, c)
        x_copy(far, c + middle, me.along(1), 2).wait_recv()
        multiply(far, c + middle)

    send_grads(EARLY, heads)
    prepare(far)
    down_t[...] = down_b[...].astype(jnp.float32).T.astype(jnp.bfloat16)

    row = lax.broadcasted_iota(jnp.int32, (QB, QB), 0)
    col = lax.broadcasted_iota(jnp.int32, (QB, QB), 1)
    causal = row >= col
    factor = SCORE_SCALE * LOG2E

    def send_out(h):
        own_out(h).start()
        for c in (1, 3, 2):
            out_copy(h, c).start()

    @pl.loop(0, heads)
    def _(head):
        own_grad(head).wait()
        for c in (1, 3, 2):
            grad_arrival(head, c).wait_recv()
        head_lanes = pl.ds(pl.multiple_of(head * HD, HD), HD)

        for i in range(blocks):
            own_rows = slice(i * QB, (i + 1) * QB)
            q = q_buf[head, own_rows, :]
            grad = g_buf[head, own_rows, :]
            grad_t = grad.T
            scores = []
            for j in range(i + 1):
                s = dot_nt(q, k_scr[j * QB : (j + 1) * QB, :])
                if j == i:
                    s = jnp.where(causal, s, -1e30)
                scores.append(s)
            top = functools.reduce(jnp.maximum, scores)
            top = jnp.max(top, axis=-1, keepdims=True) * factor
            weights = [jnp.exp2(s * factor - top) for s in scores]
            whole = jnp.sum(functools.reduce(jnp.add, weights), axis=-1, keepdims=True)
            inverse = 1.0 / whole
            probs = [w * inverse for w in weights]
            rounded = [p.astype(jnp.bfloat16) for p in probs]
            attended = functools.reduce(
                jnp.add, [dot_nn(rounded[j], v_scr[j * QB : (j + 1) * QB, :]) for j in range(i + 1)]
            )
            o_buf[head, own_rows, :] = attended.astype(jnp.bfloat16)
            prods = []
            for j in range(i + 1):
                keys = slice(j * QB, (j + 1) * QB)
                dp = dot_nt(grad, v_scr[keys, :])
                prods.append(probs[j] * dp)
                dv_scr[:, keys] += dot_nn(grad_t, rounded[j])
            inner = jnp.sum(functools.reduce(jnp.add, prods), axis=-1, keepdims=True)
            ds = [(prods[j] - probs[j] * inner).astype(jnp.bfloat16) for j in range(i + 1)]
            dq = functools.reduce(
                jnp.add, [dot_nn(ds[j], k_scr[j * QB : (j + 1) * QB, :]) for j in range(i + 1)]
            )
            dq = (dq * SCORE_SCALE).astype(jnp.bfloat16).astype(jnp.float32)
            dq_all[own_rows, head_lanes] = rotate(dq, cos_ref[own_rows, :], -sin_ref[own_rows, :]).astype(
                jnp.bfloat16
            )


        @pl.when(head >= LAG)
        def _():
            send_out(head - LAG)

    dv = dv_scr[...].T.astype(jnp.bfloat16)
    mid = jnp.concatenate([dot_nt(dq_all[...], qup_ref[...]), dot_nt(dv, vup_ref[...])], 1)
    mid_t = mid.T
    for b in range(4):
        mid_scr[b] = mid_t[:, b * rows : (b + 1) * rows]

    def mid_copy(c):
        return remote(
            mid_scr.at[lax.rem(me.y + c, 4)],
            mid_recv.at[c - 1],
            m_send.at[c - 1],
            m_recv.at[c - 1],
            me.along(c),
        )

    def mid_share(c):
        return remote(
            mid_all.at[me.y], mid_all.at[me.y], m_send.at[2 + c], m_recv.at[2 + c], me.along(c)
        )

    def mid_other(c):
        ref = mid_all.at[lax.rem(me.y + 4 - c, 4)]
        return remote(ref, ref, m_send.at[2 + c], m_recv.at[2 + c], me.along(c))

    for c in (1, 3, 2):
        mid_copy(c).start()
    for n in range(4):
        up = dot_nn(down_t[:RANK, :], dq_all[:, n * 256 : (n + 1) * 256])
        for h in range(2):
            up_part[0, 2 * n + h] = up[:8, h * HD : (h + 1) * HD]
            up_part[1, 2 * n + h] = up[8:, h * HD : (h + 1) * HD]
    up = dot_nn(down_t[RANK:, :], dv)
    up_part[0, heads] = up[:8]
    up_part[1, heads] = up[8:]
    for c in (1, 3, 2):
        mid_copy(c).wait_recv()
    mid_all[me.y] = (mid_scr[me.y] + mid_recv[0] + mid_recv[1] + mid_recv[2]).astype(jnp.bfloat16)
    for c in (1, 3, 2):
        mid_share(c).start()

    send_out(4)
    for c in (1, 3, 2):
        mid_other(c).wait_recv()

    def partial(half):
        for n in range(2):
            chunk = 4 * me.y + 2 * half + n
            made = dot_nn(mid_all[0], x_buf[0, chunk])
            for b in range(1, 4):
                made += dot_nn(mid_all[b], x_buf[b, chunk])
            for r in range(2):
                for k in range(4):
                    part[half, r * 8 + n * 4 + k] = made[
                        r * 16 : (r + 1) * 16, k * HD : (k + 1) * HD
                    ]

    partial(1 - me.core)
    swap = remote(part.at[1 - me.core], part_recv, c_send.at[0], c_recv.at[0], me.partner())
    up_swap = remote(up_part.at[1 - me.core], up_recv, c_send.at[1], c_recv.at[1], me.partner())
    swap.start()
    up_swap.start()
    partial(me.core)
    up_swap.wait_recv()
    swap.wait_recv()
    total[:, :16] = part[me.core] + part_recv[...]
    total[:, 16:] = up_part[me.core] + up_recv[...]

    for n, (a, b) in enumerate(AROUND[:-1]):
        dp, fs = me.plane(me.core, a, b)
        remote(
            total.at[lax.div(dp, 2) * 8 + fs],
            rs_recv.at[n],
            r_send.at[0],
            r_recv.at[0],
            (dp, fs, me.y),
        ).start()

    send_out(5)
    send_out(6)
    many = remote(rs_recv, rs_recv, r_send.at[0], r_recv.at[0], me.partner())
    many.wait_recv()
    summed = total[plane]
    for o in range(PLANE - 1):
        summed += rs_recv[o]
    final[...] = (ADAPTER_SCALE * summed[:16]).astype(jnp.bfloat16)
    up_final[...] = ADAPTER_SCALE * summed[16:]

    at_rows = pl.ds(pl.multiple_of(lax.div(plane, 8) * 16, 16), 16)
    at_cols = pl.ds(pl.multiple_of(lax.rem(plane, 8) * HD, HD), HD)
    up_cols = pl.ds(pl.multiple_of(plane * HD, HD), HD)

    for a, b in AROUND:
        near = me.plane(me.core, a, b)
        for c in (2, 1, 3, 0):
            if a or b or c:
                remote(
                    final,
                    res.at[me.core, me.y, at_rows, at_cols],
                    r_send.at[1],
                    r_recv.at[1],
                    (*near, lax.rem(me.y + c, 4)),
                ).start()
    for a, b in AROUND[:-1]:
        remote(
            up_final, up_res.at[me.core, :, up_cols], r_send.at[2], r_recv.at[2], me.near(a, b)
        ).start()

    send_out(7)
    res[me.core, me.y, at_rows, at_cols] = final[...]
    up_res[me.core, :, up_cols] = up_final[...]
    all_of = remote(ag_size, ag_size, r_send.at[1], r_recv.at[1], me.partner())
    up_size = rs_recv.at[:, pl.ds(0, 8)]
    up_all = remote(up_size, up_size, r_send.at[2], r_recv.at[2], me.partner())
    up_all.wait_recv()
    up_half = remote(
        up_res.at[me.core], up_res.at[me.core], c_send.at[2], c_recv.at[2], me.partner()
    )
    up_half.start()
    all_of.wait_recv()
    half = remote(res.at[me.core], res.at[me.core], c_send.at[3], c_recv.at[3], me.partner())
    half.start()

    def grad_a_writes(b, first):
        copies = []
        for yy in range(4):
            cols_out = pl.ds(pl.multiple_of(yy * 2048 + b * 1024, 1024), 1024)
            for i, dst in enumerate((ga_q_hbm, ga_v_hbm)):
                copies.append(
                    pltpu.make_async_copy(
                        res.at[b, yy, pl.ds(i * RANK, RANK)],
                        dst.at[:, cols_out],
                        write_sem.at[first + yy * 2 + i],
                    )
                )
        return copies

    def grad_b_writes(b, first):
        eight = pl.ds(pl.multiple_of(b * 8, 8), 8)
        return [
            pltpu.make_async_copy(
                up_res.at[b, :, pl.ds(0, group + HD)], gb_hbm.at[eight], write_sem.at[first]
            )
        ]

    writes = grad_a_writes(me.core, 0) + grad_b_writes(me.core, 8)
    for copy in writes:
        copy.start()
    @pl.loop(0, heads)
    def _(h):
        own_out(h).wait()
        for c in (1, 3, 2):
            grad_copy(h, c).wait_send()
            out_copy(h, c).wait_send()
            out_arrival(h, c).wait_recv()

    for copy in sends:
        copy.wait_send()
    up_other = up_res.at[1 - me.core]
    remote(up_other, up_other, c_send.at[2], c_recv.at[2], me.partner()).wait_recv()
    other = res.at[1 - me.core]
    remote(other, other, c_send.at[3], c_recv.at[3], me.partner()).wait_recv()
    late = grad_a_writes(1 - me.core, 10) + grad_b_writes(1 - me.core, 18)
    for copy in late:
        copy.start()
    for c in (1, 3, 2):
        mid_copy(c).wait_send()
        mid_share(c).wait_send()
    for copy in (up_swap, swap, many, all_of, up_all, up_half, half):
        copy.wait_send()
    for copy in writes + late:
        copy.wait()


def fused_step(tokens, gain, w_qkv, aq_t, av_t, qup, vup, cos, sin, out_grad):
    rows, width = tokens.shape
    shard, cols = w_qkv.shape
    heads = QUERY_PER_KV
    seq = 4 * rows
    wide = width // CHUNKS
    anywhere = pl.BlockSpec(memory_space=pl.ANY)
    dma = pltpu.SemaphoreType.DMA
    f32, bf16 = jnp.float32, jnp.bfloat16
    return pl.pallas_call(
        functools.partial(step_kernel, rows),
        in_specs=[anywhere] * 10,
        out_specs=[anywhere] * 4,
        out_shape=[
            jax.ShapeDtypeStruct((rows, 4 * heads * HD), bf16),
            jax.ShapeDtypeStruct((RANK, width), bf16),
            jax.ShapeDtypeStruct((RANK, width), bf16),
            jax.ShapeDtypeStruct((RANK, (heads + 1) * HD), f32),
        ],
        scratch_shapes=[
            pltpu.VMEM((rows, width), bf16),
            pltpu.VMEM((rows, 128), f32),
            pltpu.VMEM((4, CHUNKS, rows, wide), bf16),
            pltpu.VMEM((width, cols), bf16),
            pltpu.VMEM((seq, cols), f32),
            pltpu.VMEM((seq, 2 * RANK), f32),
            pltpu.VMEM((1, width), f32),
            pltpu.VMEM((2 * RANK, width), bf16),
            pltpu.VMEM((RANK, heads * HD), bf16),
            pltpu.VMEM((RANK, HD), bf16),
            pltpu.VMEM((seq, HD), f32),
            pltpu.VMEM((seq, HD), f32),
            pltpu.VMEM((rows, 4 * heads * HD), bf16),
            pltpu.VMEM((heads, seq, HD), bf16),
            pltpu.VMEM((seq, HD), bf16),
            pltpu.VMEM((seq, HD), bf16),
            pltpu.VMEM((seq, 2 * RANK), bf16),
            pltpu.VMEM((2 * RANK, seq), bf16),
            pltpu.VMEM((HD, seq), f32),
            pltpu.VMEM((seq, heads * HD), bf16),
            pltpu.VMEM((4, 2 * RANK, rows), f32),
            pltpu.VMEM((3, 2 * RANK, rows), f32),
            pltpu.VMEM((4, 2 * RANK, rows), bf16),
            pltpu.VMEM((heads, seq, HD), bf16),
            pltpu.VMEM((heads, seq, HD), bf16),
            pltpu.VMEM((2, PLANE, 16, HD), f32),
            pltpu.VMEM((PLANE, 16, HD), f32),
            pltpu.VMEM((2, PLANE, 8, HD), f32),
            pltpu.VMEM((PLANE, 8, HD), f32),
            pltpu.VMEM((PLANE, 24, HD), f32),
            pltpu.VMEM((PLANE - 1, 24, HD), f32),
            pltpu.VMEM((16, HD), bf16),
            pltpu.VMEM((8, HD), f32),
            pltpu.VMEM((2, 4, 2 * RANK, 1024), bf16),
            pltpu.VMEM((2, 8, PLANE * HD), f32),
            pltpu.VMEM((CHIPS - 1, 16, HD), bf16),
            dma((4,)),
            dma((8,)),
            dma(()),
            dma((5, 4)),
            dma((5, 4)),
            dma((16,)),
            dma((16,)),
            dma((3, CHUNKS)),
            dma((3, CHUNKS)),
            dma((heads,)),
            dma((heads,)),
            dma((heads, 3)),
            dma((heads, 3)),
            dma((heads, 3)),
            dma((heads, 3)),
            dma((6,)),
            dma((6,)),
            dma((4,)),
            dma((4,)),
            dma((3,)),
            dma((3,)),
            dma((20,)),
        ],
        compiler_params=pltpu.CompilerParams(
            collective_id=1, has_side_effects=True, vmem_limit_bytes=63 << 20
        ),
        cost_estimate=pl.CostEstimate(
            flops=2 * seq * width * cols,
            bytes_accessed=10 * 1000 * 1000,
            transcendentals=heads * seq * seq,
        ),
        name="fused_step",
    )(tokens, gain.reshape(1, width), w_qkv, aq_t, av_t, qup, vup, cos, sin, out_grad)


def finish_kernel(
    out_in, gq_in, gv_in, gb_in, out, gq, gv, bq, bv, rows, aq, av, fq, fv, b_buf, in_sem, out_sem
):
    parts = 4
    size = rows.shape[0] // parts
    cols = bq.shape[1]
    small = [
        pltpu.make_async_copy(src, dst, in_sem.at[parts + i])
        for i, (src, dst) in enumerate(((gq_in, aq), (gv_in, av), (gb_in, b_buf)))
    ]
    large = [
        pltpu.make_async_copy(
            out_in.at[pl.ds(i * size, size)], rows.at[pl.ds(i * size, size)], in_sem.at[i]
        )
        for i in range(parts)
    ]
    for copy in small + large:
        copy.start()
    writes = []

    def write(src, dst):
        copy = pltpu.make_async_copy(src, dst, out_sem.at[len(writes)])
        copy.start()
        writes.append(copy)

    small[0].wait()
    fq[...] = aq[...].astype(jnp.float32)
    write(fq, gq)
    small[1].wait()
    fv[...] = av[...].astype(jnp.float32)
    write(fv, gv)
    for i in range(parts):
        large[i].wait()
        write(rows.at[pl.ds(i * size, size)], out.at[pl.ds(i * size, size)])
    small[2].wait()
    write(b_buf.at[:, pl.ds(0, cols)], bq)
    write(b_buf.at[:, pl.ds(cols, HD)], bv)
    for copy in writes:
        copy.wait()


def finish(out_rows, ga_query, ga_value, grad_b):
    anywhere = pl.BlockSpec(memory_space=pl.ANY)
    cols = grad_b.shape[1] - HD
    f32 = jnp.float32
    return pl.pallas_call(
        finish_kernel,
        in_specs=[anywhere] * 4,
        out_specs=[anywhere] * 5,
        out_shape=[
            jax.ShapeDtypeStruct(out_rows.shape, out_rows.dtype),
            jax.ShapeDtypeStruct(ga_query.shape, f32),
            jax.ShapeDtypeStruct(ga_value.shape, f32),
            jax.ShapeDtypeStruct((RANK, cols), f32),
            jax.ShapeDtypeStruct((RANK, HD), f32),
        ],
        scratch_shapes=[
            pltpu.VMEM(out_rows.shape, out_rows.dtype),
            pltpu.VMEM(ga_query.shape, ga_query.dtype),
            pltpu.VMEM(ga_value.shape, ga_value.dtype),
            pltpu.VMEM(ga_query.shape, f32),
            pltpu.VMEM(ga_value.shape, f32),
            pltpu.VMEM(grad_b.shape, f32),
            pltpu.SemaphoreType.DMA((7,)),
            pltpu.SemaphoreType.DMA((8,)),
        ],
        name="finish",
    )(out_rows, ga_query, ga_value, grad_b)


def local(tokens, norm_gain, w_qkv, a_query, query_up_adapter, a_value, value_up_adapter, out_grad):
    cos, sin = rotary_tables(4 * tokens.shape[1])
    out_rows, ga_query, ga_value, grad_b = fused_step(
        tokens[0],
        norm_gain,
        w_qkv,
        a_query.T,
        a_value.T,
        query_up_adapter,
        value_up_adapter,
        cos,
        sin,
        out_grad[0],
    )
    out_rows, ga_query, ga_value, gb_query, gb_value = finish(out_rows, ga_query, ga_value, grad_b)
    return out_rows[None], ga_query.T, gb_query, ga_value.T, gb_value


def solution(mesh):
    return jax.shard_map(
        local,
        mesh=mesh,
        in_specs=(
            P(("dp", "fsdp"), "tensor", None),
            P(),
            P(("dp", "fsdp"), "tensor"),
            P(),
            P(None, "tensor"),
            P(),
            P(None, "tensor"),
            P(("dp", "fsdp"), "tensor", None),
        ),
        out_specs=(
            P(("dp", "fsdp"), "tensor", None),
            P(),
            P(None, "tensor"),
            P(),
            P(None, "tensor"),
        ),
        check_vma=False,
    )
```

```python
import functools
import math

import jax
import jax.numpy as jnp
import numpy as np
from jax import lax
from jax.experimental import pallas as pl
from jax.experimental.pallas import tpu as pltpu
from jax.sharding import PartitionSpec as P

HD = 128
QUERY_PER_KV = 8
RANK = 16
QB = 384

EPSILON = 1e-05
ADAPTER_SCALE = 2.0
ROPE_BASE = 500000.0
SCORE_SCALE = 1.0 / math.sqrt(HD)
LOG2E = 1.4426950408889634


def rotary_tables(sequence_length):
    half_dim = HD // 2
    inv_freq = ROPE_BASE ** (-np.arange(half_dim) / half_dim)
    angles = np.arange(sequence_length)[:, None] * inv_freq
    cosine, sine = np.cos(angles), np.sin(angles)
    return (
        np.concatenate([cosine, cosine], 1).astype(np.float32),
        np.concatenate([-sine, sine], 1).astype(np.float32),
    )


def dot_nt(a, b):
    return lax.dot_general(a, b, (((1,), (1,)), ((), ())), preferred_element_type=jnp.float32)


def dot_nn(a, b):
    return jnp.dot(a, b, preferred_element_type=jnp.float32)


def rotate(x, cos, sin):
    return x * cos + pltpu.roll(x, HD // 2, 1) * sin


MESH = pl.DeviceIdType.MESH
CHUNKS = 16
OFFSETS = (0, 3, 1, 2)


class Place:
    def __init__(self):
        self.dp = lax.axis_index("dp")
        self.fs = lax.axis_index("fsdp")
        self.y = lax.axis_index("tensor")
        self.core = lax.rem(self.dp, 2)
        self.x = lax.div(self.dp, 2) * 2 + lax.rem(self.fs, 2)
        self.z = lax.div(self.fs, 2)

    def ring(self, core):
        first = self.x * (1 - core) + self.z * core
        second = self.z * (1 - core) + self.x * core
        return first, second

    def plane(self, core, a, b):
        first, second = self.ring(core)
        first = lax.rem(first + a, 4)
        second = lax.rem(second + b, 4)
        x = first * (1 - core) + second * core
        z = second * (1 - core) + first * core
        return lax.div(x, 2) * 2 + core, z * 2 + lax.rem(x, 2)

    def near(self, a, b):
        return (*self.plane(self.core, a, b), self.y)

    def along(self, c):
        return (self.dp, self.fs, lax.rem(self.y + c, 4))

    def partner(self):
        return (self.dp + 1 - 2 * self.core, self.fs, self.y)


CHIPS = 64
PLANE = 16
LAG = 4
EARLY = 2
AROUND = sorted(
    ((a, b) for a in range(4) for b in range(4)),
    key=lambda step: -sum(min(n, 4 - n) for n in step),
)


def step_kernel(
    rows,
    tok_hbm,
    gain_hbm,
    w_hbm,
    aq_hbm,
    av_hbm,
    qup_hbm,
    vup_hbm,
    cos_hbm,
    sin_hbm,
    grad_hbm,
    out_hbm,
    ga_q_hbm,
    ga_v_hbm,
    gb_hbm,
    raw,
    scale_scr,
    x_buf,
    w_buf,
    acc,
    down_scr,
    gain_ref,
    adapt_ref,
    qup_ref,
    vup_ref,
    cos_ref,
    sin_ref,
    stage,
    q_buf,
    k_scr,
    v_scr,
    down_b,
    down_t,
    dv_scr,
    dq_all,
    mid_scr,
    mid_mine,
    mid_recv,
    mid_all,
    g_buf,
    o_buf,
    part,
    part_recv,
    up_part,
    up_recv,
    total,
    rs_recv,
    final,
    up_final,
    res,
    up_res,
    ag_size,
    tok_sem,
    load_sem,
    own_sem,
    w_send,
    w_recv,
    d_send,
    d_recv,
    x_send,
    x_recv,
    own_g_sem,
    o_own_sem,
    g_send,
    g_recv,
    o_send,
    o_recv,
    m_send,
    m_recv,
    c_send,
    c_recv,
    r_send,
    r_recv,
    write_sem,
):
    heads = QUERY_PER_KV
    group = heads * HD
    seq = 4 * rows
    blocks = seq // QB

    me = Place()
    shard = w_hbm.shape[0]
    half_shard = shard // 2
    width = tok_hbm.shape[1]
    wide = width // CHUNKS
    cols = w_hbm.shape[1]
    parts = tok_sem.shape[0]
    span = rows // parts

    def tok_copy(i):
        piece = pl.ds(i * span, span)
        return pltpu.make_async_copy(tok_hbm.at[piece], raw.at[piece], tok_sem.at[i])

    for i in range(parts):
        tok_copy(i).start()

    loads = [
        pltpu.make_async_copy(src, dst, load_sem.at[i])
        for i, (src, dst) in enumerate(
            (
                (gain_hbm, gain_ref),
                (aq_hbm, adapt_ref.at[pl.ds(0, RANK)]),
                (av_hbm, adapt_ref.at[pl.ds(RANK, RANK)]),
                (qup_hbm, qup_ref),
                (vup_hbm, vup_ref),
                (cos_hbm, cos_ref),
                (sin_hbm, sin_ref),
                (grad_hbm, stage),
            )
        )
    ]

    def block(core, a, b):
        dp, fs = me.plane(core, a, b)
        return pl.multiple_of((dp * 8 + fs) * shard, shard)

    own = block(me.core, 0, 0)
    own_copy = pltpu.make_async_copy(w_hbm, w_buf.at[pl.ds(own, shard)], own_sem)
    own_copy.start()

    plane = lax.div(me.dp, 2) * 8 + me.fs

    barrier = pltpu.get_barrier_semaphore()

    neighbours = (
        me.along(1),
        me.along(3),
        me.along(2),
        me.near(1, 0),
        me.near(3, 0),
        me.near(0, 1),
        me.near(0, 3),
        me.partner(),
    )
    for device in neighbours:
        pl.semaphore_signal(barrier, inc=1, device_id=device, device_id_type=MESH)
    for load in loads:
        load.start()

    def lines_of(block):
        return pl.ds(pl.multiple_of(block * rows, rows), rows)

    def columns(block, h):
        return pl.ds(pl.multiple_of(block * group + h * HD, HD), HD)

    def remote(src, dst, send, recv, device):
        return pltpu.make_async_remote_copy(
            src_ref=src,
            dst_ref=dst,
            send_sem=send,
            recv_sem=recv,
            device_id=device,
            device_id_type=MESH,
        )

    def own_grad(h):
        return pltpu.make_async_copy(
            grad_hbm.at[:, columns(me.y, h)], g_buf.at[h, lines_of(me.y)], own_g_sem.at[h]
        )

    def grad_copy(h, c):
        to = lax.rem(me.y + c, 4)
        return remote(
            stage.at[:, columns(to, h)],
            g_buf.at[h, lines_of(me.y)],
            g_send.at[h, c - 1],
            g_recv.at[h, c - 1],
            me.along(c),
        )

    def grad_arrival(h, c):
        ref = g_buf.at[h, lines_of(lax.rem(me.y + 4 - c, 4))]
        return remote(ref, ref, g_send.at[h, c - 1], g_recv.at[h, c - 1], me.along(c))

    def own_out(h):
        return pltpu.make_async_copy(
            o_buf.at[h, lines_of(me.y)], out_hbm.at[:, columns(me.y, h)], o_own_sem.at[h]
        )

    def out_copy(h, c):
        to = lax.rem(me.y + c, 4)
        return remote(
            o_buf.at[h, lines_of(to)],
            out_hbm.at[:, columns(me.y, h)],
            o_send.at[h, c - 1],
            o_recv.at[h, c - 1],
            me.along(c),
        )

    def out_arrival(h, c):
        ref = out_hbm.at[:, columns(lax.rem(me.y + 4 - c, 4), h)]
        return remote(ref, ref, o_send.at[h, c - 1], o_recv.at[h, c - 1], me.along(c))

    sends = []

    def w_copy(a, b, device, kind, way, piece=None, source=None):
        start = block(me.core, a, b)
        size = shard
        if piece is not None:
            start, size = pl.multiple_of(start + piece * half_shard, half_shard), half_shard
        dst = w_buf.at[pl.ds(start, size)]
        return pltpu.make_async_remote_copy(
            src_ref=dst if source is None else source,
            dst_ref=dst,
            send_sem=w_send.at[kind, way],
            recv_sem=w_recv.at[kind, way],
            device_id=device,
            device_id_type=MESH,
        )

    def w_start(*args, **kwargs):
        copy = w_copy(*args, **kwargs)
        copy.start()
        sends.append(copy)

    def d_copy(core, event, a, b, source=None):
        dst = w_buf.at[pl.ds(block(core, a, b), shard)]
        return pltpu.make_async_remote_copy(
            src_ref=dst if source is None else source,
            dst_ref=dst,
            send_sem=d_send.at[event],
            recv_sem=d_recv.at[event],
            device_id=me.partner(),
            device_id_type=MESH,
        )

    order = []

    def share(a, b, source=None):
        copy = d_copy(me.core, len(order), a, b, source)
        copy.start()
        sends.append(copy)
        order.append((a, b))

    for i in range(parts):
        tok_copy(i).wait()

        @pl.loop(0, span // 16)
        def _(r):
            piece = pl.ds(pl.multiple_of(i * span + r * 16, 16), 16)
            squares = jnp.zeros((16, wide), jnp.float32)
            for c in range(CHUNKS):
                value = raw[piece, c * wide : (c + 1) * wide].astype(jnp.float32)
                squares = squares + value * value
            mean = jnp.sum(squares, axis=-1, keepdims=True) * (1.0 / width)
            scale_scr[piece, :] = jnp.broadcast_to(lax.rsqrt(mean + EPSILON), (16, 128))

    def x_copy(row_block, chunk, device, way):
        ref = x_buf.at[row_block, chunk]
        return pltpu.make_async_remote_copy(
            src_ref=ref,
            dst_ref=ref,
            send_sem=x_send.at[way, chunk],
            recv_sem=x_recv.at[way // 2 * 2 if way > 1 else way, chunk],
            device_id=device,
            device_id_type=MESH,
        )

    def normalize_chunk(c):
        @pl.loop(0, rows // 16)
        def _(r):
            piece = pl.ds(pl.multiple_of(r * 16, 16), 16)
            scale = scale_scr[piece, :]
            for k in range(wide // 128):
                lanes = slice(c * wide + k * 128, c * wide + (k + 1) * 128)
                value = raw[piece, lanes].astype(jnp.float32)
                x_buf[me.y, c, piece, k * 128 : (k + 1) * 128] = (
                    value * scale * gain_ref[:, lanes]
                ).astype(jnp.bfloat16)

    def x_start(row_block, chunk, device, way):
        copy = x_copy(row_block, chunk, device, way)
        copy.start()
        sends.append(copy)

    middle = CHUNKS // 2
    loads[0].wait()
    normalize_chunk(0)
    normalize_chunk(middle)
    pl.semaphore_wait(barrier, len(neighbours))

    w_start(0, 0, me.near(1, 0), 4, 0, source=w_hbm)
    w_start(0, 0, me.near(3, 0), 4, 1, source=w_hbm)
    w_start(0, 0, me.near(0, 1), 0, 0, source=w_hbm)
    w_start(0, 0, me.near(0, 3), 0, 1, source=w_hbm)
    share(0, 0, source=w_hbm)

    for c in range(middle):
        x_start(me.y, c, me.along(1), 0)
        x_start(me.y, c + middle, me.along(3), 1)
        if c + 1 < middle:
            normalize_chunk(c + 1)
            normalize_chunk(c + 1 + middle)
    for c in range(middle):
        x_start(me.y, c + middle, me.along(1), 0)
        x_start(me.y, c, me.along(3), 1)

    acc[...] = jnp.zeros_like(acc)
    down_scr[...] = jnp.zeros_like(down_scr)

    dv_scr[...] = jnp.zeros_like(dv_scr)
    up_part[...] = jnp.zeros_like(up_part)
    for load in loads[1:]:
        load.wait()

    def arrived(a, b, kind, way, piece=None):
        w_copy(a, b, me.near(0, 1), kind, way, piece).wait_recv()

    def spread(a, kind):
        w_start(a, 0, me.near(0, 1), kind, 0)
        w_start(a, 0, me.near(0, 3), kind, 1)

    own_copy.wait()
    arrived(3, 0, 4, 0)
    w_start(3, 0, me.near(1, 0), 4, 2, piece=0)
    spread(3, 1)
    share(3, 0)
    arrived(1, 0, 4, 1)
    w_start(1, 0, me.near(3, 0), 4, 3, piece=1)
    spread(1, 2)
    share(1, 0)
    for kind, a in enumerate(OFFSETS):
        if kind == 3:
            arrived(2, 0, 4, 2, piece=0)
            arrived(2, 0, 4, 3, piece=1)
            spread(2, 3)
            share(2, 0)
        arrived(a, 3, kind, 0)
        w_start(a, 3, me.near(0, 1), kind, 2, piece=0)
        share(a, 3)
        arrived(a, 1, kind, 1)
        w_start(a, 1, me.near(0, 3), kind, 3, piece=1)
        share(a, 1)
        if kind > 0:
            before = OFFSETS[kind - 1]
            arrived(before, 2, kind - 1, 2, piece=0)
            arrived(before, 2, kind - 1, 3, piece=1)
            share(before, 2)
    arrived(OFFSETS[3], 2, 3, 2, piece=0)
    arrived(OFFSETS[3], 2, 3, 3, piece=1)
    share(OFFSETS[3], 2)

    minus = lax.rem(me.y + 3, 4)
    plus = lax.rem(me.y + 1, 4)
    far = lax.rem(me.y + 2, 4)
    for c in range(middle):
        x_copy(minus, c, me.along(1), 0).wait_recv()
        x_start(minus, c, me.along(1), 2)
        x_copy(plus, c + middle, me.along(1), 1).wait_recv()
        x_start(plus, c + middle, me.along(3), 2)

    def send_grads(first, last):
        @pl.loop(first, last)
        def _(h):
            for c in (1, 3, 2):
                grad_copy(h, c).start()

    @pl.loop(0, heads)
    def _(h):
        own_grad(h).start()

    send_grads(0, EARLY)

    for event, (a, b) in enumerate(order):
        d_copy(1 - me.core, event, a, b).wait_recv()

    def multiply(row_block, chunk):
        value = x_buf[row_block, chunk]
        lines = pl.ds(pl.multiple_of(row_block * rows, rows), rows)
        depth = pl.ds(pl.multiple_of(chunk * wide, wide), wide)
        for n in range(cols // 256):
            lanes = slice(n * 256, (n + 1) * 256)
            acc[lines, lanes] += dot_nn(value, w_buf[depth, lanes])
        down_scr[lines, :] += dot_nt(value, adapt_ref[:, depth])

    def prepare(row_block):
        lines = pl.ds(pl.multiple_of(row_block * rows, rows), rows)
        down = down_scr[lines, :].astype(jnp.bfloat16)
        down_b[lines, :] = down
        cos, sin = cos_ref[lines, :], sin_ref[lines, :]
        for h in range(heads):
            lanes = slice(h * HD, (h + 1) * HD)
            value = acc[lines, lanes] + ADAPTER_SCALE * dot_nn(down[:, :RANK], qup_ref[:, lanes])
            value = value.astype(jnp.bfloat16).astype(jnp.float32)
            q_buf[h, lines, :] = rotate(value, cos, sin).astype(jnp.bfloat16)
        value = acc[lines, group : group + HD].astype(jnp.bfloat16).astype(jnp.float32)
        k_scr[lines, :] = rotate(value, cos, sin).astype(jnp.bfloat16)
        v_scr[lines, :] = (
            acc[lines, group + HD :] + ADAPTER_SCALE * dot_nn(down[:, RANK:], vup_ref[...])
        ).astype(jnp.bfloat16)

    @pl.loop(0, CHUNKS)
    def _(c):
        multiply(me.y, c)

    @pl.loop(0, CHUNKS)
    def _(c):
        @pl.when(c >= middle)
        def _():
            x_copy(minus, c, me.along(1), 0).wait_recv()

        multiply(minus, c)

    @pl.loop(0, CHUNKS)
    def _(c):
        @pl.when(c < middle)
        def _():
            x_copy(plus, c, me.along(1), 1).wait_recv()

        multiply(plus, c)

    @pl.loop(0, 3)
    def _(c):
        prepare(lax.rem(me.y + 3 + c, 4))

    @pl.loop(0, middle)
    def _(c):
        x_copy(far, c, me.along(1), 2).wait_recv()
        multiply(far, c)
        x_copy(far, c + middle, me.along(1), 2).wait_recv()
        multiply(far, c + middle)

    send_grads(EARLY, heads)
    prepare(far)
    down_t[...] = down_b[...].astype(jnp.float32).T.astype(jnp.bfloat16)

    row = lax.broadcasted_iota(jnp.int32, (QB, QB), 0)
    col = lax.broadcasted_iota(jnp.int32, (QB, QB), 1)
    causal = row >= col
    factor = SCORE_SCALE * LOG2E

    def send_out(h):
        own_out(h).start()
        for c in (1, 3, 2):
            out_copy(h, c).start()

    @pl.loop(0, heads)
    def _(head):
        own_grad(head).wait()
        for c in (1, 3, 2):
            grad_arrival(head, c).wait_recv()
        head_lanes = pl.ds(pl.multiple_of(head * HD, HD), HD)

        for i in range(blocks):
            own_rows = slice(i * QB, (i + 1) * QB)
            q = q_buf[head, own_rows, :]
            grad = g_buf[head, own_rows, :]
            grad_t = grad.T
            scores = []
            for j in range(i + 1):
                s = dot_nt(q, k_scr[j * QB : (j + 1) * QB, :])
                if j == i:
                    s = jnp.where(causal, s, -1e30)
                scores.append(s)
            top = functools.reduce(jnp.maximum, scores)
            top = jnp.max(top, axis=-1, keepdims=True) * factor
            weights = [jnp.exp2(s * factor - top) for s in scores]
            whole = jnp.sum(functools.reduce(jnp.add, weights), axis=-1, keepdims=True)
            inverse = 1.0 / whole
            probs = [w * inverse for w in weights]
            rounded = [p.astype(jnp.bfloat16) for p in probs]
            attended = functools.reduce(
                jnp.add, [dot_nn(rounded[j], v_scr[j * QB : (j + 1) * QB, :]) for j in range(i + 1)]
            )
            o_buf[head, own_rows, :] = attended.astype(jnp.bfloat16)
            prods = []
            for j in range(i + 1):
                keys = slice(j * QB, (j + 1) * QB)
                dp = dot_nt(grad, v_scr[keys, :])
                prods.append(probs[j] * dp)
                dv_scr[:, keys] += dot_nn(grad_t, rounded[j])
            inner = jnp.sum(functools.reduce(jnp.add, prods), axis=-1, keepdims=True)
            ds = [(prods[j] - probs[j] * inner).astype(jnp.bfloat16) for j in range(i + 1)]
            dq = functools.reduce(
                jnp.add, [dot_nn(ds[j], k_scr[j * QB : (j + 1) * QB, :]) for j in range(i + 1)]
            )
            dq = (dq * SCORE_SCALE).astype(jnp.bfloat16).astype(jnp.float32)
            dq_all[own_rows, head_lanes] = rotate(dq, cos_ref[own_rows, :], -sin_ref[own_rows, :]).astype(
                jnp.bfloat16
            )


        @pl.when(head >= LAG)
        def _():
            send_out(head - LAG)

    dv_t = dv_scr[...].astype(jnp.bfloat16)
    mid_q = dot_nt(dq_all[...], qup_ref[...]).T
    mid_v = dot_nn(vup_ref[...], dv_t)
    for b in range(4):
        lanes = slice(b * rows, (b + 1) * rows)
        mid_scr[b, :RANK] = mid_q[:, lanes]
        mid_scr[b, RANK:] = mid_v[:, lanes]
        mid_mine[b, :RANK] = mid_q[:, lanes].astype(jnp.bfloat16)
        mid_mine[b, RANK:] = mid_v[:, lanes].astype(jnp.bfloat16)

    def mid_copy(c):
        return remote(
            mid_mine, mid_recv.at[c - 1], m_send.at[c - 1], m_recv.at[c - 1], me.along(c)
        )

    for c in (1, 3, 2):
        mid_copy(c).start()
    for n in range(4):
        up = dot_nn(down_t[:RANK, :], dq_all[:, n * 256 : (n + 1) * 256])
        for h in range(2):
            up_part[0, 2 * n + h] = up[:8, h * HD : (h + 1) * HD]
            up_part[1, 2 * n + h] = up[8:, h * HD : (h + 1) * HD]
    up = dot_nt(down_t[RANK:, :], dv_t)
    up_part[0, heads] = up[:8]
    up_part[1, heads] = up[8:]
    for c in (1, 3, 2):
        mid_copy(c).wait_recv()
    send_out(4)
    for b in range(4):
        summed = mid_scr[b]
        for c in range(3):
            summed += mid_recv[c, b].astype(jnp.float32)
        mid_all[b] = summed.astype(jnp.bfloat16)

    def partial(half):
        for n in range(2):
            chunk = 4 * me.y + 2 * half + n
            made = dot_nn(mid_all[0], x_buf[0, chunk])
            for b in range(1, 4):
                made += dot_nn(mid_all[b], x_buf[b, chunk])
            for r in range(2):
                for k in range(4):
                    part[half, r * 8 + n * 4 + k] = made[
                        r * 16 : (r + 1) * 16, k * HD : (k + 1) * HD
                    ]

    partial(1 - me.core)
    swap = remote(part.at[1 - me.core], part_recv, c_send.at[0], c_recv.at[0], me.partner())
    up_swap = remote(up_part.at[1 - me.core], up_recv, c_send.at[1], c_recv.at[1], me.partner())
    swap.start()
    up_swap.start()
    partial(me.core)
    up_swap.wait_recv()
    swap.wait_recv()
    total[:, :16] = (part[me.core] + part_recv[...]).astype(jnp.bfloat16)
    total[:, 16:] = (up_part[me.core] + up_recv[...]).astype(jnp.bfloat16)

    for n, (a, b) in enumerate(AROUND[:-1]):
        dp, fs = me.plane(me.core, a, b)
        remote(
            total.at[lax.div(dp, 2) * 8 + fs],
            rs_recv.at[n],
            r_send.at[0],
            r_recv.at[0],
            (dp, fs, me.y),
        ).start()

    send_out(5)
    send_out(6)
    many = remote(rs_recv, rs_recv, r_send.at[0], r_recv.at[0], me.partner())
    many.wait_recv()
    summed = total[plane].astype(jnp.float32)
    for o in range(PLANE - 1):
        summed += rs_recv[o].astype(jnp.float32)
    final[...] = (ADAPTER_SCALE * summed[:16]).astype(jnp.bfloat16)
    up_final[...] = ADAPTER_SCALE * summed[16:]

    at_rows = pl.ds(pl.multiple_of(lax.div(plane, 8) * 16, 16), 16)
    at_cols = pl.ds(pl.multiple_of(lax.rem(plane, 8) * HD, HD), HD)
    up_cols = pl.ds(pl.multiple_of(plane * HD, HD), HD)

    for a, b in AROUND:
        near = me.plane(me.core, a, b)
        for c in (2, 1, 3, 0):
            if a or b or c:
                remote(
                    final,
                    res.at[me.core, me.y, at_rows, at_cols],
                    r_send.at[1],
                    r_recv.at[1],
                    (*near, lax.rem(me.y + c, 4)),
                ).start()
    for a, b in AROUND[:-1]:
        remote(
            up_final, up_res.at[me.core, :, up_cols], r_send.at[2], r_recv.at[2], me.near(a, b)
        ).start()

    send_out(7)
    res[me.core, me.y, at_rows, at_cols] = final[...]
    up_res[me.core, :, up_cols] = up_final[...]
    all_of = remote(ag_size, ag_size, r_send.at[1], r_recv.at[1], me.partner())
    up_size = ag_size.at[pl.ds(0, PLANE - 1)]
    up_all = remote(up_size, up_size, r_send.at[2], r_recv.at[2], me.partner())
    up_all.wait_recv()
    up_half = remote(
        up_res.at[me.core], up_res.at[me.core], c_send.at[2], c_recv.at[2], me.partner()
    )
    up_half.start()
    all_of.wait_recv()
    half = remote(res.at[me.core], res.at[me.core], c_send.at[3], c_recv.at[3], me.partner())
    half.start()

    def grad_a_writes(b, first):
        copies = []
        for yy in range(4):
            cols_out = pl.ds(pl.multiple_of(yy * 2048 + b * 1024, 1024), 1024)
            for i, dst in enumerate((ga_q_hbm, ga_v_hbm)):
                copies.append(
                    pltpu.make_async_copy(
                        res.at[b, yy, pl.ds(i * RANK, RANK)],
                        dst.at[:, cols_out],
                        write_sem.at[first + yy * 2 + i],
                    )
                )
        return copies

    def grad_b_writes(b, first):
        eight = pl.ds(pl.multiple_of(b * 8, 8), 8)
        return [
            pltpu.make_async_copy(
                up_res.at[b, :, pl.ds(0, group + HD)], gb_hbm.at[eight], write_sem.at[first]
            )
        ]

    writes = grad_a_writes(me.core, 0) + grad_b_writes(me.core, 8)
    for copy in writes:
        copy.start()
    @pl.loop(0, heads)
    def _(h):
        own_out(h).wait()
        for c in (1, 3, 2):
            grad_copy(h, c).wait_send()
            out_copy(h, c).wait_send()
            out_arrival(h, c).wait_recv()

    for copy in sends:
        copy.wait_send()
    up_other = up_res.at[1 - me.core]
    remote(up_other, up_other, c_send.at[2], c_recv.at[2], me.partner()).wait_recv()
    other = res.at[1 - me.core]
    remote(other, other, c_send.at[3], c_recv.at[3], me.partner()).wait_recv()
    late = grad_a_writes(1 - me.core, 10) + grad_b_writes(1 - me.core, 18)
    for copy in late:
        copy.start()
    for c in (1, 3, 2):
        mid_copy(c).wait_send()
    for copy in (up_swap, swap, many, all_of, up_all, up_half, half):
        copy.wait_send()
    for copy in writes + late:
        copy.wait()


def fused_step(tokens, gain, w_qkv, aq_t, av_t, qup, vup, cos, sin, out_grad):
    rows, width = tokens.shape
    shard, cols = w_qkv.shape
    heads = QUERY_PER_KV
    seq = 4 * rows
    wide = width // CHUNKS
    anywhere = pl.BlockSpec(memory_space=pl.ANY)
    dma = pltpu.SemaphoreType.DMA
    f32, bf16 = jnp.float32, jnp.bfloat16
    return pl.pallas_call(
        functools.partial(step_kernel, rows),
        in_specs=[anywhere] * 10,
        out_specs=[anywhere] * 4,
        out_shape=[
            jax.ShapeDtypeStruct((rows, 4 * heads * HD), bf16),
            jax.ShapeDtypeStruct((RANK, width), bf16),
            jax.ShapeDtypeStruct((RANK, width), bf16),
            jax.ShapeDtypeStruct((RANK, (heads + 1) * HD), f32),
        ],
        scratch_shapes=[
            pltpu.VMEM((rows, width), bf16),
            pltpu.VMEM((rows, 128), f32),
            pltpu.VMEM((4, CHUNKS, rows, wide), bf16),
            pltpu.VMEM((width, cols), bf16),
            pltpu.VMEM((seq, cols), f32),
            pltpu.VMEM((seq, 2 * RANK), f32),
            pltpu.VMEM((1, width), f32),
            pltpu.VMEM((2 * RANK, width), bf16),
            pltpu.VMEM((RANK, heads * HD), bf16),
            pltpu.VMEM((RANK, HD), bf16),
            pltpu.VMEM((seq, HD), f32),
            pltpu.VMEM((seq, HD), f32),
            pltpu.VMEM((rows, 4 * heads * HD), bf16),
            pltpu.VMEM((heads, seq, HD), bf16),
            pltpu.VMEM((seq, HD), bf16),
            pltpu.VMEM((seq, HD), bf16),
            pltpu.VMEM((seq, 2 * RANK), bf16),
            pltpu.VMEM((2 * RANK, seq), bf16),
            pltpu.VMEM((HD, seq), f32),
            pltpu.VMEM((seq, heads * HD), bf16),
            pltpu.VMEM((4, 2 * RANK, rows), f32),
            pltpu.VMEM((4, 2 * RANK, rows), bf16),
            pltpu.VMEM((3, 4, 2 * RANK, rows), bf16),
            pltpu.VMEM((4, 2 * RANK, rows), bf16),
            pltpu.VMEM((heads, seq, HD), bf16),
            pltpu.VMEM((heads, seq, HD), bf16),
            pltpu.VMEM((2, PLANE, 16, HD), f32),
            pltpu.VMEM((PLANE, 16, HD), f32),
            pltpu.VMEM((2, PLANE, 8, HD), f32),
            pltpu.VMEM((PLANE, 8, HD), f32),
            pltpu.VMEM((PLANE, 24, HD), bf16),
            pltpu.VMEM((PLANE - 1, 24, HD), bf16),
            pltpu.VMEM((16, HD), bf16),
            pltpu.VMEM((8, HD), f32),
            pltpu.VMEM((2, 4, 2 * RANK, 1024), bf16),
            pltpu.VMEM((2, 8, PLANE * HD), f32),
            pltpu.VMEM((CHIPS - 1, 16, HD), bf16),
            dma((4,)),
            dma((8,)),
            dma(()),
            dma((5, 4)),
            dma((5, 4)),
            dma((16,)),
            dma((16,)),
            dma((3, CHUNKS)),
            dma((3, CHUNKS)),
            dma((heads,)),
            dma((heads,)),
            dma((heads, 3)),
            dma((heads, 3)),
            dma((heads, 3)),
            dma((heads, 3)),
            dma((3,)),
            dma((3,)),
            dma((4,)),
            dma((4,)),
            dma((3,)),
            dma((3,)),
            dma((20,)),
        ],
        compiler_params=pltpu.CompilerParams(
            collective_id=1, has_side_effects=True, vmem_limit_bytes=63 << 20
        ),
        cost_estimate=pl.CostEstimate(
            flops=2 * seq * width * cols,
            bytes_accessed=10 * 1000 * 1000,
            transcendentals=heads * seq * seq,
        ),
        name="fused_step",
    )(tokens, gain.reshape(1, width), w_qkv, aq_t, av_t, qup, vup, cos, sin, out_grad)


def finish_kernel(
    out_in, gq_in, gv_in, gb_in, out, gq, gv, bq, bv, rows, aq, av, fq, fv, b_buf, in_sem, out_sem
):
    parts = 4
    size = rows.shape[0] // parts
    cols = bq.shape[1]
    small = [
        pltpu.make_async_copy(src, dst, in_sem.at[parts + i])
        for i, (src, dst) in enumerate(((gq_in, aq), (gv_in, av), (gb_in, b_buf)))
    ]
    large = [
        pltpu.make_async_copy(
            out_in.at[pl.ds(i * size, size)], rows.at[pl.ds(i * size, size)], in_sem.at[i]
        )
        for i in range(parts)
    ]
    for copy in small + large:
        copy.start()
    writes = []

    def write(src, dst):
        copy = pltpu.make_async_copy(src, dst, out_sem.at[len(writes)])
        copy.start()
        writes.append(copy)

    small[0].wait()
    fq[...] = aq[...].astype(jnp.float32)
    write(fq, gq)
    small[1].wait()
    fv[...] = av[...].astype(jnp.float32)
    write(fv, gv)
    for i in range(parts):
        large[i].wait()
        write(rows.at[pl.ds(i * size, size)], out.at[pl.ds(i * size, size)])
    small[2].wait()
    write(b_buf.at[:, pl.ds(0, cols)], bq)
    write(b_buf.at[:, pl.ds(cols, HD)], bv)
    for copy in writes:
        copy.wait()


def finish(out_rows, ga_query, ga_value, grad_b):
    anywhere = pl.BlockSpec(memory_space=pl.ANY)
    cols = grad_b.shape[1] - HD
    f32 = jnp.float32
    return pl.pallas_call(
        finish_kernel,
        in_specs=[anywhere] * 4,
        out_specs=[anywhere] * 5,
        out_shape=[
            jax.ShapeDtypeStruct(out_rows.shape, out_rows.dtype),
            jax.ShapeDtypeStruct(ga_query.shape, f32),
            jax.ShapeDtypeStruct(ga_value.shape, f32),
            jax.ShapeDtypeStruct((RANK, cols), f32),
            jax.ShapeDtypeStruct((RANK, HD), f32),
        ],
        scratch_shapes=[
            pltpu.VMEM(out_rows.shape, out_rows.dtype),
            pltpu.VMEM(ga_query.shape, ga_query.dtype),
            pltpu.VMEM(ga_value.shape, ga_value.dtype),
            pltpu.VMEM(ga_query.shape, f32),
            pltpu.VMEM(ga_value.shape, f32),
            pltpu.VMEM(grad_b.shape, f32),
            pltpu.SemaphoreType.DMA((7,)),
            pltpu.SemaphoreType.DMA((8,)),
        ],
        name="finish",
    )(out_rows, ga_query, ga_value, grad_b)


def local(tokens, norm_gain, w_qkv, a_query, query_up_adapter, a_value, value_up_adapter, out_grad):
    cos, sin = rotary_tables(4 * tokens.shape[1])
    out_rows, ga_query, ga_value, grad_b = fused_step(
        tokens[0],
        norm_gain,
        w_qkv,
        a_query.T,
        a_value.T,
        query_up_adapter,
        value_up_adapter,
        cos,
        sin,
        out_grad[0],
    )
    out_rows, ga_query, ga_value, gb_query, gb_value = finish(out_rows, ga_query, ga_value, grad_b)
    return out_rows[None], ga_query.T, gb_query, ga_value.T, gb_value


def solution(mesh):
    return jax.shard_map(
        local,
        mesh=mesh,
        in_specs=(
            P(("dp", "fsdp"), "tensor", None),
            P(),
            P(("dp", "fsdp"), "tensor"),
            P(),
            P(None, "tensor"),
            P(),
            P(None, "tensor"),
            P(("dp", "fsdp"), "tensor", None),
        ),
        out_specs=(
            P(("dp", "fsdp"), "tensor", None),
            P(),
            P(None, "tensor"),
            P(),
            P(None, "tensor"),
        ),
        check_vma=False,
    )
```

```python
import functools
import math

import jax
import jax.numpy as jnp
import numpy as np
from jax import lax
from jax.experimental import pallas as pl
from jax.experimental.pallas import tpu as pltpu
from jax.sharding import PartitionSpec as P

HD = 128
QUERY_PER_KV = 8
RANK = 16
QB = 384

EPSILON = 1e-05
ADAPTER_SCALE = 2.0
ROPE_BASE = 500000.0
SCORE_SCALE = 1.0 / math.sqrt(HD)
LOG2E = 1.4426950408889634


def rotary_tables(sequence_length):
    half_dim = HD // 2
    inv_freq = ROPE_BASE ** (-np.arange(half_dim) / half_dim)
    angles = np.arange(sequence_length)[:, None] * inv_freq
    cosine, sine = np.cos(angles), np.sin(angles)
    return (
        np.concatenate([cosine, cosine], 1).astype(np.float32),
        np.concatenate([-sine, sine], 1).astype(np.float32),
    )


def dot_nt(a, b):
    return lax.dot_general(a, b, (((1,), (1,)), ((), ())), preferred_element_type=jnp.float32)


def dot_nn(a, b):
    return jnp.dot(a, b, preferred_element_type=jnp.float32)


def rotate(x, cos, sin):
    return x * cos + pltpu.roll(x, HD // 2, 1) * sin


MESH = pl.DeviceIdType.MESH
CHUNKS = 16
OFFSETS = (0, 3, 1, 2)


class Place:
    def __init__(self):
        self.dp = lax.axis_index("dp")
        self.fs = lax.axis_index("fsdp")
        self.y = lax.axis_index("tensor")
        self.core = lax.rem(self.dp, 2)
        self.x = lax.div(self.dp, 2) * 2 + lax.rem(self.fs, 2)
        self.z = lax.div(self.fs, 2)

    def ring(self, core):
        first = self.x * (1 - core) + self.z * core
        second = self.z * (1 - core) + self.x * core
        return first, second

    def plane(self, core, a, b):
        first, second = self.ring(core)
        first = lax.rem(first + a, 4)
        second = lax.rem(second + b, 4)
        x = first * (1 - core) + second * core
        z = second * (1 - core) + first * core
        return lax.div(x, 2) * 2 + core, z * 2 + lax.rem(x, 2)

    def near(self, a, b):
        return (*self.plane(self.core, a, b), self.y)

    def along(self, c):
        return (self.dp, self.fs, lax.rem(self.y + c, 4))

    def partner(self):
        return (self.dp + 1 - 2 * self.core, self.fs, self.y)


CHIPS = 64
PLANE = 16
LAG = 4
EARLY = 2
AROUND = sorted(
    ((a, b) for a in range(4) for b in range(4)),
    key=lambda step: -sum(min(n, 4 - n) for n in step),
)


def step_kernel(
    rows,
    tok_hbm,
    gain_hbm,
    w_hbm,
    aq_hbm,
    av_hbm,
    qup_hbm,
    vup_hbm,
    cos_hbm,
    sin_hbm,
    grad_hbm,
    out_hbm,
    ga_q_hbm,
    ga_v_hbm,
    gb_hbm,
    raw,
    scale_scr,
    x_buf,
    w_buf,
    acc,
    down_scr,
    gain_ref,
    adapt_ref,
    qup_ref,
    vup_ref,
    cos_ref,
    sin_ref,
    stage,
    q_buf,
    k_scr,
    v_scr,
    down_b,
    down_t,
    dv_scr,
    dq_all,
    mid_scr,
    mid_mine,
    mid_recv,
    mid_all,
    g_buf,
    o_buf,
    part,
    part_recv,
    up_part,
    up_recv,
    total,
    rs_recv,
    final,
    up_final,
    res,
    up_res,
    ag_size,
    tok_sem,
    load_sem,
    own_sem,
    w_send,
    w_recv,
    d_send,
    d_recv,
    x_send,
    x_recv,
    own_g_sem,
    o_own_sem,
    g_send,
    g_recv,
    o_send,
    o_recv,
    m_send,
    m_recv,
    c_send,
    c_recv,
    r_send,
    r_recv,
    write_sem,
):
    heads = QUERY_PER_KV
    group = heads * HD
    seq = 4 * rows
    blocks = seq // QB

    me = Place()
    shard = w_hbm.shape[0]
    half_shard = shard // 2
    width = tok_hbm.shape[1]
    wide = width // CHUNKS
    cols = w_hbm.shape[1]
    parts = tok_sem.shape[0]
    span = rows // parts

    def tok_copy(i):
        piece = pl.ds(i * span, span)
        return pltpu.make_async_copy(tok_hbm.at[piece], raw.at[piece], tok_sem.at[i])

    for i in range(parts):
        tok_copy(i).start()

    loads = [
        pltpu.make_async_copy(src, dst, load_sem.at[i])
        for i, (src, dst) in enumerate(
            (
                (gain_hbm, gain_ref),
                (aq_hbm, adapt_ref.at[pl.ds(0, RANK)]),
                (av_hbm, adapt_ref.at[pl.ds(RANK, RANK)]),
                (qup_hbm, qup_ref),
                (vup_hbm, vup_ref),
                (cos_hbm, cos_ref),
                (sin_hbm, sin_ref),
                (grad_hbm, stage),
            )
        )
    ]

    def block(core, a, b):
        dp, fs = me.plane(core, a, b)
        return pl.multiple_of((dp * 8 + fs) * shard, shard)

    own = block(me.core, 0, 0)
    own_copy = pltpu.make_async_copy(w_hbm, w_buf.at[pl.ds(own, shard)], own_sem)
    own_copy.start()

    plane = lax.div(me.dp, 2) * 8 + me.fs

    barrier = pltpu.get_barrier_semaphore()

    neighbours = (
        me.along(1),
        me.along(3),
        me.along(2),
        me.near(1, 0),
        me.near(3, 0),
        me.near(0, 1),
        me.near(0, 3),
        me.partner(),
    )
    for device in neighbours:
        pl.semaphore_signal(barrier, inc=1, device_id=device, device_id_type=MESH)
    for load in loads:
        load.start()

    def lines_of(block):
        return pl.ds(pl.multiple_of(block * rows, rows), rows)

    def columns(block, h):
        return pl.ds(pl.multiple_of(block * group + h * HD, HD), HD)

    def remote(src, dst, send, recv, device):
        return pltpu.make_async_remote_copy(
            src_ref=src,
            dst_ref=dst,
            send_sem=send,
            recv_sem=recv,
            device_id=device,
            device_id_type=MESH,
        )

    def own_grad(h):
        return pltpu.make_async_copy(
            grad_hbm.at[:, columns(me.y, h)], g_buf.at[h, lines_of(me.y)], own_g_sem.at[h]
        )

    def grad_copy(h, c):
        to = lax.rem(me.y + c, 4)
        return remote(
            stage.at[:, columns(to, h)],
            g_buf.at[h, lines_of(me.y)],
            g_send.at[h, c - 1],
            g_recv.at[h, c - 1],
            me.along(c),
        )

    def grad_arrival(h, c):
        ref = g_buf.at[h, lines_of(lax.rem(me.y + 4 - c, 4))]
        return remote(ref, ref, g_send.at[h, c - 1], g_recv.at[h, c - 1], me.along(c))

    def own_out(h):
        return pltpu.make_async_copy(
            o_buf.at[h, lines_of(me.y)], out_hbm.at[:, columns(me.y, h)], o_own_sem.at[h]
        )

    def out_copy(h, c):
        to = lax.rem(me.y + c, 4)
        return remote(
            o_buf.at[h, lines_of(to)],
            out_hbm.at[:, columns(me.y, h)],
            o_send.at[h, c - 1],
            o_recv.at[h, c - 1],
            me.along(c),
        )

    def out_arrival(h, c):
        ref = out_hbm.at[:, columns(lax.rem(me.y + 4 - c, 4), h)]
        return remote(ref, ref, o_send.at[h, c - 1], o_recv.at[h, c - 1], me.along(c))

    sends = []

    def w_copy(a, b, device, kind, way, piece=None, source=None):
        start = block(me.core, a, b)
        size = shard
        if piece is not None:
            start, size = pl.multiple_of(start + piece * half_shard, half_shard), half_shard
        dst = w_buf.at[pl.ds(start, size)]
        return pltpu.make_async_remote_copy(
            src_ref=dst if source is None else source,
            dst_ref=dst,
            send_sem=w_send.at[kind, way],
            recv_sem=w_recv.at[kind, way],
            device_id=device,
            device_id_type=MESH,
        )

    def w_start(*args, **kwargs):
        copy = w_copy(*args, **kwargs)
        copy.start()
        sends.append(copy)

    def d_copy(core, event, a, b, source=None):
        dst = w_buf.at[pl.ds(block(core, a, b), shard)]
        return pltpu.make_async_remote_copy(
            src_ref=dst if source is None else source,
            dst_ref=dst,
            send_sem=d_send.at[event],
            recv_sem=d_recv.at[event],
            device_id=me.partner(),
            device_id_type=MESH,
        )

    order = []

    def share(a, b, source=None):
        copy = d_copy(me.core, len(order), a, b, source)
        copy.start()
        sends.append(copy)
        order.append((a, b))

    for i in range(parts):
        tok_copy(i).wait()

        @pl.loop(0, span // 16)
        def _(r):
            piece = pl.ds(pl.multiple_of(i * span + r * 16, 16), 16)
            squares = jnp.zeros((16, wide), jnp.float32)
            for c in range(CHUNKS):
                value = raw[piece, c * wide : (c + 1) * wide].astype(jnp.float32)
                squares = squares + value * value
            mean = jnp.sum(squares, axis=-1, keepdims=True) * (1.0 / width)
            scale_scr[piece, :] = jnp.broadcast_to(lax.rsqrt(mean + EPSILON), (16, 128))

    def x_copy(row_block, chunk, device, way):
        ref = x_buf.at[row_block, chunk]
        return pltpu.make_async_remote_copy(
            src_ref=ref,
            dst_ref=ref,
            send_sem=x_send.at[way, chunk],
            recv_sem=x_recv.at[way // 2 * 2 if way > 1 else way, chunk],
            device_id=device,
            device_id_type=MESH,
        )

    def normalize_chunk(c):
        @pl.loop(0, rows // 16)
        def _(r):
            piece = pl.ds(pl.multiple_of(r * 16, 16), 16)
            scale = scale_scr[piece, :]
            for k in range(wide // 128):
                lanes = slice(c * wide + k * 128, c * wide + (k + 1) * 128)
                value = raw[piece, lanes].astype(jnp.float32)
                x_buf[me.y, c, piece, k * 128 : (k + 1) * 128] = (
                    value * scale * gain_ref[:, lanes]
                ).astype(jnp.bfloat16)

    def x_start(row_block, chunk, device, way):
        copy = x_copy(row_block, chunk, device, way)
        copy.start()
        sends.append(copy)

    middle = CHUNKS // 2
    loads[0].wait()
    normalize_chunk(0)
    normalize_chunk(middle)
    pl.semaphore_wait(barrier, len(neighbours))

    w_start(0, 0, me.near(1, 0), 4, 0, source=w_hbm)
    w_start(0, 0, me.near(3, 0), 4, 1, source=w_hbm)
    w_start(0, 0, me.near(0, 1), 0, 0, source=w_hbm)
    w_start(0, 0, me.near(0, 3), 0, 1, source=w_hbm)
    share(0, 0, source=w_hbm)

    for c in range(middle):
        x_start(me.y, c, me.along(1), 0)
        x_start(me.y, c + middle, me.along(3), 1)
        if c + 1 < middle:
            normalize_chunk(c + 1)
            normalize_chunk(c + 1 + middle)
    for c in range(middle):
        x_start(me.y, c + middle, me.along(1), 0)
        x_start(me.y, c, me.along(3), 1)

    acc[...] = jnp.zeros_like(acc)
    down_scr[...] = jnp.zeros_like(down_scr)

    dv_scr[...] = jnp.zeros_like(dv_scr)
    up_part[...] = jnp.zeros_like(up_part)
    for load in loads[1:]:
        load.wait()

    def arrived(a, b, kind, way, piece=None):
        w_copy(a, b, me.near(0, 1), kind, way, piece).wait_recv()

    def spread(a, kind):
        w_start(a, 0, me.near(0, 1), kind, 0)
        w_start(a, 0, me.near(0, 3), kind, 1)

    own_copy.wait()
    arrived(3, 0, 4, 0)
    w_start(3, 0, me.near(1, 0), 4, 2, piece=0)
    spread(3, 1)
    share(3, 0)
    arrived(1, 0, 4, 1)
    w_start(1, 0, me.near(3, 0), 4, 3, piece=1)
    spread(1, 2)
    share(1, 0)
    for kind, a in enumerate(OFFSETS):
        if kind == 3:
            arrived(2, 0, 4, 2, piece=0)
            arrived(2, 0, 4, 3, piece=1)
            spread(2, 3)
            share(2, 0)
        arrived(a, 3, kind, 0)
        w_start(a, 3, me.near(0, 1), kind, 2, piece=0)
        share(a, 3)
        arrived(a, 1, kind, 1)
        w_start(a, 1, me.near(0, 3), kind, 3, piece=1)
        share(a, 1)
        if kind > 0:
            before = OFFSETS[kind - 1]
            arrived(before, 2, kind - 1, 2, piece=0)
            arrived(before, 2, kind - 1, 3, piece=1)
            share(before, 2)
    arrived(OFFSETS[3], 2, 3, 2, piece=0)
    arrived(OFFSETS[3], 2, 3, 3, piece=1)
    share(OFFSETS[3], 2)

    minus = lax.rem(me.y + 3, 4)
    plus = lax.rem(me.y + 1, 4)
    far = lax.rem(me.y + 2, 4)
    for c in range(middle):
        x_copy(minus, c, me.along(1), 0).wait_recv()
        x_start(minus, c, me.along(1), 2)
        x_copy(plus, c + middle, me.along(1), 1).wait_recv()
        x_start(plus, c + middle, me.along(3), 2)

    def send_grads(first, last):
        @pl.loop(first, last)
        def _(h):
            for c in (1, 3, 2):
                grad_copy(h, c).start()

    @pl.loop(0, heads)
    def _(h):
        own_grad(h).start()

    send_grads(0, EARLY)

    for event, (a, b) in enumerate(order):
        d_copy(1 - me.core, event, a, b).wait_recv()

    def multiply(row_block, chunk):
        value = x_buf[row_block, chunk]
        lines = pl.ds(pl.multiple_of(row_block * rows, rows), rows)
        depth = pl.ds(pl.multiple_of(chunk * wide, wide), wide)
        for n in range(cols // 256):
            lanes = slice(n * 256, (n + 1) * 256)
            acc[lines, lanes] += dot_nn(value, w_buf[depth, lanes])
        down_scr[lines, :] += dot_nt(value, adapt_ref[:, depth])

    def prepare(row_block):
        lines = pl.ds(pl.multiple_of(row_block * rows, rows), rows)
        down = down_scr[lines, :].astype(jnp.bfloat16)
        down_b[lines, :] = down
        cos, sin = cos_ref[lines, :], sin_ref[lines, :]
        for h in range(heads):
            lanes = slice(h * HD, (h + 1) * HD)
            value = acc[lines, lanes] + ADAPTER_SCALE * dot_nn(down[:, :RANK], qup_ref[:, lanes])
            value = value.astype(jnp.bfloat16).astype(jnp.float32)
            q_buf[h, lines, :] = rotate(value, cos, sin).astype(jnp.bfloat16)
        value = acc[lines, group : group + HD].astype(jnp.bfloat16).astype(jnp.float32)
        k_scr[lines, :] = rotate(value, cos, sin).astype(jnp.bfloat16)
        v_scr[lines, :] = (
            acc[lines, group + HD :] + ADAPTER_SCALE * dot_nn(down[:, RANK:], vup_ref[...])
        ).astype(jnp.bfloat16)

    @pl.loop(0, CHUNKS)
    def _(c):
        multiply(me.y, c)

    @pl.loop(0, CHUNKS)
    def _(c):
        @pl.when(c >= middle)
        def _():
            x_copy(minus, c, me.along(1), 0).wait_recv()

        multiply(minus, c)

    @pl.loop(0, CHUNKS)
    def _(c):
        @pl.when(c < middle)
        def _():
            x_copy(plus, c, me.along(1), 1).wait_recv()

        multiply(plus, c)

    @pl.loop(0, 3)
    def _(c):
        prepare(lax.rem(me.y + 3 + c, 4))

    @pl.loop(0, middle)
    def _(c):
        x_copy(far, c, me.along(1), 2).wait_recv()
        multiply(far, c)
        x_copy(far, c + middle, me.along(1), 2).wait_recv()
        multiply(far, c + middle)

    send_grads(EARLY, heads)
    prepare(far)
    down_t[...] = down_b[...].astype(jnp.float32).T.astype(jnp.bfloat16)

    row = lax.broadcasted_iota(jnp.int32, (QB, QB), 0)
    col = lax.broadcasted_iota(jnp.int32, (QB, QB), 1)
    causal = row >= col
    factor = SCORE_SCALE * LOG2E

    def send_out(h):
        own_out(h).start()
        for c in (1, 3, 2):
            out_copy(h, c).start()

    @pl.loop(0, heads)
    def _(head):
        own_grad(head).wait()
        for c in (1, 3, 2):
            grad_arrival(head, c).wait_recv()
        head_lanes = pl.ds(pl.multiple_of(head * HD, HD), HD)

        for i in range(blocks):
            own_rows = slice(i * QB, (i + 1) * QB)
            q = q_buf[head, own_rows, :]
            grad = g_buf[head, own_rows, :]
            grad_t = grad.T
            scores = []
            for j in range(i + 1):
                s = dot_nt(q, k_scr[j * QB : (j + 1) * QB, :])
                if j == i:
                    s = jnp.where(causal, s, -1e30)
                scores.append(s)
            top = functools.reduce(jnp.maximum, scores)
            top = jnp.max(top, axis=-1, keepdims=True) * factor
            weights = [jnp.exp2(s * factor - top) for s in scores]
            whole = jnp.sum(functools.reduce(jnp.add, weights), axis=-1, keepdims=True)
            inverse = 1.0 / whole
            probs = [w * inverse for w in weights]
            rounded = [p.astype(jnp.bfloat16) for p in probs]
            attended = functools.reduce(
                jnp.add, [dot_nn(rounded[j], v_scr[j * QB : (j + 1) * QB, :]) for j in range(i + 1)]
            )
            o_buf[head, own_rows, :] = attended.astype(jnp.bfloat16)
            prods = []
            for j in range(i + 1):
                keys = slice(j * QB, (j + 1) * QB)
                dp = dot_nt(grad, v_scr[keys, :])
                prods.append(probs[j] * dp)
                dv_scr[:, keys] += dot_nn(grad_t, rounded[j])
            inner = jnp.sum(functools.reduce(jnp.add, prods), axis=-1, keepdims=True)
            ds = [(prods[j] - probs[j] * inner).astype(jnp.bfloat16) for j in range(i + 1)]
            dq = functools.reduce(
                jnp.add, [dot_nn(ds[j], k_scr[j * QB : (j + 1) * QB, :]) for j in range(i + 1)]
            )
            dq = (dq * SCORE_SCALE).astype(jnp.bfloat16).astype(jnp.float32)
            dq_all[own_rows, head_lanes] = rotate(dq, cos_ref[own_rows, :], -sin_ref[own_rows, :]).astype(
                jnp.bfloat16
            )


        @pl.when(head >= LAG)
        def _():
            send_out(head - LAG)

    dv_t = dv_scr[...].astype(jnp.bfloat16)
    mid_q = dot_nt(dq_all[...], qup_ref[...]).T
    mid_v = dot_nn(vup_ref[...], dv_t)
    for b in range(4):
        lanes = slice(b * rows, (b + 1) * rows)
        mid_scr[b, :RANK] = mid_q[:, lanes]
        mid_scr[b, RANK:] = mid_v[:, lanes]
        mid_mine[b, :RANK] = mid_q[:, lanes].astype(jnp.bfloat16)
        mid_mine[b, RANK:] = mid_v[:, lanes].astype(jnp.bfloat16)

    def mid_copy(c):
        return remote(
            mid_mine, mid_recv.at[c - 1], m_send.at[c - 1], m_recv.at[c - 1], me.along(c)
        )

    for c in (1, 3, 2):
        mid_copy(c).start()
    for n in range(4):
        up = dot_nn(down_t[:RANK, :], dq_all[:, n * 256 : (n + 1) * 256])
        for h in range(2):
            up_part[0, 2 * n + h] = up[:8, h * HD : (h + 1) * HD]
            up_part[1, 2 * n + h] = up[8:, h * HD : (h + 1) * HD]
    up = dot_nt(down_t[RANK:, :], dv_t)
    up_part[0, heads] = up[:8]
    up_part[1, heads] = up[8:]
    for c in (1, 3, 2):
        mid_copy(c).wait_recv()
    send_out(4)
    for b in range(4):
        summed = mid_scr[b]
        for c in range(3):
            summed += mid_recv[c, b].astype(jnp.float32)
        mid_all[b] = summed.astype(jnp.bfloat16)

    def partial(half):
        for n in range(2):
            chunk = 4 * me.y + 2 * half + n
            made = dot_nn(mid_all[0], x_buf[0, chunk])
            for b in range(1, 4):
                made += dot_nn(mid_all[b], x_buf[b, chunk])
            for r in range(2):
                for k in range(4):
                    part[half, r * 8 + n * 4 + k] = made[
                        r * 16 : (r + 1) * 16, k * HD : (k + 1) * HD
                    ]

    partial(1 - me.core)
    swap = remote(part.at[1 - me.core], part_recv, c_send.at[0], c_recv.at[0], me.partner())
    up_swap = remote(up_part.at[1 - me.core], up_recv, c_send.at[1], c_recv.at[1], me.partner())
    swap.start()
    up_swap.start()
    partial(me.core)
    up_swap.wait_recv()
    swap.wait_recv()
    total[:, :16] = (part[me.core] + part_recv[...]).astype(jnp.bfloat16)
    total[:, 16:] = (up_part[me.core] + up_recv[...]).astype(jnp.bfloat16)

    for n, (a, b) in enumerate(AROUND[:-1]):
        dp, fs = me.plane(me.core, a, b)
        remote(
            total.at[lax.div(dp, 2) * 8 + fs],
            rs_recv.at[n],
            r_send.at[0],
            r_recv.at[0],
            (dp, fs, me.y),
        ).start()

    send_out(5)
    send_out(6)
    many = remote(rs_recv, rs_recv, r_send.at[0], r_recv.at[0], me.partner())
    many.wait_recv()
    summed = total[plane].astype(jnp.float32)
    for o in range(PLANE - 1):
        summed += rs_recv[o].astype(jnp.float32)
    final[...] = (ADAPTER_SCALE * summed[:16]).astype(jnp.bfloat16)
    up_final[...] = ADAPTER_SCALE * summed[16:]

    at_rows = pl.ds(pl.multiple_of(lax.div(plane, 8) * 16, 16), 16)
    at_cols = pl.ds(pl.multiple_of(lax.rem(plane, 8) * HD, HD), HD)
    up_cols = pl.ds(pl.multiple_of(plane * HD, HD), HD)

    for a, b in AROUND:
        near = me.plane(me.core, a, b)
        for c in (2, 1, 3, 0):
            if a or b or c:
                remote(
                    final,
                    res.at[me.core, me.y, at_rows, at_cols],
                    r_send.at[1],
                    r_recv.at[1],
                    (*near, lax.rem(me.y + c, 4)),
                ).start()
    for a, b in AROUND[:-1]:
        remote(
            up_final, up_res.at[me.core, :, up_cols], r_send.at[2], r_recv.at[2], me.near(a, b)
        ).start()

    send_out(7)
    res[me.core, me.y, at_rows, at_cols] = final[...]
    up_res[me.core, :, up_cols] = up_final[...]
    all_of = remote(ag_size, ag_size, r_send.at[1], r_recv.at[1], me.partner())
    up_size = ag_size.at[pl.ds(0, PLANE - 1)]
    up_all = remote(up_size, up_size, r_send.at[2], r_recv.at[2], me.partner())
    up_all.wait_recv()
    up_half = remote(
        up_res.at[me.core], up_res.at[me.core], c_send.at[2], c_recv.at[2], me.partner()
    )
    up_half.start()
    all_of.wait_recv()
    half = remote(res.at[me.core], res.at[me.core], c_send.at[3], c_recv.at[3], me.partner())
    half.start()

    def grad_a_writes(b, first):
        copies = []
        for yy in range(4):
            cols_out = pl.ds(pl.multiple_of(yy * 2048 + b * 1024, 1024), 1024)
            for i, dst in enumerate((ga_q_hbm, ga_v_hbm)):
                copies.append(
                    pltpu.make_async_copy(
                        res.at[b, yy, pl.ds(i * RANK, RANK)],
                        dst.at[:, cols_out],
                        write_sem.at[first + yy * 2 + i],
                    )
                )
        return copies

    def grad_b_writes(b, first):
        eight = pl.ds(pl.multiple_of(b * 8, 8), 8)
        return [
            pltpu.make_async_copy(
                up_res.at[b, :, pl.ds(0, group + HD)], gb_hbm.at[eight], write_sem.at[first]
            )
        ]

    writes = grad_a_writes(me.core, 0) + grad_b_writes(me.core, 8)
    for copy in writes:
        copy.start()
    @pl.loop(0, heads)
    def _(h):
        own_out(h).wait()
        for c in (1, 3, 2):
            grad_copy(h, c).wait_send()
            out_copy(h, c).wait_send()
            out_arrival(h, c).wait_recv()

    for copy in sends:
        copy.wait_send()
    up_other = up_res.at[1 - me.core]
    remote(up_other, up_other, c_send.at[2], c_recv.at[2], me.partner()).wait_recv()
    other = res.at[1 - me.core]
    remote(other, other, c_send.at[3], c_recv.at[3], me.partner()).wait_recv()
    late = grad_a_writes(1 - me.core, 10) + grad_b_writes(1 - me.core, 18)
    for copy in late:
        copy.start()
    for c in (1, 3, 2):
        mid_copy(c).wait_send()
    for copy in (up_swap, swap, many, all_of, up_all, up_half, half):
        copy.wait_send()
    for copy in writes + late:
        copy.wait()


def fused_step(tokens, gain, w_qkv, aq_t, av_t, qup, vup, cos, sin, out_grad):
    rows, width = tokens.shape
    shard, cols = w_qkv.shape
    heads = QUERY_PER_KV
    seq = 4 * rows
    wide = width // CHUNKS
    anywhere = pl.BlockSpec(memory_space=pl.ANY)
    dma = pltpu.SemaphoreType.DMA
    f32, bf16 = jnp.float32, jnp.bfloat16
    return pl.pallas_call(
        functools.partial(step_kernel, rows),
        in_specs=[anywhere] * 10,
        out_specs=[anywhere] * 4,
        out_shape=[
            jax.ShapeDtypeStruct((rows, 4 * heads * HD), bf16),
            jax.ShapeDtypeStruct((RANK, width), bf16),
            jax.ShapeDtypeStruct((RANK, width), bf16),
            jax.ShapeDtypeStruct((RANK, (heads + 1) * HD), f32),
        ],
        scratch_shapes=[
            pltpu.VMEM((rows, width), bf16),
            pltpu.VMEM((rows, 128), f32),
            pltpu.VMEM((4, CHUNKS, rows, wide), bf16),
            pltpu.VMEM((width, cols), bf16),
            pltpu.VMEM((seq, cols), f32),
            pltpu.VMEM((seq, 2 * RANK), f32),
            pltpu.VMEM((1, width), f32),
            pltpu.VMEM((2 * RANK, width), bf16),
            pltpu.VMEM((RANK, heads * HD), bf16),
            pltpu.VMEM((RANK, HD), bf16),
            pltpu.VMEM((seq, HD), f32),
            pltpu.VMEM((seq, HD), f32),
            pltpu.VMEM((rows, 4 * heads * HD), bf16),
            pltpu.VMEM((heads, seq, HD), bf16),
            pltpu.VMEM((seq, HD), bf16),
            pltpu.VMEM((seq, HD), bf16),
            pltpu.VMEM((seq, 2 * RANK), bf16),
            pltpu.VMEM((2 * RANK, seq), bf16),
            pltpu.VMEM((HD, seq), f32),
            pltpu.VMEM((seq, heads * HD), bf16),
            pltpu.VMEM((4, 2 * RANK, rows), f32),
            pltpu.VMEM((4, 2 * RANK, rows), bf16),
            pltpu.VMEM((3, 4, 2 * RANK, rows), bf16),
            pltpu.VMEM((4, 2 * RANK, rows), bf16),
            pltpu.VMEM((heads, seq, HD), bf16),
            pltpu.VMEM((heads, seq, HD), bf16),
            pltpu.VMEM((2, PLANE, 16, HD), f32),
            pltpu.VMEM((PLANE, 16, HD), f32),
            pltpu.VMEM((2, PLANE, 8, HD), f32),
            pltpu.VMEM((PLANE, 8, HD), f32),
            pltpu.VMEM((PLANE, 24, HD), bf16),
            pltpu.VMEM((PLANE - 1, 24, HD), bf16),
            pltpu.VMEM((16, HD), bf16),
            pltpu.VMEM((8, HD), f32),
            pltpu.VMEM((2, 4, 2 * RANK, 1024), bf16),
            pltpu.VMEM((2, 8, PLANE * HD), f32),
            pltpu.VMEM((CHIPS - 1, 16, HD), bf16),
            dma((4,)),
            dma((8,)),
            dma(()),
            dma((5, 4)),
            dma((5, 4)),
            dma((16,)),
            dma((16,)),
            dma((3, CHUNKS)),
            dma((3, CHUNKS)),
            dma((heads,)),
            dma((heads,)),
            dma((heads, 3)),
            dma((heads, 3)),
            dma((heads, 3)),
            dma((heads, 3)),
            dma((3,)),
            dma((3,)),
            dma((4,)),
            dma((4,)),
            dma((3,)),
            dma((3,)),
            dma((20,)),
        ],
        compiler_params=pltpu.CompilerParams(
            collective_id=1, has_side_effects=True, vmem_limit_bytes=63 << 20
        ),
        cost_estimate=pl.CostEstimate(
            flops=2 * seq * width * cols,
            bytes_accessed=10 * 1000 * 1000,
            transcendentals=heads * seq * seq,
        ),
        name="fused_step",
    )(tokens, gain.reshape(1, width), w_qkv, aq_t, av_t, qup, vup, cos, sin, out_grad)


def finish_kernel(
    out_in, gq_in, gv_in, gb_in, out, gq, gv, bq, bv, rows, aq, av, fq, fv, b_buf, in_sem, out_sem
):
    parts = 4
    size = rows.shape[0] // parts
    cols = bq.shape[1]
    small = [
        pltpu.make_async_copy(src, dst, in_sem.at[parts + i])
        for i, (src, dst) in enumerate(((gq_in, aq), (gv_in, av), (gb_in, b_buf)))
    ]
    large = [
        pltpu.make_async_copy(
            out_in.at[pl.ds(i * size, size)], rows.at[pl.ds(i * size, size)], in_sem.at[i]
        )
        for i in range(parts)
    ]
    for copy in large + small:
        copy.start()
    writes = []

    def write(src, dst):
        copy = pltpu.make_async_copy(src, dst, out_sem.at[len(writes)])
        copy.start()
        writes.append(copy)

    for i in range(parts):
        large[i].wait()
        write(rows.at[pl.ds(i * size, size)], out.at[pl.ds(i * size, size)])
    small[0].wait()
    fq[...] = aq[...].astype(jnp.float32)
    write(fq, gq)
    small[1].wait()
    fv[...] = av[...].astype(jnp.float32)
    write(fv, gv)
    small[2].wait()
    write(b_buf.at[:, pl.ds(0, cols)], bq)
    write(b_buf.at[:, pl.ds(cols, HD)], bv)
    for copy in writes:
        copy.wait()


def finish(out_rows, ga_query, ga_value, grad_b):
    anywhere = pl.BlockSpec(memory_space=pl.ANY)
    cols = grad_b.shape[1] - HD
    f32 = jnp.float32
    return pl.pallas_call(
        finish_kernel,
        in_specs=[anywhere] * 4,
        out_specs=[anywhere] * 5,
        out_shape=[
            jax.ShapeDtypeStruct(out_rows.shape, out_rows.dtype),
            jax.ShapeDtypeStruct(ga_query.shape, f32),
            jax.ShapeDtypeStruct(ga_value.shape, f32),
            jax.ShapeDtypeStruct((RANK, cols), f32),
            jax.ShapeDtypeStruct((RANK, HD), f32),
        ],
        scratch_shapes=[
            pltpu.VMEM(out_rows.shape, out_rows.dtype),
            pltpu.VMEM(ga_query.shape, ga_query.dtype),
            pltpu.VMEM(ga_value.shape, ga_value.dtype),
            pltpu.VMEM(ga_query.shape, f32),
            pltpu.VMEM(ga_value.shape, f32),
            pltpu.VMEM(grad_b.shape, f32),
            pltpu.SemaphoreType.DMA((7,)),
            pltpu.SemaphoreType.DMA((8,)),
        ],
        name="finish",
    )(out_rows, ga_query, ga_value, grad_b)


def local(tokens, norm_gain, w_qkv, a_query, query_up_adapter, a_value, value_up_adapter, out_grad):
    cos, sin = rotary_tables(4 * tokens.shape[1])
    out_rows, ga_query, ga_value, grad_b = fused_step(
        tokens[0],
        norm_gain,
        w_qkv,
        a_query.T,
        a_value.T,
        query_up_adapter,
        value_up_adapter,
        cos,
        sin,
        out_grad[0],
    )
    out_rows, ga_query, ga_value, gb_query, gb_value = finish(out_rows, ga_query, ga_value, grad_b)
    return out_rows[None], ga_query.T, gb_query, ga_value.T, gb_value


def solution(mesh):
    return jax.shard_map(
        local,
        mesh=mesh,
        in_specs=(
            P(("dp", "fsdp"), "tensor", None),
            P(),
            P(("dp", "fsdp"), "tensor"),
            P(),
            P(None, "tensor"),
            P(),
            P(None, "tensor"),
            P(("dp", "fsdp"), "tensor", None),
        ),
        out_specs=(
            P(("dp", "fsdp"), "tensor", None),
            P(),
            P(None, "tensor"),
            P(),
            P(None, "tensor"),
        ),
        check_vma=False,
    )
```
